32 devices in a mesh: row: 8 (over z, core), col: 4 (over y, x).
Axes of the slice: x: 2, y: 2, z: 4, core: 2. Of those that a mesh axis runs over, the one named last changes fastest.
Arguments:
- energy: float32 [4, 2048, 2048], P('col', 'row'), may hold values from 0.5 to 8
- damage_old: float32 [4, 2048, 2048], P('col', 'row'), may hold values from 0 to 0.8
- crack_seeds: int32 [4, 2048, 2048], P('col', 'row'), may hold values 0 or 1
- irreversible: int32 [4, 2048, 2048], P('col', 'row'), may hold values 0 or 1
- line_inverses: float32 [8, 256, 256], replicated, may hold values from -0.6 to 2.8
- z_inverse: float32 [4, 4], replicated, may hold values from -0.8 to 1.9
Outputs:
- damage: float32 [4, 2048, 2048], P('col', 'row')
- update_norms: float32 [2], replicated
The draws below stay inside these ranges and needn't reach their ends.
All inputs are finite; a program needn't handle non-finite values. No bound on the sum of `crack_seeds` or of `irreversible` on one device may be relied on, other than what follows from the above.
Results may differ from the reference program's by a relative error of at most 0.0001.
Values sent between devices are 32-bit elements; how exact they have to be, the bound alone decides.
A program may use at most 128 MiB of HBM per device.

```python
import math
import jax
import jax.numpy as jnp
from jax import lax

L = 2048
BLK = 256
NBLK = 8
NZ = 4
ITERS = 2


def dominant_blocks(key, block_count, extent, low, high, spread):
    key_diag, key_rest = jax.random.split(key)
    diagonal = jax.random.uniform(key_diag, (block_count, extent), jnp.float32, low, high)
    scatter_part = spread * jax.random.truncated_normal(key_rest, -4.0, 4.0, (block_count, extent, extent), jnp.float32)
    return scatter_part + diagonal[:, :, None] * jnp.eye(extent, dtype=jnp.float32)[None]


def draw_line_inverses(key, part):
    return dominant_blocks(jax.random.fold_in(key, 11), NBLK, BLK, 1.0, 2.0, 0.5 / math.sqrt(BLK))


def draw_z_inverse(key, part):
    return dominant_blocks(jax.random.fold_in(key, 23), 1, NZ, 0.5, 1.0, 0.25 / math.sqrt(NZ))[0]


def plant(array, rng, low, top_value):
    index_at = [jax.random.randint(jax.random.fold_in(rng, axis), (), 0, length) for axis, length in enumerate(array.shape)]
    main_axis = array.shape.index(max(array.shape))
    next_to = index_at[:main_axis] + [(index_at[main_axis] + 1) % array.shape[main_axis]] + index_at[main_axis + 1:]
    return array.at[tuple(index_at)].set(low).at[tuple(next_to)].set(top_value)


def levels(rng, dims, pieces, smallest, high):
    loudness = 1.0
    for dim, blocks in pieces:
        steps = jax.random.uniform(jax.random.fold_in(jax.random.fold_in(rng, 6), dim), (blocks,), jnp.float32, smallest / len(pieces), high / len(pieces))
        loudness = loudness * jnp.repeat(jnp.exp(steps), dims[dim] // blocks).reshape((-1,) + (1,) * (len(dims) - 1 - dim))
    return loudness


def setup_inputs(seed: int = 0) -> dict:
    key_list = jax.random.split(jax.random.key(seed), 7)
    return {
        "energy": jnp.clip(jnp.exp(math.log(8.0) - 2.7725887 * jax.random.uniform(key_list[0], (NZ, L, L), jnp.float32) ** levels(key_list[0], (NZ, L, L), ((0, 4), (1, 8)), -0.2, 0.2)), 0.5, 8.0),
        "damage_old": jnp.clip(0.8 * jax.random.uniform(key_list[1], (NZ, L, L), jnp.float32) ** levels(key_list[1], (NZ, L, L), ((0, 4), (1, 8)), -0.2, 0.2), 0.0, 0.8),
        "crack_seeds": plant((jax.random.randint(key_list[2], (NZ, L, L), 0, 32) < 1).astype(jnp.int32), jax.random.fold_in(key_list[2], 1), 0, 1),
        "irreversible": plant((jax.random.randint(key_list[3], (NZ, L, L), 0, 2) < 1).astype(jnp.int32), jax.random.fold_in(key_list[3], 1), 0, 1),
        "line_inverses": draw_line_inverses(jax.random.fold_in(key_list[6], 71), 0),
        "z_inverse": draw_z_inverse(jax.random.fold_in(key_list[6], 71), 0),
    }


KAPPA = 2.0
STEP = 0.02
COUPLE = 0.5
EPSILON = 1e-06

def second_difference(grid_field, along):
    extent = grid_field.shape[along]
    forward_diff = lax.slice_in_dim(grid_field, 1, extent, axis=along) - lax.slice_in_dim(grid_field, 0, extent - 1, axis=along)
    zero_shape = list(grid_field.shape)
    zero_shape[along] = 1
    zero_rim = jnp.zeros(zero_shape, grid_field.dtype)
    ahead = jnp.concatenate([forward_diff, zero_rim], axis=along)
    behind = jnp.concatenate([zero_rim, forward_diff], axis=along)
    return ahead - behind

def line_solve(line_rows, inverses):
    block_count, block_cells, _ = inverses.shape
    line_count = line_rows.shape[0]
    blocks = line_rows.reshape(line_count, block_count, block_cells)
    products = jnp.einsum('rkb,kcb->rkc', blocks, inverses, precision=lax.Precision.HIGHEST)
    first_col = inverses[:, :, 0]
    last_col = inverses[:, :, block_cells - 1]
    incoming = [jnp.zeros((line_count,), line_rows.dtype)]
    for block_index in range(block_count - 1):
        incoming.append(products[:, block_index, block_cells - 1] + COUPLE * incoming[block_index] * inverses[block_index, block_cells - 1, 0])
    inflow = jnp.stack(incoming, axis=1)
    forward = products + COUPLE * inflow[:, :, None] * first_col[None]
    head_terms = [jnp.zeros((line_count,), line_rows.dtype) for block_index in range(block_count)]
    carried = forward[:, block_count - 1, 0]
    for block_index in range(block_count - 2, -1, -1):
        head_terms[block_index] = carried
        carried = forward[:, block_index, 0] + COUPLE * carried * inverses[block_index, 0, block_cells - 1]
    outflow = jnp.stack(head_terms, axis=1)
    solved = forward + COUPLE * outflow[:, :, None] * last_col[None]
    return solved.reshape(line_count, block_count * block_cells)

def reference(energy, damage_old, crack_seeds, irreversible, line_inverses, z_inverse):
    seeded = crack_seeds == 1
    damage = jnp.where(seeded, 1.0, damage_old)
    lower_bound = jnp.where(irreversible == 1, damage_old, 0.0)
    line_length = energy.shape[2]
    update_sizes = []
    for sweep_index in range(ITERS):
        laplace = second_difference(damage, 0) + second_difference(damage, 1) + second_difference(damage, 2)
        residual = energy - (1.0 + energy) * damage + KAPPA * laplace
        along_x = line_solve(residual.reshape(-1, line_length), line_inverses).reshape(residual.shape)
        turned = jnp.swapaxes(along_x, 1, 2)
        along_y = line_solve(turned.reshape(-1, line_length), line_inverses).reshape(turned.shape)
        along_z = jnp.einsum('zk,kxy->zxy', z_inverse, along_y, precision=lax.Precision.HIGHEST)
        update = STEP * jnp.swapaxes(along_z, 1, 2)
        clamped = jnp.minimum(jnp.maximum(damage + update, lower_bound), 1.0)
        renewed = jnp.where(seeded, 1.0, clamped)
        update_sizes.append(jnp.sqrt(jnp.mean((renewed - damage) ** 2) + EPSILON) / STEP)
        damage = renewed
    return (damage, jnp.stack(update_sizes))
```

```python
import functools

import jax
import jax.numpy as jnp
from jax import lax
from jax.experimental import pallas as pl
from jax.experimental.pallas import tpu as pltpu
from jax.sharding import PartitionSpec as P

ITERS = 2


KAPPA = 2.0
STEP = 0.02
COUPLE = 0.5
EPSILON = 1e-06
HIGHEST = lax.Precision.HIGHEST


def second_difference(grid_field, along):
    extent = grid_field.shape[along]
    forward_diff = lax.slice_in_dim(grid_field, 1, extent, axis=along) - lax.slice_in_dim(
        grid_field, 0, extent - 1, axis=along
    )
    zero_shape = list(grid_field.shape)
    zero_shape[along] = 1
    zero_rim = jnp.zeros(zero_shape, grid_field.dtype)
    ahead = jnp.concatenate([forward_diff, zero_rim], axis=along)
    behind = jnp.concatenate([zero_rim, forward_diff], axis=along)
    return ahead - behind


def line_solve(line_rows, inverses):
    block_count, block_cells, _ = inverses.shape
    line_count = line_rows.shape[0]
    blocks = line_rows.reshape(line_count, block_count, block_cells)
    products = jnp.einsum("rkb,kcb->rkc", blocks, inverses, precision=lax.Precision.HIGHEST)
    first_col = inverses[:, :, 0]
    last_col = inverses[:, :, block_cells - 1]
    incoming = [jnp.zeros((line_count,), line_rows.dtype)]
    for block_index in range(block_count - 1):
        incoming.append(
            products[:, block_index, block_cells - 1]
            + COUPLE * incoming[block_index] * inverses[block_index, block_cells - 1, 0]
        )
    inflow = jnp.stack(incoming, axis=1)
    forward = products + COUPLE * inflow[:, :, None] * first_col[None]
    head_terms = [jnp.zeros((line_count,), line_rows.dtype) for block_index in range(block_count)]
    carried = forward[:, block_count - 1, 0]
    for block_index in range(block_count - 2, -1, -1):
        head_terms[block_index] = carried
        carried = (
            forward[:, block_index, 0]
            + COUPLE * carried * inverses[block_index, 0, block_cells - 1]
        )
    outflow = jnp.stack(head_terms, axis=1)
    solved = forward + COUPLE * outflow[:, :, None] * last_col[None]
    return solved.reshape(line_count, block_count * block_cells)


def local_turned(energy, damage_old, crack_seeds, irreversible, line_inverses, z_inverse):
    planes, rows_here, line_length = energy.shape
    row_count = lax.axis_size("row")
    col_count = lax.axis_size("col")
    total_planes = planes * col_count
    cell_count = total_planes * rows_here * row_count * line_length
    seeded = crack_seeds == 1
    damage = jnp.where(seeded, 1.0, damage_old)
    lower_bound = jnp.where(irreversible == 1, damage_old, 0.0)
    own_sums = []
    for sweep_index in range(ITERS):
        local_lap = second_difference(damage, 2)
        partial_value = energy - (1.0 + energy) * damage + KAPPA * local_lap
        moved_part, moved_damage = (
            lax.all_to_all(
                lax.all_to_all(
                    jnp.swapaxes(partial_value, 1, 2),
                    "row",
                    split_axis=1,
                    concat_axis=2,
                    tiled=True,
                ),
                "col",
                split_axis=1,
                concat_axis=0,
                tiled=True,
            ),
            lax.all_to_all(
                lax.all_to_all(
                    jnp.swapaxes(damage, 1, 2), "row", split_axis=1, concat_axis=2, tiled=True
                ),
                "col",
                split_axis=1,
                concat_axis=0,
                tiled=True,
            ),
        )
        lap_rest = second_difference(moved_damage, 2) + second_difference(moved_damage, 0)
        turned = moved_part + KAPPA * lap_rest
        turned_shape = turned.shape
        along_y = line_solve(turned.reshape(-1, turned_shape[2]), line_inverses).reshape(
            turned_shape
        )
        along_z = jnp.einsum("zk,kxy->zxy", z_inverse, along_y, precision=lax.Precision.HIGHEST)
        gathered = lax.all_to_all(
            lax.all_to_all(along_z, "row", split_axis=2, concat_axis=1, tiled=True),
            "col",
            split_axis=0,
            concat_axis=1,
            tiled=True,
        )
        piece_cells = gathered.shape[1] // (row_count * col_count)
        reordered = gathered.reshape(planes, col_count, row_count, piece_cells, rows_here)
        restored = jnp.transpose(reordered, (0, 4, 2, 1, 3)).reshape(planes, rows_here, line_length)
        update = STEP * line_solve(restored.reshape(-1, line_length), line_inverses).reshape(
            restored.shape
        )
        clamped = jnp.minimum(jnp.maximum(damage + update, lower_bound), 1.0)
        renewed = jnp.where(seeded, 1.0, clamped)
        own_sum = jnp.sum((renewed - damage) ** 2)
        own_sums.append(own_sum)
        damage = renewed
    global_sums = lax.psum(jnp.stack(own_sums), ("row", "col"))
    update_norms = jnp.sqrt(global_sums / cell_count + EPSILON) / STEP
    return (damage, update_norms)


def line_kernel(
    shape,
    z_inv,
    energy,
    damage_hbm,
    seeds_hbm,
    irreversible_hbm,
    inverses,
    out,
    norms,
    damage_old,
    crack_seeds,
    irreversible,
    start,
    bound,
    ez,
    fz,
    landing,
    dz,
    final,
    w_high,
    w_low,
    mix,
    corner,
    gx,
    gy,
    gx_high,
    gx_low,
    gy_high,
    gy_low,
    gy_ends,
    gend,
    ab_x,
    ab_y,
    carry_rows,
    x_send,
    x_all,
    y_send,
    y_all,
    s_send,
    s_row,
    s_col_send,
    s_col,
    local_sems,
    e_ssem,
    e_rsem,
    d_ssem,
    d_rsem,
    f_ssem,
    f_rsem,
    back_ssem,
    back_rsem,
    x_ssem,
    x_rsem,
    v_ssem,
    v_rsem,
    y_ssem,
    y_rsem,
    sc_ssem,
    sc_rsem,
    sr_ssem,
    sr_rsem,
):
    rows, cols, cells, width, x_blocks, blocks, cell_count = shape
    planes = cols
    last = cells - 1
    groups = width // 128
    pieces = 4
    piece = cells // pieces
    ends = 8
    f32 = jnp.float32
    row, col = lax.axis_index("row"), lax.axis_index("col")
    row_peers = [lax.rem(row + o, rows) for o in range(1, rows)]
    col_peers = [lax.rem(col + o, cols) for o in range(1, cols)]

    def slab(who):
        return pl.ds(pl.multiple_of(who * width, width), width)

    def eight(at):
        return pl.ds(pl.multiple_of(at, 8), 8)

    def send(src, dst, ssem, rsem, **where):
        copy = pltpu.make_async_remote_copy(
            src_ref=src, dst_ref=dst, send_sem=ssem, recv_sem=rsem,
            device_id=where, device_id_type=pl.DeviceIdType.MESH,
        )
        copy.start()
        return copy

    def finish(sent):
        for copy in sent:
            copy.wait()

    def weighted(weights, field, kept):
        total = None
        for n in kept:
            term = weights[:, n : n + 1] * field[n : n + 1]
            total = term if total is None else total + term
        return total

    def split(a):
        high = a.astype(jnp.bfloat16)
        return high, (a - high.astype(f32)).astype(jnp.bfloat16)

    def dot3(a, b):
        def part(u, v):
            return jnp.dot(u, v, preferred_element_type=f32)

        return part(a[0], b[0]) + (part(a[0], b[1]) + part(a[1], b[0]))

    def line_ends(field):
        tile_lane = lax.broadcasted_iota(jnp.int32, (cells, 128), 1)
        packed = field[:, :128]
        for j in range(x_blocks):
            begin = field[:, j * cells : j * cells + 128]
            end = field[:, (j + 1) * cells - 128 : (j + 1) * cells]
            if j > 0:
                begin = pltpu.roll(begin, j, 1)
                end = pltpu.roll(end, 128 - j, 1)
            packed = jnp.where(tile_lane == j, begin, packed)
            packed = jnp.where(tile_lane == 127 - j, end, packed)
        turned = packed.T
        at = lax.broadcasted_iota(jnp.int32, (8, cells), 0)
        return jnp.where(at < x_blocks, turned[:8], turned[120:])

    barrier = pltpu.get_barrier_semaphore()
    for peer in col_peers:
        pl.semaphore_signal(
            barrier, inc=1, device_id={"col": peer}, device_id_type=pl.DeviceIdType.MESH
        )
    for peer in row_peers:
        pl.semaphore_signal(
            barrier, inc=1, device_id={"row": peer}, device_id_type=pl.DeviceIdType.MESH
        )

    pulls = [
        pltpu.make_async_copy(damage_hbm, damage_old, local_sems.at[0]),
        pltpu.make_async_copy(seeds_hbm, crack_seeds, local_sems.at[1]),
        pltpu.make_async_copy(irreversible_hbm, irreversible, local_sems.at[2]),
    ]
    fetch = [
        pltpu.make_async_copy(energy.at[:, slab(col)], ez.at[col], local_sems.at[3]),
        pltpu.make_async_copy(inverses.at[row], gy, local_sems.at[4]),
    ]
    for n in range(4):
        down, over = (cells - 8) * (n // 2), (cells - 128) * (n % 2)
        fetch.append(
            pltpu.make_async_copy(
                inverses.at[:, pl.ds(down, 8), pl.ds(over, 128)], corner.at[n], local_sems.at[5 + n]
            )
        )
    for j in range(x_blocks):
        fetch.append(
            pltpu.make_async_copy(inverses.at[col * x_blocks + j], gx.at[j], local_sems.at[9 + j])
        )
    for copy in pulls + fetch:
        copy.start()
    pl.semaphore_wait(barrier, rows + cols - 2)

    def move(src, landing_at, ssem, rsem):
        return [
            send(src.at[:, slab(peer)], landing_at, ssem.at[n], rsem.at[n], col=peer)
            for n, peer in enumerate(col_peers)
        ]

    def move_bound(index):
        at = pl.ds(index * piece, piece)
        return [
            send(bound.at[at, slab(peer)], fz.at[col, at, :], f_ssem.at[index, n],
                 f_rsem.at[index, n], col=peer)
            for n, peer in enumerate(col_peers)
        ]

    moved_e = move(energy, ez.at[col], e_ssem, e_rsem)
    finish(pulls)

    @pl.loop(0, cells // 16)
    def _(i):
        at = pl.ds(pl.multiple_of(i * 16, 16), 16)
        old = damage_old[at, :]
        seeded = crack_seeds[at, :] == 1
        start[at, :] = jnp.where(seeded, 1.0, old)
        bound[at, :] = jnp.where(seeded, 1.0, jnp.where(irreversible[at, :] == 1, old, 0.0))

    moved_d = move(start, landing.at[col], d_ssem, d_rsem)
    moved_f = {n: move_bound(n) for n in (0, pieces - 1)}
    landing[col] = start[:, slab(col)]
    fz[col] = bound[:, slab(col)]

    lane = lax.broadcasted_iota(jnp.int32, (8, 128), 1)
    sub = lax.broadcasted_iota(jnp.int32, (8, 128), 0)
    finish(fetch)

    def corner_of(down, over, k):
        tile = corner[2 * down + over, k]
        at = (7 if down else 0, 127 if over else 0)
        return jnp.broadcast_to(tile[at[0] : at[0] + 1, at[1] : at[1] + 1], (8, 128))

    def hot(index):
        return jnp.where(lane == index, 1.0, 0.0)

    def carries(first, final_of, own, lower=None, upper=None):
        zero = jnp.zeros((8, 128), f32)
        firsts, finals = [], []
        for k in range(blocks):
            begin, end = hot(first(k)), hot(final_of(k))
            low = None if lower is None else lower(k)
            high = None if upper is None else upper(k)
            if low is not None:
                begin = begin + corner_of(0, 0, k) * hot(low)
                end = end + corner_of(1, 0, k) * hot(low)
            if high is not None:
                begin = begin + corner_of(0, 1, k) * hot(high)
                end = end + corner_of(1, 1, k) * hot(high)
            firsts.append(begin)
            finals.append(end)
        incoming = [zero]
        for k in range(blocks - 1):
            incoming.append(finals[k] + COUPLE * corner_of(1, 0, k) * incoming[k])
        heads = [
            firsts[k] + COUPLE * corner_of(0, 0, k) * incoming[k] for k in range(blocks)
        ]
        carried = heads[blocks - 1]
        outgoing = [zero] * blocks
        for k in range(blocks - 2, -1, -1):
            outgoing[k] = carried
            carried = heads[k] + COUPLE * corner_of(0, 1, k) * carried
        picked = zero
        even = lax.rem(sub, 2) == 0
        for k in range(blocks):
            enter, leave = COUPLE * incoming[k], COUPLE * outgoing[k]
            if lower is not None and lower(k) is not None:
                enter = enter + hot(lower(k))
            if upper is not None and upper(k) is not None:
                leave = leave + hot(upper(k))
            picked = picked + jnp.where(own == k, jnp.where(even, enter, leave), 0.0)
        return picked

    half = lax.div(sub, 2)

    def left_of(k):
        c = k // x_blocks
        return ends * (c - 1) + x_blocks + 1 if k % x_blocks == 0 and c > 0 else None

    def right_of(k):
        c = k // x_blocks
        return ends * (c + 1) + x_blocks if k % x_blocks == x_blocks - 1 and c < cols - 1 else None

    ab_x[...] = carries(
        lambda k: ends * (k // x_blocks) + k % x_blocks,
        lambda k: ends * (k // x_blocks) + 7 - k % x_blocks,
        jnp.where(half < x_blocks, col * x_blocks + half, -1),
        left_of,
        right_of,
    )
    ab_y[...] = carries(
        lambda k: 2 * planes * k + 2 * half,
        lambda k: 2 * planes * k + 2 * half + 1,
        row + 0 * sub,
    )

    for j in range(x_blocks):
        turned = gx[j].T
        gx_high[j], gx_low[j] = split(turned)
        gend[2 * j] = jnp.broadcast_to(turned[:1], (8, cells))
        gend[2 * j + 1] = jnp.broadcast_to(turned[last:], (8, cells))
    gy_high[...], gy_low[...] = split(gy[...])
    gy_ends[0] = jnp.broadcast_to(gy[:, :1], (cells, 128))
    gy_ends[1] = jnp.broadcast_to(gy[:, last:], (cells, 128))

    first_col = jnp.where(col == 0, 1.0, 0.0)
    last_col = jnp.where(col == cols - 1, 1.0, 0.0)
    lane16 = lax.broadcasted_iota(jnp.int32, (16, 128), 1)
    at_first, at_last = lane16 == 0, lane16 == 127

    finish(moved_d)

    @pl.loop(0, cells // 8)
    def _(i):
        for z in range(planes):
            tile = landing[z, eight(i * 8), :]
            for g in range(groups):
                dz[0, z, g, eight(i * 8 + 8), :] = tile[:, g * 128 : (g + 1) * 128]

    def share_rows(it):
        return [
            send(dz.at[it, :, :, pl.ds(cells, 8), :], dz.at[it, :, :, pl.ds(0, 8), :],
                 v_ssem.at[it, 0], v_rsem.at[it, 0], row=lax.rem(row + 1, rows)),
            send(dz.at[it, :, :, pl.ds(8, 8), :], dz.at[it, :, :, pl.ds(cells + 8, 8), :],
                 v_ssem.at[it, 1], v_rsem.at[it, 1], row=lax.rem(row + rows - 1, rows)),
        ]

    def mirror(it):
        for z in range(planes):
            for g in range(groups):
                dz[it, z, g, 7:8, :] = jnp.where(
                    row == 0, dz[it, z, g, 8:9, :], dz[it, z, g, 7:8, :]
                )
                dz[it, z, g, cells + 8 : cells + 9, :] = jnp.where(
                    row == rows - 1,
                    dz[it, z, g, cells + 7 : cells + 8, :],
                    dz[it, z, g, cells + 8 : cells + 9, :],
                )

    def residual(it, low, high):
        @pl.loop(low // 16, high // 16)
        def _(i):
            base = pl.multiple_of(i * 16, 16)
            here = pl.ds(base, 16)
            padded = pl.ds(pl.multiple_of(base + 8, 8), 16)
            for g in range(groups):
                lanes = slice(g * 128, (g + 1) * 128)
                mids = [dz[it, z, g, padded, :] for z in range(planes)]
                value = []
                for z in range(planes):
                    d = mids[z]
                    near = dz[it, z, g, pl.ds(base + 7, 16), :] + dz[it, z, g, pl.ds(base + 9, 16), :]
                    before = d * first_col
                    if g > 0:
                        before = pltpu.roll(dz[it, z, g - 1, padded, :], 1, 1)
                    after = d * last_col
                    if g < groups - 1:
                        after = pltpu.roll(dz[it, z, g + 1, padded, :], 127, 1)
                    near = near + jnp.where(at_first, before, pltpu.roll(d, 1, 1))
                    near = near + jnp.where(at_last, after, pltpu.roll(d, 127, 1))
                    sides = 4
                    if z > 0:
                        near = near + mids[z - 1]
                        sides += 1
                    if z < planes - 1:
                        near = near + mids[z + 1]
                        sides += 1
                    e = ez[z, here, lanes]
                    value.append((e - (e + (1.0 + KAPPA * sides)) * d) + KAPPA * near)
                for z in range(planes):
                    total = z_inv[z, 0] * value[0]
                    for k in range(1, planes):
                        total = total + z_inv[z, k] * value[k]
                    w_high[z, here, lanes], w_low[z, here, lanes] = split(total)

    def products(it):
        @pl.loop(0, planes)
        def _(z):
            along = jnp.concatenate(
                [
                    dot3(
                        (w_high[z, :, j * cells : (j + 1) * cells],
                         w_low[z, :, j * cells : (j + 1) * cells]),
                        (gx_high[j], gx_low[j]),
                    )
                    for j in range(x_blocks)
                ],
                axis=1,
            )
            both = dot3((gy_high[...], gy_low[...]), split(along))
            mix[z] = both
            x_send[it, :, pl.ds(pl.multiple_of(z * cells, cells), cells)] = line_ends(both)

    def edges(it):
        tile_lane = lax.broadcasted_iota(jnp.int32, (cells, 128), 1)
        packed = jnp.zeros((cells, 128), f32)
        for z in range(planes):
            begin = dz[it, z, 0, pl.ds(8, cells), :]
            end = dz[it, z, groups - 1, pl.ds(8, cells), :]
            if z > 0:
                begin = pltpu.roll(begin, z, 1)
            end = pltpu.roll(end, planes + z + 1, 1)
            packed = jnp.where(tile_lane == z, begin, packed)
            packed = jnp.where(tile_lane == planes + z, end, packed)
        turned = dot3((gy_high[...], gy_low[...]), split(packed)).T
        for z in range(planes):
            for side in range(2):
                total = None
                for k in range(planes):
                    n = side * planes + k
                    term = (KAPPA * z_inv[z, k]) * turned[n : n + 1]
                    total = term if total is None else total + term
                x_send[it, x_blocks + side : x_blocks + side + 1,
                       z * cells : (z + 1) * cells] = total

    kept_x = [
        ends * c + n for c in range(cols) for n in range(ends)
        if n < x_blocks + 2 or n >= ends - x_blocks
    ]

    def x_share(it):
        own = pl.ds(pl.multiple_of(col * ends, ends), ends)
        sent = [
            send(x_send.at[it], x_all.at[it, own, :], x_ssem.at[it, n], x_rsem.at[it, n], col=peer)
            for n, peer in enumerate(col_peers)
        ]
        x_all[it, own, :] = x_send[it]
        return sent

    def y_share(it):
        lines = []
        for z in range(planes):
            lines.append(weighted(ab_x[...], x_all[it, :, z * cells : (z + 1) * cells], kept_x))
        for z in range(planes):
            for top, at in ((0, 0), (1, last)):
                for j in range(x_blocks):
                    block = slice(j * cells, (j + 1) * cells)
                    line = (
                        mix[z, at : at + 1, block]
                        + lines[z][2 * j : 2 * j + 1, at : at + 1] * gend[2 * j, :1, :]
                        + lines[z][2 * j + 1 : 2 * j + 2, at : at + 1] * gend[2 * j + 1, :1, :]
                    )
                    y_send[it, 2 * z + top : 2 * z + top + 1, block] = line
        own = pl.ds(pl.multiple_of(row * 2 * planes, 2 * planes), 2 * planes)
        sent = [
            send(y_send.at[it], y_all.at[it, own, :], y_ssem.at[it, n], y_rsem.at[it, n], row=peer)
            for n, peer in enumerate(row_peers)
        ]
        y_all[it, own, :] = y_send[it]
        stacked = jnp.concatenate(
            lines + [jnp.zeros((128 - 8 * planes, cells), f32)], axis=0
        ).T
        for t in range(cells // 8):
            here = slice(t * 8, t * 8 + 8)
            tile = stacked[here]
            for z in range(planes):
                for j in range(x_blocks):
                    block = slice(j * cells, (j + 1) * cells)
                    n = 8 * z + 2 * j
                    mix[z, here, block] = (
                        mix[z, here, block]
                        + tile[:, n : n + 1] * gend[2 * j]
                        + tile[:, n + 1 : n + 2] * gend[2 * j + 1]
                    )
        finish(sent)
        carry = weighted(ab_y[...], y_all[it], range(rows * 2 * planes))
        for n in range(2 * planes):
            carry_rows[n] = jnp.broadcast_to(carry[n : n + 1], (8, width))

    def settle(it, low, high, squares):
        def step(i, acc):
            here, padded = eight(i * 8), eight(i * 8 + 8)
            g_first = jnp.concatenate([gy_ends[0, here, :]] * groups, axis=1)
            g_last = jnp.concatenate([gy_ends[1, here, :]] * groups, axis=1)
            for z in range(planes):
                solved = mix[z, here, :] + g_first * carry_rows[2 * z] + g_last * carry_rows[2 * z + 1]
                d = jnp.concatenate([dz[it, z, g, padded, :] for g in range(groups)], axis=1)
                renewed = jnp.minimum(jnp.maximum(d + STEP * solved, fz[z, here, :]), 1.0)
                if it + 1 < ITERS:
                    for g in range(groups):
                        dz[it + 1, z, g, padded, :] = renewed[:, g * 128 : (g + 1) * 128]
                else:
                    final[z, here, :] = renewed
                change = renewed - d
                acc = acc + change * change
            return acc

        return lax.fori_loop(low // 8, high // 8, step, squares)

    totals = []
    blank = jnp.zeros((8, width), f32)

    shared = share_rows(0)
    finish(moved_e)
    finish(shared)
    mirror(0)
    residual(0, 0, cells)
    products(0)
    edges(0)
    sent = x_share(0)
    for n in range(1, pieces - 1):
        moved_f[n] = move_bound(n)
    finish(sent)
    y_share(0)

    squares = blank
    finish(moved_f[0])
    squares = settle(0, 0, piece, squares)
    finish(moved_f[pieces - 1])
    squares = settle(0, cells - piece, cells, squares)
    shared = share_rows(1)
    residual(1, cells - piece + 16, cells - 16)
    for n in range(1, pieces - 1):
        finish(moved_f[n])
        squares = settle(0, n * piece, (n + 1) * piece, squares)
        low = 16 if n == 1 else n * piece - 16
        high = (n + 1) * piece - 16
        residual(1, low, high if n < pieces - 2 else high + 32)
    totals.append(jnp.sum(squares))
    finish(shared)
    mirror(1)
    residual(1, 0, 16)
    residual(1, cells - 16, cells)
    products(1)
    edges(1)
    finish(x_share(1))
    y_share(1)

    def give_back(n):
        at = pl.ds(n * piece, piece)
        return [
            send(final.at[peer, at, :], out.at[at, slab(col)], back_ssem.at[n, m],
                 back_rsem.at[n, m], col=peer)
            for m, peer in enumerate(col_peers)
        ]

    squares = blank
    backs = []
    for n in range(pieces):
        squares = settle(ITERS - 1, n * piece, (n + 1) * piece, squares)
        if n < 2:
            backs += give_back(n)
    totals.append(jnp.sum(squares))
    s_send[...] = jnp.where(sub == 0, totals[0], jnp.where(sub == 1, totals[1], 0.0))
    shares = [
        send(s_send, s_row.at[n], sr_ssem.at[n], sr_rsem.at[n], row=peer)
        for n, peer in enumerate(row_peers)
    ]
    out[:, slab(col)] = final[col]
    finish(shares)
    total = s_send[...]
    for n in range(rows - 1):
        total = total + s_row[n]
    s_col_send[...] = total
    shares = [
        send(s_col_send, s_col.at[n], sc_ssem.at[n], sc_rsem.at[n], col=peer)
        for n, peer in enumerate(col_peers)
    ]
    for n in range(2, pieces):
        backs += give_back(n)
    finish(shares)
    for n in range(cols - 1):
        total = total + s_col[n]
    norms[...] = jnp.sqrt(total / cell_count + EPSILON) / STEP
    finish(backs)


def local(energy, damage_old, crack_seeds, irreversible, line_inverses, z_inverse):
    planes, cells, line_length = energy.shape
    rows, cols = lax.axis_size("row"), lax.axis_size("col")
    blocks, _, _ = line_inverses.shape
    width = line_length // cols
    x_blocks = width // cells
    lines = cols * cells
    pieces = 4
    shape = (rows, cols, cells, width, x_blocks, blocks, float(cols * rows * cells * line_length))
    f32 = jnp.float32
    bf16 = jnp.bfloat16
    dma = pltpu.SemaphoreType.DMA
    vmem = pl.BlockSpec(memory_space=pltpu.VMEM)
    smem = pl.BlockSpec(memory_space=pltpu.SMEM)
    damage, norms = pl.pallas_call(
        functools.partial(line_kernel, shape),
        out_shape=(
            jax.ShapeDtypeStruct((cells, line_length), f32),
            jax.ShapeDtypeStruct((8, 128), f32),
        ),
        in_specs=[smem] + [pl.BlockSpec(memory_space=pl.ANY)] * 5,
        out_specs=(vmem, vmem),
        scratch_shapes=[
            pltpu.VMEM((cells, line_length), f32),
            pltpu.VMEM((cells, line_length), jnp.int32),
            pltpu.VMEM((cells, line_length), jnp.int32),
            pltpu.VMEM((cells, line_length), f32),
            pltpu.VMEM((cells, line_length), f32),
            pltpu.VMEM((cols, cells, width), f32),
            pltpu.VMEM((cols, cells, width), f32),
            pltpu.VMEM((cols, cells, width), f32),
            pltpu.VMEM((ITERS, cols, width // 128, cells + 16, 128), f32),
            pltpu.VMEM((cols, cells, width), f32),
            pltpu.VMEM((cols, cells, width), bf16),
            pltpu.VMEM((cols, cells, width), bf16),
            pltpu.VMEM((cols, cells, width), f32),
            pltpu.VMEM((4, blocks, 8, 128), f32),
            pltpu.VMEM((x_blocks, cells, cells), f32),
            pltpu.VMEM((cells, cells), f32),
            pltpu.VMEM((x_blocks, cells, cells), bf16),
            pltpu.VMEM((x_blocks, cells, cells), bf16),
            pltpu.VMEM((cells, cells), bf16),
            pltpu.VMEM((cells, cells), bf16),
            pltpu.VMEM((2, cells, 128), f32),
            pltpu.VMEM((2 * x_blocks, 8, cells), f32),
            pltpu.VMEM((8, 128), f32),
            pltpu.VMEM((8, 128), f32),
            pltpu.VMEM((2 * cols, 8, width), f32),
            pltpu.VMEM((ITERS, 8, lines), f32),
            pltpu.VMEM((ITERS, 8 * cols, lines), f32),
            pltpu.VMEM((ITERS, 2 * cols, width), f32),
            pltpu.VMEM((ITERS, 2 * cols * rows, width), f32),
            pltpu.VMEM((8, 128), f32),
            pltpu.VMEM((rows - 1, 8, 128), f32),
            pltpu.VMEM((8, 128), f32),
            pltpu.VMEM((cols - 1, 8, 128), f32),
            dma((x_blocks + 9,)),
            dma((cols - 1,)),
            dma((cols - 1,)),
            dma((cols - 1,)),
            dma((cols - 1,)),
            dma((pieces, cols - 1)),
            dma((pieces, cols - 1)),
            dma((pieces, cols - 1)),
            dma((pieces, cols - 1)),
            dma((ITERS, cols - 1)),
            dma((ITERS, cols - 1)),
            dma((ITERS, 2)),
            dma((ITERS, 2)),
            dma((ITERS, rows - 1)),
            dma((ITERS, rows - 1)),
            dma((cols - 1,)),
            dma((cols - 1,)),
            dma((rows - 1,)),
            dma((rows - 1,)),
        ],
        compiler_params=pltpu.CompilerParams(
            has_side_effects=True, collective_id=0, vmem_limit_bytes=60 * 1024 * 1024
        ),
        name="line_iterations",
    )(
        z_inverse,
        energy[0],
        damage_old[0],
        crack_seeds[0],
        irreversible[0],
        line_inverses,
    )
    return damage[None], norms[:ITERS, 0]


def solution(mesh):
    def local_any(energy, damage_old, crack_seeds, irreversible, line_inverses, z_inverse):
        rows, cols = mesh.shape["row"], mesh.shape["col"]
        block_cells = line_inverses.shape[1]
        width = energy.shape[2] // cols
        whole_blocks = (
            energy.shape[0] == 1
            and energy.shape[1] == block_cells
            and width % block_cells == 0
            and 2 * (width // block_cells) + 2 <= 8
            and block_cells % 128 == 0
            and 2 * cols == 8
            and 8 * max(rows, cols) <= 128
            and min(rows, cols) > 2
        )
        chosen = local if whole_blocks else local_turned
        return chosen(energy, damage_old, crack_seeds, irreversible, line_inverses, z_inverse)

    return jax.shard_map(
        local_any,
        mesh=mesh,
        in_specs=(
            P("col", "row", None),
            P("col", "row", None),
            P("col", "row", None),
            P("col", "row", None),
            P(),
            P(),
        ),
        out_specs=(P("col", "row", None), P()),
        check_vma=False,
    )
```

```python
import functools

import jax
import jax.numpy as jnp
from jax import lax
from jax.experimental import pallas as pl
from jax.experimental.pallas import tpu as pltpu
from jax.sharding import PartitionSpec as P

ITERS = 2


KAPPA = 2.0
STEP = 0.02
COUPLE = 0.5
EPSILON = 1e-06
HIGHEST = lax.Precision.HIGHEST


def second_difference(grid_field, along):
    extent = grid_field.shape[along]
    forward_diff = lax.slice_in_dim(grid_field, 1, extent, axis=along) - lax.slice_in_dim(
        grid_field, 0, extent - 1, axis=along
    )
    zero_shape = list(grid_field.shape)
    zero_shape[along] = 1
    zero_rim = jnp.zeros(zero_shape, grid_field.dtype)
    ahead = jnp.concatenate([forward_diff, zero_rim], axis=along)
    behind = jnp.concatenate([zero_rim, forward_diff], axis=along)
    return ahead - behind


def line_solve(line_rows, inverses):
    block_count, block_cells, _ = inverses.shape
    line_count = line_rows.shape[0]
    blocks = line_rows.reshape(line_count, block_count, block_cells)
    products = jnp.einsum("rkb,kcb->rkc", blocks, inverses, precision=lax.Precision.HIGHEST)
    first_col = inverses[:, :, 0]
    last_col = inverses[:, :, block_cells - 1]
    incoming = [jnp.zeros((line_count,), line_rows.dtype)]
    for block_index in range(block_count - 1):
        incoming.append(
            products[:, block_index, block_cells - 1]
            + COUPLE * incoming[block_index] * inverses[block_index, block_cells - 1, 0]
        )
    inflow = jnp.stack(incoming, axis=1)
    forward = products + COUPLE * inflow[:, :, None] * first_col[None]
    head_terms = [jnp.zeros((line_count,), line_rows.dtype) for block_index in range(block_count)]
    carried = forward[:, block_count - 1, 0]
    for block_index in range(block_count - 2, -1, -1):
        head_terms[block_index] = carried
        carried = (
            forward[:, block_index, 0]
            + COUPLE * carried * inverses[block_index, 0, block_cells - 1]
        )
    outflow = jnp.stack(head_terms, axis=1)
    solved = forward + COUPLE * outflow[:, :, None] * last_col[None]
    return solved.reshape(line_count, block_count * block_cells)


def local_turned(energy, damage_old, crack_seeds, irreversible, line_inverses, z_inverse):
    planes, rows_here, line_length = energy.shape
    row_count = lax.axis_size("row")
    col_count = lax.axis_size("col")
    total_planes = planes * col_count
    cell_count = total_planes * rows_here * row_count * line_length
    seeded = crack_seeds == 1
    damage = jnp.where(seeded, 1.0, damage_old)
    lower_bound = jnp.where(irreversible == 1, damage_old, 0.0)
    own_sums = []
    for sweep_index in range(ITERS):
        local_lap = second_difference(damage, 2)
        partial_value = energy - (1.0 + energy) * damage + KAPPA * local_lap
        moved_part, moved_damage = (
            lax.all_to_all(
                lax.all_to_all(
                    jnp.swapaxes(partial_value, 1, 2),
                    "row",
                    split_axis=1,
                    concat_axis=2,
                    tiled=True,
                ),
                "col",
                split_axis=1,
                concat_axis=0,
                tiled=True,
            ),
            lax.all_to_all(
                lax.all_to_all(
                    jnp.swapaxes(damage, 1, 2), "row", split_axis=1, concat_axis=2, tiled=True
                ),
                "col",
                split_axis=1,
                concat_axis=0,
                tiled=True,
            ),
        )
        lap_rest = second_difference(moved_damage, 2) + second_difference(moved_damage, 0)
        turned = moved_part + KAPPA * lap_rest
        turned_shape = turned.shape
        along_y = line_solve(turned.reshape(-1, turned_shape[2]), line_inverses).reshape(
            turned_shape
        )
        along_z = jnp.einsum("zk,kxy->zxy", z_inverse, along_y, precision=lax.Precision.HIGHEST)
        gathered = lax.all_to_all(
            lax.all_to_all(along_z, "row", split_axis=2, concat_axis=1, tiled=True),
            "col",
            split_axis=0,
            concat_axis=1,
            tiled=True,
        )
        piece_cells = gathered.shape[1] // (row_count * col_count)
        reordered = gathered.reshape(planes, col_count, row_count, piece_cells, rows_here)
        restored = jnp.transpose(reordered, (0, 4, 2, 1, 3)).reshape(planes, rows_here, line_length)
        update = STEP * line_solve(restored.reshape(-1, line_length), line_inverses).reshape(
            restored.shape
        )
        clamped = jnp.minimum(jnp.maximum(damage + update, lower_bound), 1.0)
        renewed = jnp.where(seeded, 1.0, clamped)
        own_sum = jnp.sum((renewed - damage) ** 2)
        own_sums.append(own_sum)
        damage = renewed
    global_sums = lax.psum(jnp.stack(own_sums), ("row", "col"))
    update_norms = jnp.sqrt(global_sums / cell_count + EPSILON) / STEP
    return (damage, update_norms)


def line_kernel(
    shape,
    z_inv,
    energy,
    damage_hbm,
    seeds_hbm,
    irreversible_hbm,
    inverses,
    out,
    norms,
    damage_old,
    crack_seeds,
    irreversible,
    start,
    bound,
    ez,
    fz,
    landing,
    dz,
    final,
    w_high,
    w_low,
    a_high,
    a_low,
    mix,
    corner,
    gx,
    gy,
    gx_high,
    gx_low,
    gy_both,
    gy_ends,
    gend,
    wx_send,
    wx_in,
    wx_own,
    wy_in,
    wy_turn,
    carry_rows,
    own_rows,
    y_base,
    x_send,
    x_all,
    y_send,
    y_all,
    s_send,
    s_row,
    s_col_send,
    s_col,
    local_sems,
    e_ssem,
    e_rsem,
    d_ssem,
    d_rsem,
    f_ssem,
    f_rsem,
    back_ssem,
    back_rsem,
    x_ssem,
    x_rsem,
    v_ssem,
    v_rsem,
    y_ssem,
    y_rsem,
    sc_ssem,
    sc_rsem,
    sr_ssem,
    sr_rsem,
):
    rows, cols, cells, width, x_blocks, blocks, cell_count, cuts, backs_at = shape
    planes = cols
    last = cells - 1
    groups = width // 128
    kinds = 2 * x_blocks + 2
    f32 = jnp.float32
    row, col = lax.axis_index("row"), lax.axis_index("col")
    row_peers = [lax.rem(row + o, rows) for o in range(1, rows)]
    col_peers = [lax.rem(col + o, cols) for o in range(1, cols)]

    def slab(who):
        return pl.ds(pl.multiple_of(who * width, width), width)

    def eight(at):
        return pl.ds(pl.multiple_of(at, 8), 8)

    def send(src, dst, ssem, rsem, **where):
        copy = pltpu.make_async_remote_copy(
            src_ref=src, dst_ref=dst, send_sem=ssem, recv_sem=rsem,
            device_id=where, device_id_type=pl.DeviceIdType.MESH,
        )
        copy.start()
        return copy

    def finish(sent):
        for copy in sent:
            copy.wait()

    def split(a):
        high = a.astype(jnp.bfloat16)
        return high, (a - high.astype(f32)).astype(jnp.bfloat16)

    def dot(a, b):
        return jnp.dot(a, b, preferred_element_type=f32)

    def line_ends(field):
        tile_lane = lax.broadcasted_iota(jnp.int32, (cells, 128), 1)
        packed = field[:, :128]
        for j in range(x_blocks):
            begin = field[:, j * cells : j * cells + 128]
            end = field[:, (j + 1) * cells - 128 : (j + 1) * cells]
            if j > 0:
                begin = pltpu.roll(begin, j, 1)
                packed = jnp.where(tile_lane == j, begin, packed)
            end = pltpu.roll(end, x_blocks + j + 1, 1)
            packed = jnp.where(tile_lane == x_blocks + j, end, packed)
        return packed.T[:8]

    barrier = pltpu.get_barrier_semaphore()
    for peer in col_peers:
        pl.semaphore_signal(
            barrier, inc=1, device_id={"col": peer}, device_id_type=pl.DeviceIdType.MESH
        )
    for peer in row_peers:
        pl.semaphore_signal(
            barrier, inc=1, device_id={"row": peer}, device_id_type=pl.DeviceIdType.MESH
        )

    pulls = [
        pltpu.make_async_copy(damage_hbm, damage_old, local_sems.at[0]),
        pltpu.make_async_copy(seeds_hbm, crack_seeds, local_sems.at[1]),
        pltpu.make_async_copy(irreversible_hbm, irreversible, local_sems.at[2]),
    ]
    fetch = [
        pltpu.make_async_copy(energy.at[:, slab(col)], ez.at[col], local_sems.at[3]),
        pltpu.make_async_copy(inverses.at[row], gy, local_sems.at[4]),
    ]
    for n in range(4):
        down, over = (cells - 8) * (n // 2), (cells - 128) * (n % 2)
        fetch.append(
            pltpu.make_async_copy(
                inverses.at[:, pl.ds(down, 8), pl.ds(over, 128)], corner.at[n], local_sems.at[5 + n]
            )
        )
    for j in range(x_blocks):
        fetch.append(
            pltpu.make_async_copy(inverses.at[col * x_blocks + j], gx.at[j], local_sems.at[9 + j])
        )
    for copy in pulls + fetch:
        copy.start()
    pl.semaphore_wait(barrier, rows + cols - 2)

    def move_piece(src, target, index, ssem, rsem):
        at = pl.ds(cuts[index], cuts[index + 1] - cuts[index])
        return [
            send(src.at[at, slab(peer)], target.at[col, at, :], ssem.at[index, n],
                 rsem.at[index, n], col=peer)
            for n, peer in enumerate(col_peers)
        ]

    moved_e = [
        send(energy.at[:, slab(peer)], ez.at[col], e_ssem.at[n], e_rsem.at[n], col=peer)
        for n, peer in enumerate(col_peers)
    ]
    finish(pulls)

    @pl.loop(0, cells // 16)
    def _(i):
        at = pl.ds(pl.multiple_of(i * 16, 16), 16)
        old = damage_old[at, :]
        seeded = crack_seeds[at, :] == 1
        start[at, :] = jnp.where(seeded, 1.0, old)
        bound[at, :] = jnp.where(seeded, 1.0, jnp.where(irreversible[at, :] == 1, old, 0.0))

    order = (0, 3, 1, 2)
    moved_d = {n: move_piece(start, landing, n, d_ssem, d_rsem) for n in order}
    moved_f = {n: move_piece(bound, fz, n, f_ssem, f_rsem) for n in order[:2]}
    landing[col] = start[:, slab(col)]
    fz[col] = bound[:, slab(col)]

    lane = lax.broadcasted_iota(jnp.int32, (8, 128), 1)
    sub = lax.broadcasted_iota(jnp.int32, (8, 128), 0)
    upper_half = sub < planes
    zero = jnp.zeros((8, 128), f32)
    finish(fetch)

    def lane_of(a, n):
        return jnp.broadcast_to(a[:, n : n + 1], (8, 128))

    def corner_of(down, over, k):
        tile = corner[2 * down + over, k]
        at = (7 if down else 0, 127 if over else 0)
        return jnp.broadcast_to(tile[at[0] : at[0] + 1, at[1] : at[1] + 1], (8, 128))

    def hot(index):
        return jnp.where(lane == index, 1.0, 0.0)

    def carries(first, final_of, lower=None, upper=None):
        firsts, finals = [], []
        low = [None if lower is None else lower(k) for k in range(blocks)]
        high = [None if upper is None else upper(k) for k in range(blocks)]
        for k in range(blocks):
            begin, end = hot(first(k)), hot(final_of(k))
            if low[k] is not None:
                begin = begin + corner_of(0, 0, k) * hot(low[k])
                end = end + corner_of(1, 0, k) * hot(low[k])
            if high[k] is not None:
                begin = begin + corner_of(0, 1, k) * hot(high[k])
                end = end + corner_of(1, 1, k) * hot(high[k])
            firsts.append(begin)
            finals.append(end)
        incoming = [zero]
        for k in range(blocks - 1):
            incoming.append(finals[k] + COUPLE * corner_of(1, 0, k) * incoming[k])
        heads = [
            firsts[k] + COUPLE * corner_of(0, 0, k) * incoming[k] for k in range(blocks)
        ]
        carried = heads[blocks - 1]
        outgoing = [zero] * blocks
        for k in range(blocks - 2, -1, -1):
            outgoing[k] = carried
            carried = heads[k] + COUPLE * corner_of(0, 1, k) * carried
        enter, leave = [], []
        for k in range(blocks):
            enter.append(COUPLE * incoming[k] + (zero if low[k] is None else hot(low[k])))
            leave.append(COUPLE * outgoing[k] + (zero if high[k] is None else hot(high[k])))
        return incoming, outgoing, enter, leave

    def picked(which, options):
        total = zero
        for n, option in enumerate(options):
            if option is not None:
                total = total + jnp.where(which == n, option, 0.0)
        return total

    def at_own(c, weights):
        return pltpu.roll(weights, 128 - 8 * c, 1) if c > 0 else weights

    def left_of(k):
        c = k // x_blocks
        return 8 * (c - 1) + 2 * x_blocks + 1 if k % x_blocks == 0 and c > 0 else None

    def right_of(k):
        c = k // x_blocks
        return 8 * (c + 1) + 2 * x_blocks if k % x_blocks == x_blocks - 1 and c < cols - 1 else None

    incoming, outgoing, enter, leave = carries(
        lambda k: 8 * (k // x_blocks) + k % x_blocks,
        lambda k: 8 * (k // x_blocks) + x_blocks + k % x_blocks,
        left_of,
        right_of,
    )
    to_right = picked(col, [
        at_own(c, incoming[(c + 1) * x_blocks] + hot(8 * c + 2 * x_blocks + 1) / COUPLE)
        if c < cols - 1 else None
        for c in range(cols)
    ])
    to_left = picked(col, [
        at_own(c, leave[c * x_blocks - 1] / COUPLE) if c > 0 else None for c in range(cols)
    ])
    for n in range(kinds):
        wx_send[n] = jnp.where(upper_half, lane_of(to_right, n), lane_of(to_left, n))
    for m in range(2 * x_blocks):
        table = (enter, leave)[m % 2]
        everywhere = picked(col, [table[c * x_blocks + m // 2] for c in range(cols)])
        here = picked(col, [at_own(c, table[c * x_blocks + m // 2]) for c in range(cols)])
        for c in range(cols):
            from_left = jnp.where(col > c, lane_of(everywhere, 8 * c + 2 * x_blocks - 1), 0.0)
            from_right = jnp.where(col < c, lane_of(everywhere, 8 * c), 0.0)
            wx_in[m, c] = jnp.where(upper_half, from_left, from_right)
        for n in range(kinds):
            wx_own[m, n] = lane_of(here, n)

    incoming, outgoing, enter, leave = carries(lambda k: 2 * k, lambda k: 2 * k + 1)
    enters, leaves = picked(row, enter), picked(row, leave)
    for k in range(rows):
        wy_in[0, k] = lane_of(enters, 2 * k + 1)
        wy_in[1, k] = jnp.where(row >= k, lane_of(leaves, 2 * k + 1), lane_of(leaves, 2 * k))
    wy_turn[...] = picked(
        row, [lane_of(outgoing[k - 1], 2 * k + 1) if k > 0 else None for k in range(rows)]
    )

    upper_wide = lax.broadcasted_iota(jnp.int32, (8, cells), 0) < planes
    for j in range(x_blocks):
        turned = gx[j].T
        gx_high[j], gx_low[j] = split(turned)
        for side, at in ((0, 0), (1, last)):
            line = jnp.broadcast_to(turned[at : at + 1], (8, cells))
            gend[side, j] = line
            if j == 0:
                gend[side, x_blocks] = line
            else:
                gend[side, x_blocks] = jnp.where(upper_wide, gend[side, x_blocks], line)
    gy_both[:cells], gy_both[cells:] = split(gy[...])
    gy_ends[0] = jnp.broadcast_to(gy[:, :1], (cells, 128))
    gy_ends[1] = jnp.broadcast_to(gy[:, last:], (cells, 128))

    first_col = jnp.where(col == 0, 1.0, 0.0)
    last_col = jnp.where(col == cols - 1, 1.0, 0.0)
    lane16 = lax.broadcasted_iota(jnp.int32, (16, 128), 1)
    at_first, at_last = lane16 == 0, lane16 == 127

    def regroup(low, high):
        @pl.loop(low // 8, high // 8)
        def _(i):
            for z in range(planes):
                tile = landing[z, eight(i * 8), :]
                for g in range(groups):
                    dz[0, z, g, eight(i * 8 + 8), :] = tile[:, g * 128 : (g + 1) * 128]

    def share_rows(it):
        return [
            send(dz.at[it, :, :, pl.ds(cells, 8), :], dz.at[it, :, :, pl.ds(0, 8), :],
                 v_ssem.at[it, 0], v_rsem.at[it, 0], row=lax.rem(row + 1, rows)),
            send(dz.at[it, :, :, pl.ds(8, 8), :], dz.at[it, :, :, pl.ds(cells + 8, 8), :],
                 v_ssem.at[it, 1], v_rsem.at[it, 1], row=lax.rem(row + rows - 1, rows)),
        ]

    def mirror(it):
        for z in range(planes):
            for g in range(groups):
                dz[it, z, g, 7:8, :] = jnp.where(
                    row == 0, dz[it, z, g, 8:9, :], dz[it, z, g, 7:8, :]
                )
                dz[it, z, g, cells + 8 : cells + 9, :] = jnp.where(
                    row == rows - 1,
                    dz[it, z, g, cells + 7 : cells + 8, :],
                    dz[it, z, g, cells + 8 : cells + 9, :],
                )

    def residual(it, low, high):
        @pl.loop(low // 16, high // 16)
        def _(i):
            base = pl.multiple_of(i * 16, 16)
            here = pl.ds(base, 16)
            padded = pl.ds(pl.multiple_of(base + 8, 8), 16)
            for g in range(groups):
                lanes = slice(g * 128, (g + 1) * 128)
                mids = [dz[it, z, g, padded, :] for z in range(planes)]
                value = []
                for z in range(planes):
                    d = mids[z]
                    near = dz[it, z, g, pl.ds(base + 7, 16), :] + dz[it, z, g, pl.ds(base + 9, 16), :]
                    before = d * first_col
                    if g > 0:
                        before = pltpu.roll(dz[it, z, g - 1, padded, :], 1, 1)
                    after = d * last_col
                    if g < groups - 1:
                        after = pltpu.roll(dz[it, z, g + 1, padded, :], 127, 1)
                    near = near + jnp.where(at_first, before, pltpu.roll(d, 1, 1))
                    near = near + jnp.where(at_last, after, pltpu.roll(d, 127, 1))
                    sides = 4
                    if z > 0:
                        near = near + mids[z - 1]
                        sides += 1
                    if z < planes - 1:
                        near = near + mids[z + 1]
                        sides += 1
                    e = ez[z, here, lanes]
                    value.append((e - (e + (1.0 + KAPPA * sides)) * d) + KAPPA * near)
                for z in range(planes):
                    total = z_inv[z, 0] * value[0]
                    for k in range(1, planes):
                        total = total + z_inv[z, k] * value[k]
                    w_high[z, here, lanes], w_low[z, here, lanes] = split(total)

    def x_product(ranges):
        for j in range(x_blocks):
            block = slice(j * cells, (j + 1) * cells)
            parts = [(z, low, high) for z in range(planes) for low, high in ranges]
            high_rows = jnp.concatenate([w_high[z, a:b, block] for z, a, b in parts], axis=0)
            low_rows = jnp.concatenate([w_low[z, a:b, block] for z, a, b in parts], axis=0)
            count = high_rows.shape[0]
            twice = dot(jnp.concatenate([high_rows, low_rows], axis=0), gx_high[j])
            along = twice[:count] + (twice[count:] + dot(high_rows, gx_low[j]))
            at = 0
            for z, a, b in parts:
                a_high[z, a:b, block], a_low[z, a:b, block] = split(along[at : at + b - a])
                at += b - a

    def y_times(high, low):
        twice = dot(gy_both[...], high)
        return twice[:cells] + (twice[cells:] + dot(gy_both[:cells], low))

    def y_product():
        for z in range(planes):
            both = y_times(a_high[z], a_low[z])
            mix[z] = both
            turned = line_ends(both)
            for n in range(2 * x_blocks):
                own_rows[n, z : z + 1, :] = turned[n : n + 1]
                own_rows[n, planes + z : planes + z + 1, :] = turned[n : n + 1]
            for side, at in ((0, 0), (1, last)):
                for j in range(x_blocks):
                    n = j * planes + z
                    y_base[side, n : n + 1, :] = both[at : at + 1, j * cells : (j + 1) * cells]

    def edges(it):
        tile_lane = lax.broadcasted_iota(jnp.int32, (cells, 128), 1)
        packed = jnp.zeros((cells, 128), f32)
        for z in range(planes):
            begin = dz[it, z, 0, pl.ds(8, cells), :]
            end = dz[it, z, groups - 1, pl.ds(8, cells), :]
            if z > 0:
                begin = pltpu.roll(begin, z, 1)
            end = pltpu.roll(end, planes + z + 1, 1)
            packed = jnp.where(tile_lane == z, begin, packed)
            packed = jnp.where(tile_lane == planes + z, end, packed)
        turned = y_times(*split(packed)).T
        for z in range(planes):
            for side in range(2):
                total = None
                for k in range(planes):
                    n = side * planes + k
                    term = (KAPPA * z_inv[z, k]) * turned[n : n + 1]
                    total = term if total is None else total + term
                own_rows[2 * x_blocks + side, z : z + 1, :] = total
                own_rows[2 * x_blocks + side, planes + z : planes + z + 1, :] = total

    def wide(weights):
        return jnp.concatenate([weights] * (cells // 128), axis=1)

    def x_share(it):
        total = None
        for n in range(kinds):
            term = wide(wx_send[n]) * own_rows[n]
            total = term if total is None else total + term
        x_send[it] = total
        x_all[it, col] = total
        return [
            send(x_send.at[it], x_all.at[it, col], x_ssem.at[it, n], x_rsem.at[it, n], col=peer)
            for n, peer in enumerate(col_peers)
        ]

    def y_share(it):
        sides = []
        for side in range(2):
            parts = []
            for j in range(x_blocks):
                m = 2 * j + side
                total = wide(wx_in[m, 0]) * x_all[it, 0]
                for c in range(1, cols):
                    total = total + wide(wx_in[m, c]) * x_all[it, c]
                total = total + pltpu.roll(total, planes, 0)
                for n in range(kinds):
                    total = total + wide(wx_own[m, n]) * own_rows[n]
                parts.append(total)
            sides.append(jnp.where(upper_wide, parts[0], parts[1]))
        lines = []
        for side, at in ((0, 0), (1, last)):
            line = y_base[side]
            for n in range(2):
                scale = jnp.broadcast_to(sides[n][:, at : at + 1], (8, cells))
                line = line + scale * gend[n, x_blocks]
            lines.append(line)
        y_send[it, 0] = lines[1]
        y_send[it, 1] = lines[0] + wide(wy_turn[...]) * lines[1]
        y_all[it, row] = lines[1]
        sent = [
            send(y_send.at[it, lax.div(row + n + 1, rows)], y_all.at[it, row], y_ssem.at[it, n],
                 y_rsem.at[it, n], row=peer)
            for n, peer in enumerate(row_peers)
        ]
        stacked = jnp.concatenate(sides + [jnp.zeros((112, cells), f32)], axis=0).T
        for t in range(cells // 8):
            here = slice(t * 8, t * 8 + 8)
            tile = stacked[here]
            for z in range(planes):
                for j in range(x_blocks):
                    block = slice(j * cells, (j + 1) * cells)
                    n = j * planes + z
                    mix[z, here, block] = (
                        mix[z, here, block]
                        + tile[:, n : n + 1] * gend[0, j]
                        + tile[:, 8 + n : 9 + n] * gend[1, j]
                    )
        finish(sent)
        for side in range(2):
            total = wide(wy_in[side, 0]) * y_all[it, 0]
            for k in range(1, rows):
                total = total + wide(wy_in[side, k]) * y_all[it, k]
            for z in range(planes):
                for j in range(x_blocks):
                    n = j * planes + z
                    carry_rows[2 * z + side, :, j * cells : (j + 1) * cells] = jnp.broadcast_to(
                        total[n : n + 1], (8, cells)
                    )

    def settle(it, low, high, squares):
        def step(i, acc):
            here, padded = eight(i * 8), eight(i * 8 + 8)
            g_first = jnp.concatenate([gy_ends[0, here, :]] * groups, axis=1)
            g_last = jnp.concatenate([gy_ends[1, here, :]] * groups, axis=1)
            for z in range(planes):
                solved = mix[z, here, :] + g_first * carry_rows[2 * z] + g_last * carry_rows[2 * z + 1]
                d = jnp.concatenate([dz[it, z, g, padded, :] for g in range(groups)], axis=1)
                renewed = jnp.minimum(jnp.maximum(d + STEP * solved, fz[z, here, :]), 1.0)
                if it + 1 < ITERS:
                    for g in range(groups):
                        dz[it + 1, z, g, padded, :] = renewed[:, g * 128 : (g + 1) * 128]
                else:
                    final[z, here, :] = renewed
                change = renewed - d
                acc = acc + change * change
            return acc

        return lax.fori_loop(low // 8, high // 8, step, squares)

    def stream(it, ready):
        ready(0)
        ready(3)
        shared = share_rows(it)
        residual(it, 16, cuts[1] - 16)
        residual(it, cuts[3] + 16, cells - 16)
        ready(1)
        residual(it, cuts[1] - 16, cuts[2] - 16)
        x_product([(16, cuts[2] - 16), (cuts[3] + 16, cells - 16)])
        ready(2)
        residual(it, cuts[2] - 16, cuts[3] + 16)
        finish(shared)
        mirror(it)
        residual(it, 0, 16)
        residual(it, cells - 16, cells)
        x_product([(0, 16), (cuts[2] - 16, cuts[3] + 16), (cells - 16, cells)])
        edges(it)
        y_product()

    def arrived(n):
        finish(moved_d[n])
        regroup(cuts[n], cuts[n + 1])

    finish(moved_e)
    stream(0, arrived)
    sent = x_share(0)
    for n in order[2:]:
        moved_f[n] = move_piece(bound, fz, n, f_ssem, f_rsem)
    finish(sent)
    y_share(0)

    totals = []
    blank = jnp.zeros((8, width), f32)
    held = [blank]

    def settled(n):
        finish(moved_f[n])
        held.append(settle(0, cuts[n], cuts[n + 1], held.pop()))

    stream(1, settled)
    sent = x_share(1)
    totals.append(jnp.sum(held[0]))
    finish(sent)
    y_share(1)

    def give_back(n):
        at = pl.ds(backs_at[n], backs_at[n + 1] - backs_at[n])
        return [
            send(final.at[peer, at, :], out.at[at, slab(col)], back_ssem.at[n, m],
                 back_rsem.at[n, m], col=peer)
            for m, peer in enumerate(col_peers)
        ]

    squares = blank
    backs = []
    for n in range(len(backs_at) - 1):
        squares = settle(ITERS - 1, backs_at[n], backs_at[n + 1], squares)
        if n < 2:
            backs += give_back(n)
    totals.append(jnp.sum(squares))
    s_send[...] = jnp.where(sub == 0, totals[0], jnp.where(sub == 1, totals[1], 0.0))
    shares = [
        send(s_send, s_row.at[n], sr_ssem.at[n], sr_rsem.at[n], row=peer)
        for n, peer in enumerate(row_peers)
    ]
    out[:, slab(col)] = final[col]
    finish(shares)
    total = s_send[...]
    for n in range(rows - 1):
        total = total + s_row[n]
    s_col_send[...] = total
    shares = [
        send(s_col_send, s_col.at[n], sc_ssem.at[n], sc_rsem.at[n], col=peer)
        for n, peer in enumerate(col_peers)
    ]
    for n in range(2, len(backs_at) - 1):
        backs += give_back(n)
    finish(shares)
    for n in range(cols - 1):
        total = total + s_col[n]
    sizes = jnp.sqrt(total / cell_count + EPSILON) / STEP
    for n in range(ITERS):
        norms[n] = sizes[n, 0]
    finish(backs)


def local(energy, damage_old, crack_seeds, irreversible, line_inverses, z_inverse):
    planes, cells, line_length = energy.shape
    rows, cols = lax.axis_size("row"), lax.axis_size("col")
    blocks, _, _ = line_inverses.shape
    width = line_length // cols
    x_blocks = width // cells
    kinds = 2 * x_blocks + 2
    pieces = 4
    step = cells // 16
    cuts = (0, 3 * step, 11 * step, 13 * step, cells)
    backs_at = tuple(cells * n // pieces for n in range(pieces + 1))
    cell_count = float(cols * rows * cells * line_length)
    shape = (rows, cols, cells, width, x_blocks, blocks, cell_count, cuts, backs_at)
    f32 = jnp.float32
    bf16 = jnp.bfloat16
    dma = pltpu.SemaphoreType.DMA
    vmem = pl.BlockSpec(memory_space=pltpu.VMEM)
    smem = pl.BlockSpec(memory_space=pltpu.SMEM)
    damage, norms = pl.pallas_call(
        functools.partial(line_kernel, shape),
        out_shape=(
            pltpu.VMEM((cells, line_length), f32),
            jax.ShapeDtypeStruct((ITERS,), f32),
        ),
        in_specs=[smem] + [pl.BlockSpec(memory_space=pl.ANY)] * 5,
        out_specs=(vmem, smem),
        scratch_shapes=[
            pltpu.VMEM((cells, line_length), f32),
            pltpu.VMEM((cells, line_length), jnp.int32),
            pltpu.VMEM((cells, line_length), jnp.int32),
            pltpu.VMEM((cells, line_length), f32),
            pltpu.VMEM((cells, line_length), f32),
            pltpu.VMEM((cols, cells, width), f32),
            pltpu.VMEM((cols, cells, width), f32),
            pltpu.VMEM((cols, cells, width), f32),
            pltpu.VMEM((ITERS, cols, width // 128, cells + 16, 128), f32),
            pltpu.VMEM((cols, cells, width), f32),
            pltpu.VMEM((cols, cells, width), bf16),
            pltpu.VMEM((cols, cells, width), bf16),
            pltpu.VMEM((cols, cells, width), bf16),
            pltpu.VMEM((cols, cells, width), bf16),
            pltpu.VMEM((cols, cells, width), f32),
            pltpu.VMEM((4, blocks, 8, 128), f32),
            pltpu.VMEM((x_blocks, cells, cells), f32),
            pltpu.VMEM((cells, cells), f32),
            pltpu.VMEM((x_blocks, cells, cells), bf16),
            pltpu.VMEM((x_blocks, cells, cells), bf16),
            pltpu.VMEM((2 * cells, cells), bf16),
            pltpu.VMEM((2, cells, 128), f32),
            pltpu.VMEM((2, x_blocks + 1, 8, cells), f32),
            pltpu.VMEM((kinds, 8, 128), f32),
            pltpu.VMEM((2 * x_blocks, cols, 8, 128), f32),
            pltpu.VMEM((2 * x_blocks, kinds, 8, 128), f32),
            pltpu.VMEM((2, rows, 8, 128), f32),
            pltpu.VMEM((8, 128), f32),
            pltpu.VMEM((2 * cols, 8, width), f32),
            pltpu.VMEM((kinds, 8, cells), f32),
            pltpu.VMEM((2, 8, cells), f32),
            pltpu.VMEM((ITERS, 8, cells), f32),
            pltpu.VMEM((ITERS, cols, 8, cells), f32),
            pltpu.VMEM((ITERS, 2, 8, cells), f32),
            pltpu.VMEM((ITERS, rows, 8, cells), f32),
            pltpu.VMEM((8, 128), f32),
            pltpu.VMEM((rows - 1, 8, 128), f32),
            pltpu.VMEM((8, 128), f32),
            pltpu.VMEM((cols - 1, 8, 128), f32),
            dma((x_blocks + 9,)),
            dma((cols - 1,)),
            dma((cols - 1,)),
            dma((pieces, cols - 1)),
            dma((pieces, cols - 1)),
            dma((pieces, cols - 1)),
            dma((pieces, cols - 1)),
            dma((pieces, cols - 1)),
            dma((pieces, cols - 1)),
            dma((ITERS, cols - 1)),
            dma((ITERS, cols - 1)),
            dma((ITERS, 2)),
            dma((ITERS, 2)),
            dma((ITERS, rows - 1)),
            dma((ITERS, rows - 1)),
            dma((cols - 1,)),
            dma((cols - 1,)),
            dma((rows - 1,)),
            dma((rows - 1,)),
        ],
        compiler_params=pltpu.CompilerParams(
            has_side_effects=True, collective_id=0, vmem_limit_bytes=60 * 1024 * 1024
        ),
        name="line_iterations",
    )(
        z_inverse,
        energy[0],
        damage_old[0],
        crack_seeds[0],
        irreversible[0],
        line_inverses,
    )
    return damage[None], norms


def solution(mesh):
    def local_any(energy, damage_old, crack_seeds, irreversible, line_inverses, z_inverse):
        rows, cols = mesh.shape["row"], mesh.shape["col"]
        block_cells = line_inverses.shape[1]
        width = energy.shape[2] // cols
        whole_blocks = (
            energy.shape[0] == 1
            and energy.shape[1] == block_cells
            and width == 2 * block_cells
            and block_cells % 256 == 0
            and 2 * cols == 8
            and 2 * rows <= 128
            and min(rows, cols) > 2
        )
        chosen = local if whole_blocks else local_turned
        return chosen(energy, damage_old, crack_seeds, irreversible, line_inverses, z_inverse)

    return jax.shard_map(
        local_any,
        mesh=mesh,
        in_specs=(
            P("col", "row", None),
            P("col", "row", None),
            P("col", "row", None),
            P("col", "row", None),
            P(),
            P(),
        ),
        out_specs=(P("col", "row", None), P()),
        check_vma=False,
    )
```

```python
import functools

import jax
import jax.numpy as jnp
from jax import lax
from jax.experimental import pallas as pl
from jax.experimental.pallas import tpu as pltpu
from jax.sharding import PartitionSpec as P

ITERS = 2


KAPPA = 2.0
STEP = 0.02
COUPLE = 0.5
EPSILON = 1e-06
HIGHEST = lax.Precision.HIGHEST


def second_difference(grid_field, along):
    extent = grid_field.shape[along]
    forward_diff = lax.slice_in_dim(grid_field, 1, extent, axis=along) - lax.slice_in_dim(
        grid_field, 0, extent - 1, axis=along
    )
    zero_shape = list(grid_field.shape)
    zero_shape[along] = 1
    zero_rim = jnp.zeros(zero_shape, grid_field.dtype)
    ahead = jnp.concatenate([forward_diff, zero_rim], axis=along)
    behind = jnp.concatenate([zero_rim, forward_diff], axis=along)
    return ahead - behind


def line_solve(line_rows, inverses):
    block_count, block_cells, _ = inverses.shape
    line_count = line_rows.shape[0]
    blocks = line_rows.reshape(line_count, block_count, block_cells)
    products = jnp.einsum("rkb,kcb->rkc", blocks, inverses, precision=lax.Precision.HIGHEST)
    first_col = inverses[:, :, 0]
    last_col = inverses[:, :, block_cells - 1]
    incoming = [jnp.zeros((line_count,), line_rows.dtype)]
    for block_index in range(block_count - 1):
        incoming.append(
            products[:, block_index, block_cells - 1]
            + COUPLE * incoming[block_index] * inverses[block_index, block_cells - 1, 0]
        )
    inflow = jnp.stack(incoming, axis=1)
    forward = products + COUPLE * inflow[:, :, None] * first_col[None]
    head_terms = [jnp.zeros((line_count,), line_rows.dtype) for block_index in range(block_count)]
    carried = forward[:, block_count - 1, 0]
    for block_index in range(block_count - 2, -1, -1):
        head_terms[block_index] = carried
        carried = (
            forward[:, block_index, 0]
            + COUPLE * carried * inverses[block_index, 0, block_cells - 1]
        )
    outflow = jnp.stack(head_terms, axis=1)
    solved = forward + COUPLE * outflow[:, :, None] * last_col[None]
    return solved.reshape(line_count, block_count * block_cells)


def local_turned(energy, damage_old, crack_seeds, irreversible, line_inverses, z_inverse):
    planes, rows_here, line_length = energy.shape
    row_count = lax.axis_size("row")
    col_count = lax.axis_size("col")
    total_planes = planes * col_count
    cell_count = total_planes * rows_here * row_count * line_length
    seeded = crack_seeds == 1
    damage = jnp.where(seeded, 1.0, damage_old)
    lower_bound = jnp.where(irreversible == 1, damage_old, 0.0)
    own_sums = []
    for sweep_index in range(ITERS):
        local_lap = second_difference(damage, 2)
        partial_value = energy - (1.0 + energy) * damage + KAPPA * local_lap
        moved_part, moved_damage = (
            lax.all_to_all(
                lax.all_to_all(
                    jnp.swapaxes(partial_value, 1, 2),
                    "row",
                    split_axis=1,
                    concat_axis=2,
                    tiled=True,
                ),
                "col",
                split_axis=1,
                concat_axis=0,
                tiled=True,
            ),
            lax.all_to_all(
                lax.all_to_all(
                    jnp.swapaxes(damage, 1, 2), "row", split_axis=1, concat_axis=2, tiled=True
                ),
                "col",
                split_axis=1,
                concat_axis=0,
                tiled=True,
            ),
        )
        lap_rest = second_difference(moved_damage, 2) + second_difference(moved_damage, 0)
        turned = moved_part + KAPPA * lap_rest
        turned_shape = turned.shape
        along_y = line_solve(turned.reshape(-1, turned_shape[2]), line_inverses).reshape(
            turned_shape
        )
        along_z = jnp.einsum("zk,kxy->zxy", z_inverse, along_y, precision=lax.Precision.HIGHEST)
        gathered = lax.all_to_all(
            lax.all_to_all(along_z, "row", split_axis=2, concat_axis=1, tiled=True),
            "col",
            split_axis=0,
            concat_axis=1,
            tiled=True,
        )
        piece_cells = gathered.shape[1] // (row_count * col_count)
        reordered = gathered.reshape(planes, col_count, row_count, piece_cells, rows_here)
        restored = jnp.transpose(reordered, (0, 4, 2, 1, 3)).reshape(planes, rows_here, line_length)
        update = STEP * line_solve(restored.reshape(-1, line_length), line_inverses).reshape(
            restored.shape
        )
        clamped = jnp.minimum(jnp.maximum(damage + update, lower_bound), 1.0)
        renewed = jnp.where(seeded, 1.0, clamped)
        own_sum = jnp.sum((renewed - damage) ** 2)
        own_sums.append(own_sum)
        damage = renewed
    global_sums = lax.psum(jnp.stack(own_sums), ("row", "col"))
    update_norms = jnp.sqrt(global_sums / cell_count + EPSILON) / STEP
    return (damage, update_norms)


def line_kernel(
    shape,
    z_hbm,
    energy,
    damage_hbm,
    seeds_hbm,
    irreversible_hbm,
    inverses,
    out,
    norms,
    damage_old,
    crack_seeds,
    irreversible,
    start,
    bound,
    ez,
    ec,
    fz,
    landing,
    dz,
    final,
    w_high,
    w_low,
    a_high,
    a_low,
    mix,
    corner,
    gx,
    gy,
    gx_high,
    gx_low,
    gy_both,
    gy_ends,
    gend,
    wx_send,
    wx_in,
    wx_own,
    wy_in,
    wy_turn,
    carry_rows,
    own_rows,
    packed,
    w_mix,
    y_base,
    x_send,
    x_all,
    y_send,
    y_all,
    s_send,
    s_row,
    s_col_send,
    s_col,
    z_inv,
    local_sems,
    e_ssem,
    e_rsem,
    d_ssem,
    d_rsem,
    f_ssem,
    f_rsem,
    back_ssem,
    back_rsem,
    x_ssem,
    x_rsem,
    v_ssem,
    v_rsem,
    y_ssem,
    y_rsem,
    sc_ssem,
    sc_rsem,
    sr_ssem,
    sr_rsem,
):
    rows, cols, cells, width, x_blocks, blocks, cell_count, cuts, backs_at = shape
    planes = cols
    last = cells - 1
    groups = width // 128
    kinds = 2 * x_blocks + 2
    f32 = jnp.float32
    row, col = lax.axis_index("row"), lax.axis_index("col")
    row_peers = [lax.rem(row + o, rows) for o in range(1, rows)]
    col_peers = [lax.rem(col + o, cols) for o in range(1, cols)]

    def slab(who):
        return pl.ds(pl.multiple_of(who * width, width), width)

    def eight(at):
        return pl.ds(pl.multiple_of(at, 8), 8)

    def send(src, dst, ssem, rsem, **where):
        copy = pltpu.make_async_remote_copy(
            src_ref=src, dst_ref=dst, send_sem=ssem, recv_sem=rsem,
            device_id=where, device_id_type=pl.DeviceIdType.MESH,
        )
        copy.start()
        return copy

    def finish(sent):
        for copy in sent:
            copy.wait()

    def split(a):
        high = a.astype(jnp.bfloat16)
        return high, (a - high.astype(f32)).astype(jnp.bfloat16)

    def dot(a, b):
        return jnp.dot(a, b, preferred_element_type=f32)

    barrier = pltpu.get_barrier_semaphore()
    for peer in col_peers:
        pl.semaphore_signal(
            barrier, inc=1, device_id={"col": peer}, device_id_type=pl.DeviceIdType.MESH
        )
    for peer in row_peers:
        pl.semaphore_signal(
            barrier, inc=1, device_id={"row": peer}, device_id_type=pl.DeviceIdType.MESH
        )

    pulls = [
        pltpu.make_async_copy(damage_hbm, damage_old, local_sems.at[0]),
        pltpu.make_async_copy(seeds_hbm, crack_seeds, local_sems.at[1]),
        pltpu.make_async_copy(irreversible_hbm, irreversible, local_sems.at[2]),
    ]
    fetch = [
        pltpu.make_async_copy(energy.at[:, slab(col)], ez.at[col], local_sems.at[3]),
        pltpu.make_async_copy(inverses.at[row], gy, local_sems.at[4]),
        pltpu.make_async_copy(z_hbm, z_inv, local_sems.at[9 + x_blocks]),
    ]
    for n in range(4):
        down, over = (cells - 8) * (n // 2), (cells - 128) * (n % 2)
        fetch.append(
            pltpu.make_async_copy(
                inverses.at[:, pl.ds(down, 8), pl.ds(over, 128)], corner.at[n], local_sems.at[5 + n]
            )
        )
    for j in range(x_blocks):
        fetch.append(
            pltpu.make_async_copy(inverses.at[col * x_blocks + j], gx.at[j], local_sems.at[9 + j])
        )
    for copy in pulls + fetch:
        copy.start()
    pl.semaphore_wait(barrier, rows + cols - 2)

    def move_piece(src, target, index, ssem, rsem):
        at = pl.ds(cuts[index], cuts[index + 1] - cuts[index])
        return [
            send(src.at[at, slab(peer)], target.at[col, at, :], ssem.at[index, n],
                 rsem.at[index, n], col=peer)
            for n, peer in enumerate(col_peers)
        ]

    moved_e = [
        send(energy.at[:, slab(peer)], ez.at[col], e_ssem.at[n], e_rsem.at[n], col=peer)
        for n, peer in enumerate(col_peers)
    ]
    finish(pulls)

    @pl.loop(0, cells // 16)
    def _(i):
        at = pl.ds(pl.multiple_of(i * 16, 16), 16)
        old = damage_old[at, :]
        seeded = crack_seeds[at, :] == 1
        start[at, :] = jnp.where(seeded, 1.0, old)
        bound[at, :] = jnp.where(seeded, 1.0, jnp.where(irreversible[at, :] == 1, old, 0.0))

    order = (0, 4, 1, 2, 3)
    moved_d = {n: move_piece(start, landing, n, d_ssem, d_rsem) for n in order}
    moved_f = {n: move_piece(bound, fz, n, f_ssem, f_rsem) for n in order[:2]}
    landing[col] = start[:, slab(col)]
    fz[col] = bound[:, slab(col)]

    lane = lax.broadcasted_iota(jnp.int32, (8, 128), 1)
    sub = lax.broadcasted_iota(jnp.int32, (8, 128), 0)
    upper_half = sub < planes
    zero = jnp.zeros((8, 128), f32)
    finish(fetch)

    def lane_of(a, n):
        return jnp.broadcast_to(a[:, n : n + 1], (8, 128))

    def corner_of(down, over, k):
        tile = corner[2 * down + over, k]
        at = (7 if down else 0, 127 if over else 0)
        return jnp.broadcast_to(tile[at[0] : at[0] + 1, at[1] : at[1] + 1], (8, 128))

    def hot(index):
        return jnp.where(lane == index, 1.0, 0.0)

    def carries(first, final_of, lower=None, upper=None):
        firsts, finals = [], []
        low = [None if lower is None else lower(k) for k in range(blocks)]
        high = [None if upper is None else upper(k) for k in range(blocks)]
        for k in range(blocks):
            begin, end = hot(first(k)), hot(final_of(k))
            if low[k] is not None:
                begin = begin + corner_of(0, 0, k) * hot(low[k])
                end = end + corner_of(1, 0, k) * hot(low[k])
            if high[k] is not None:
                begin = begin + corner_of(0, 1, k) * hot(high[k])
                end = end + corner_of(1, 1, k) * hot(high[k])
            firsts.append(begin)
            finals.append(end)
        incoming = [zero]
        for k in range(blocks - 1):
            incoming.append(finals[k] + COUPLE * corner_of(1, 0, k) * incoming[k])
        heads = [
            firsts[k] + COUPLE * corner_of(0, 0, k) * incoming[k] for k in range(blocks)
        ]
        carried = heads[blocks - 1]
        outgoing = [zero] * blocks
        for k in range(blocks - 2, -1, -1):
            outgoing[k] = carried
            carried = heads[k] + COUPLE * corner_of(0, 1, k) * carried
        enter, leave = [], []
        for k in range(blocks):
            enter.append(COUPLE * incoming[k] + (zero if low[k] is None else hot(low[k])))
            leave.append(COUPLE * outgoing[k] + (zero if high[k] is None else hot(high[k])))
        return incoming, outgoing, enter, leave

    def picked(which, options):
        total = zero
        for n, option in enumerate(options):
            if option is not None:
                total = total + jnp.where(which == n, option, 0.0)
        return total

    def at_own(c, weights):
        return pltpu.roll(weights, 128 - 8 * c, 1) if c > 0 else weights

    def left_of(k):
        c = k // x_blocks
        return 8 * (c - 1) + 2 * x_blocks + 1 if k % x_blocks == 0 and c > 0 else None

    def right_of(k):
        c = k // x_blocks
        return 8 * (c + 1) + 2 * x_blocks if k % x_blocks == x_blocks - 1 and c < cols - 1 else None

    incoming, outgoing, enter, leave = carries(
        lambda k: 8 * (k // x_blocks) + k % x_blocks,
        lambda k: 8 * (k // x_blocks) + x_blocks + k % x_blocks,
        left_of,
        right_of,
    )
    to_right = picked(col, [
        at_own(c, incoming[(c + 1) * x_blocks] + hot(8 * c + 2 * x_blocks + 1) / COUPLE)
        if c < cols - 1 else None
        for c in range(cols)
    ])
    to_left = picked(col, [
        at_own(c, leave[c * x_blocks - 1] / COUPLE) if c > 0 else None for c in range(cols)
    ])
    for n in range(kinds):
        wx_send[n] = jnp.where(upper_half, lane_of(to_right, n), lane_of(to_left, n))
    for m in range(2 * x_blocks):
        table = (enter, leave)[m % 2]
        everywhere = picked(col, [table[c * x_blocks + m // 2] for c in range(cols)])
        here = picked(col, [at_own(c, table[c * x_blocks + m // 2]) for c in range(cols)])
        for c in range(cols):
            from_left = jnp.where(col > c, lane_of(everywhere, 8 * c + 2 * x_blocks - 1), 0.0)
            from_right = jnp.where(col < c, lane_of(everywhere, 8 * c), 0.0)
            wx_in[m, c] = jnp.where(upper_half, from_left, from_right)
        for n in range(kinds):
            wx_own[m, n] = lane_of(here, n)

    incoming, outgoing, enter, leave = carries(lambda k: 2 * k, lambda k: 2 * k + 1)
    enters, leaves = picked(row, enter), picked(row, leave)
    for k in range(rows):
        wy_in[0, k] = lane_of(enters, 2 * k + 1)
        wy_in[1, k] = jnp.where(row >= k, lane_of(leaves, 2 * k + 1), lane_of(leaves, 2 * k))
    wy_turn[...] = picked(
        row, [lane_of(outgoing[k - 1], 2 * k + 1) if k > 0 else None for k in range(rows)]
    )

    upper_wide = lax.broadcasted_iota(jnp.int32, (8, cells), 0) < planes
    for j in range(x_blocks):
        turned = gx[j].T
        gx_high[j], gx_low[j] = split(turned)
        for side, at in ((0, 0), (1, last)):
            line = jnp.broadcast_to(turned[at : at + 1], (8, cells))
            gend[side, j] = line
            if j == 0:
                gend[side, x_blocks] = line
            else:
                gend[side, x_blocks] = jnp.where(upper_wide, gend[side, x_blocks], line)
    gy_both[:cells], gy_both[cells:] = split(gy[...])
    gy_ends[0] = jnp.broadcast_to(gy[:, :1], (cells, 128))
    gy_ends[1] = jnp.broadcast_to(gy[:, last:], (cells, 128))

    first_col = jnp.where(col == 0, 1.0, 0.0)
    last_col = jnp.where(col == cols - 1, 1.0, 0.0)
    lane16 = lax.broadcasted_iota(jnp.int32, (16, 128), 1)
    at_first, at_last = lane16 == 0, lane16 == 127

    mixing = [[KAPPA * z_inv[z, k] for k in range(planes)] for z in range(planes)]
    for k in range(planes):
        weights = zero
        for z in range(planes):
            weights = jnp.where(lax.rem(sub, planes) == z, mixing[z][k], weights)
        w_mix[k] = weights

    def scale_energy():
        @pl.loop(0, cells // 8)
        def _(i):
            for z in range(planes):
                sides = 4 + (z > 0) + (z < planes - 1)
                scaled = ez[z, eight(i * 8), :] * (1.0 / KAPPA)
                ez[z, eight(i * 8), :] = scaled
                ec[z, eight(i * 8), :] = scaled + (1.0 / KAPPA + sides)

    def regroup(low, high):
        @pl.loop(low // 8, high // 8)
        def _(i):
            for z in range(planes):
                tile = landing[z, eight(i * 8), :]
                for g in range(groups):
                    dz[0, z, g, eight(i * 8 + 8), :] = tile[:, g * 128 : (g + 1) * 128]

    def share_rows(it):
        return [
            send(dz.at[it, :, :, pl.ds(cells, 8), :], dz.at[it, :, :, pl.ds(0, 8), :],
                 v_ssem.at[it, 0], v_rsem.at[it, 0], row=lax.rem(row + 1, rows)),
            send(dz.at[it, :, :, pl.ds(8, 8), :], dz.at[it, :, :, pl.ds(cells + 8, 8), :],
                 v_ssem.at[it, 1], v_rsem.at[it, 1], row=lax.rem(row + rows - 1, rows)),
        ]

    def mirror(it):
        for z in range(planes):
            for g in range(groups):
                dz[it, z, g, 7:8, :] = jnp.where(
                    row == 0, dz[it, z, g, 8:9, :], dz[it, z, g, 7:8, :]
                )
                dz[it, z, g, cells + 8 : cells + 9, :] = jnp.where(
                    row == rows - 1,
                    dz[it, z, g, cells + 7 : cells + 8, :],
                    dz[it, z, g, cells + 8 : cells + 9, :],
                )

    def residual(it, low, high):
        @pl.loop(low // 16, high // 16)
        def _(i):
            base = pl.multiple_of(i * 16, 16)
            here = pl.ds(base, 16)
            padded = pl.ds(pl.multiple_of(base + 8, 8), 16)
            for g in range(groups):
                lanes = slice(g * 128, (g + 1) * 128)
                mids = [dz[it, z, g, padded, :] for z in range(planes)]
                value = []
                for z in range(planes):
                    d = mids[z]
                    near = dz[it, z, g, pl.ds(base + 7, 16), :] + dz[it, z, g, pl.ds(base + 9, 16), :]
                    before = d * first_col
                    if g > 0:
                        before = pltpu.roll(dz[it, z, g - 1, padded, :], 1, 1)
                    after = d * last_col
                    if g < groups - 1:
                        after = pltpu.roll(dz[it, z, g + 1, padded, :], 127, 1)
                    near = near + jnp.where(at_first, before, pltpu.roll(d, 1, 1))
                    near = near + jnp.where(at_last, after, pltpu.roll(d, 127, 1))
                    if z > 0:
                        near = near + mids[z - 1]
                    if z < planes - 1:
                        near = near + mids[z + 1]
                    value.append(near + (ez[z, here, lanes] - ec[z, here, lanes] * d))
                for z in range(planes):
                    total = mixing[z][0] * value[0]
                    for k in range(1, planes):
                        total = total + mixing[z][k] * value[k]
                    w_high[z, here, lanes], w_low[z, here, lanes] = split(total)

    def x_product(it, ranges):
        packs = [jnp.zeros((b - a, 128), f32) for a, b in ranges]
        spots = [lax.broadcasted_iota(jnp.int32, (b - a, 128), 1) for a, b in ranges]

        def place(n, tile, lane_from, lane_to):
            if lane_from != lane_to:
                tile = pltpu.roll(tile, (lane_to - lane_from) % 128, 1)
            packs[n] = jnp.where(spots[n] == lane_to, tile, packs[n])

        for j in range(x_blocks):
            block = slice(j * cells, (j + 1) * cells)
            parts = [(z, n) for z in range(planes) for n in range(len(ranges))]
            cut = [slice(*ranges[n]) for _, n in parts]
            high_rows = jnp.concatenate(
                [w_high[z, c, block] for (z, _), c in zip(parts, cut)], axis=0
            )
            low_rows = jnp.concatenate(
                [w_low[z, c, block] for (z, _), c in zip(parts, cut)], axis=0
            )
            count = high_rows.shape[0]
            twice = dot(jnp.concatenate([high_rows, low_rows], axis=0), gx_high[j])
            along = twice[:count] + (twice[count:] + dot(high_rows, gx_low[j]))
            at = 0
            for (z, n), c in zip(parts, cut):
                part = along[at : at + c.stop - c.start]
                at += c.stop - c.start
                a_high[z, c, block], a_low[z, c, block] = split(part)
                place(n, part[:, :128], 0, j * planes + z)
                place(n, part[:, cells - 128 :], 127, (x_blocks + j) * planes + z)
        for n, (a, b) in enumerate(ranges):
            for z in range(planes):
                near = pl.ds(8 + a, b - a)
                place(n, dz[it, z, 0, near, :], 0, 2 * x_blocks * planes + z)
                place(n, dz[it, z, groups - 1, near, :], 127, (2 * x_blocks + 1) * planes + z)
            packed[a:b, :] = packs[n]

    def y_times(high, low):
        twice = dot(gy_both[...], high)
        return twice[:cells] + (twice[cells:] + dot(gy_both[:cells], low))

    def y_product():
        for z in range(planes):
            both = y_times(a_high[z], a_low[z])
            mix[z] = both
            for side, at in ((0, 0), (1, last)):
                for j in range(x_blocks):
                    n = j * planes + z
                    y_base[side, n : n + 1, :] = both[at : at + 1, j * cells : (j + 1) * cells]

    def x_ends():
        turned = y_times(*split(packed[...])).T

        def keep(n, tile):
            other = pltpu.roll(tile, planes, 0)
            pair = (tile, other) if n % 2 == 0 else (other, tile)
            own_rows[n] = jnp.where(upper_wide, pair[0], pair[1])

        for n in range(2 * x_blocks):
            keep(n, turned[8 * (n // 2) : 8 * (n // 2) + 8])
        tile = turned[8 * x_blocks : 8 * x_blocks + 8]
        total = None
        for k in range(planes):
            line = jnp.where(
                upper_wide,
                jnp.broadcast_to(tile[k : k + 1], (8, cells)),
                jnp.broadcast_to(tile[planes + k : planes + k + 1], (8, cells)),
            )
            term = wide(w_mix[k]) * line
            total = term if total is None else total + term
        for n in range(2):
            keep(2 * x_blocks + n, total)

    def wide(weights):
        return jnp.concatenate([weights] * (cells // 128), axis=1)

    def x_share(it):
        total = None
        for n in range(kinds):
            term = wide(wx_send[n]) * own_rows[n]
            total = term if total is None else total + term
        x_send[it] = total
        x_all[it, col] = total
        return [
            send(x_send.at[it], x_all.at[it, col], x_ssem.at[it, n], x_rsem.at[it, n], col=peer)
            for n, peer in enumerate(col_peers)
        ]

    def y_share(it):
        sides = []
        for side in range(2):
            parts = []
            for j in range(x_blocks):
                m = 2 * j + side
                total = wide(wx_in[m, 0]) * x_all[it, 0]
                for c in range(1, cols):
                    total = total + wide(wx_in[m, c]) * x_all[it, c]
                total = total + pltpu.roll(total, planes, 0)
                for n in range(kinds):
                    total = total + wide(wx_own[m, n]) * own_rows[n]
                parts.append(total)
            sides.append(jnp.where(upper_wide, parts[0], parts[1]))
        lines = []
        for side, at in ((0, 0), (1, last)):
            line = y_base[side]
            for n in range(2):
                scale = jnp.broadcast_to(sides[n][:, at : at + 1], (8, cells))
                line = line + scale * gend[n, x_blocks]
            lines.append(line)
        y_send[it, 0] = lines[1]
        y_send[it, 1] = lines[0] + wide(wy_turn[...]) * lines[1]
        y_all[it, row] = lines[1]
        sent = [
            send(y_send.at[it, lax.div(row + n + 1, rows)], y_all.at[it, row], y_ssem.at[it, n],
                 y_rsem.at[it, n], row=peer)
            for n, peer in enumerate(row_peers)
        ]
        stacked = jnp.concatenate(sides + [jnp.zeros((112, cells), f32)], axis=0).T
        for t in range(cells // 8):
            here = slice(t * 8, t * 8 + 8)
            tile = stacked[here]
            for z in range(planes):
                for j in range(x_blocks):
                    block = slice(j * cells, (j + 1) * cells)
                    n = j * planes + z
                    mix[z, here, block] = (
                        mix[z, here, block]
                        + tile[:, n : n + 1] * gend[0, j]
                        + tile[:, 8 + n : 9 + n] * gend[1, j]
                    )
        finish(sent)
        for side in range(2):
            total = wide(wy_in[side, 0]) * y_all[it, 0]
            for k in range(1, rows):
                total = total + wide(wy_in[side, k]) * y_all[it, k]
            for z in range(planes):
                for j in range(x_blocks):
                    n = j * planes + z
                    carry_rows[2 * z + side, :, j * cells : (j + 1) * cells] = jnp.broadcast_to(
                        total[n : n + 1], (8, cells)
                    )

    def settle(it, low, high, squares):
        def step(i, acc):
            here, padded = eight(i * 8), eight(i * 8 + 8)
            g_first = jnp.concatenate([gy_ends[0, here, :]] * groups, axis=1)
            g_last = jnp.concatenate([gy_ends[1, here, :]] * groups, axis=1)
            for z in range(planes):
                solved = mix[z, here, :] + g_first * carry_rows[2 * z] + g_last * carry_rows[2 * z + 1]
                d = jnp.concatenate([dz[it, z, g, padded, :] for g in range(groups)], axis=1)
                renewed = jnp.minimum(jnp.maximum(d + STEP * solved, fz[z, here, :]), 1.0)
                if it + 1 < ITERS:
                    for g in range(groups):
                        dz[it + 1, z, g, padded, :] = renewed[:, g * 128 : (g + 1) * 128]
                else:
                    final[z, here, :] = renewed
                change = renewed - d
                acc = acc + change * change
            return acc

        return lax.fori_loop(low // 8, high // 8, step, squares)

    def stream(it, ready):
        ready(order[0])
        ready(order[1])
        shared = share_rows(it)
        finish(shared)
        mirror(it)
        ranges = [(0, cuts[1] - 16), (cuts[4] + 16, cells)]
        for a, b in ranges:
            residual(it, a, b)
        x_product(it, ranges)
        for n in order[2:]:
            ready(n)
            a, b = cuts[n] - 16, cuts[n + 1] - 16
            if n == order[-1]:
                b += 32
            residual(it, a, b)
            x_product(it, [(a, b)])
        x_ends()

    def arrived(n):
        finish(moved_d[n])
        regroup(cuts[n], cuts[n + 1])

    finish(moved_e)
    scale_energy()
    stream(0, arrived)
    sent = x_share(0)
    for n in order[2:]:
        moved_f[n] = move_piece(bound, fz, n, f_ssem, f_rsem)
    y_product()
    finish(sent)
    y_share(0)

    totals = []
    blank = jnp.zeros((8, width), f32)
    held = [blank]

    def settled(n):
        finish(moved_f[n])
        held.append(settle(0, cuts[n], cuts[n + 1], held.pop()))

    stream(1, settled)
    sent = x_share(1)
    y_product()
    totals.append(jnp.sum(held[0]))
    finish(sent)
    y_share(1)

    def give_back(n):
        at = pl.ds(backs_at[n], backs_at[n + 1] - backs_at[n])
        return [
            send(final.at[peer, at, :], out.at[at, slab(col)], back_ssem.at[n, m],
                 back_rsem.at[n, m], col=peer)
            for m, peer in enumerate(col_peers)
        ]

    squares = blank
    backs = []
    for n in range(len(backs_at) - 1):
        squares = settle(ITERS - 1, backs_at[n], backs_at[n + 1], squares)
        if n < 2:
            backs += give_back(n)
    totals.append(jnp.sum(squares))
    s_send[...] = jnp.where(sub == 0, totals[0], jnp.where(sub == 1, totals[1], 0.0))
    shares = [
        send(s_send, s_row.at[n], sr_ssem.at[n], sr_rsem.at[n], row=peer)
        for n, peer in enumerate(row_peers)
    ]
    out[:, slab(col)] = final[col]
    finish(shares)
    total = s_send[...]
    for n in range(rows - 1):
        total = total + s_row[n]
    s_col_send[...] = total
    shares = [
        send(s_col_send, s_col.at[n], sc_ssem.at[n], sc_rsem.at[n], col=peer)
        for n, peer in enumerate(col_peers)
    ]
    for n in range(2, len(backs_at) - 1):
        backs += give_back(n)
    finish(shares)
    for n in range(cols - 1):
        total = total + s_col[n]
    sizes = jnp.sqrt(total / cell_count + EPSILON) / STEP
    norms[...] = jnp.where(lane == 0, sizes[:1, :], sizes[1:2, :])[0, :ITERS]
    finish(backs)


def local(energy, damage_old, crack_seeds, irreversible, line_inverses, z_inverse):
    planes, cells, line_length = energy.shape
    rows, cols = lax.axis_size("row"), lax.axis_size("col")
    blocks, _, _ = line_inverses.shape
    width = line_length // cols
    x_blocks = width // cells
    kinds = 2 * x_blocks + 2
    pieces = 4
    step = cells // 16
    cuts = (0, 3 * step, 8 * step, 12 * step, 13 * step, cells)
    backs_at = tuple(cells * n // pieces for n in range(pieces + 1))
    cell_count = float(cols * rows * cells * line_length)
    shape = (rows, cols, cells, width, x_blocks, blocks, cell_count, cuts, backs_at)
    f32 = jnp.float32
    bf16 = jnp.bfloat16
    dma = pltpu.SemaphoreType.DMA
    vmem = pl.BlockSpec(memory_space=pltpu.VMEM)
    damage, norms = pl.pallas_call(
        functools.partial(line_kernel, shape),
        out_shape=(
            pltpu.VMEM((cells, line_length), f32),
            pltpu.VMEM((ITERS,), f32),
        ),
        in_specs=[pl.BlockSpec(memory_space=pl.ANY)] * 6,
        out_specs=(vmem, vmem),
        scratch_shapes=[
            pltpu.VMEM((cells, line_length), f32),
            pltpu.VMEM((cells, line_length), jnp.int32),
            pltpu.VMEM((cells, line_length), jnp.int32),
            pltpu.VMEM((cells, line_length), f32),
            pltpu.VMEM((cells, line_length), f32),
            pltpu.VMEM((cols, cells, width), f32),
            pltpu.VMEM((cols, cells, width), f32),
            pltpu.VMEM((cols, cells, width), f32),
            pltpu.VMEM((cols, cells, width), f32),
            pltpu.VMEM((ITERS, cols, width // 128, cells + 16, 128), f32),
            pltpu.VMEM((cols, cells, width), f32),
            pltpu.VMEM((cols, cells, width), bf16),
            pltpu.VMEM((cols, cells, width), bf16),
            pltpu.VMEM((cols, cells, width), bf16),
            pltpu.VMEM((cols, cells, width), bf16),
            pltpu.VMEM((cols, cells, width), f32),
            pltpu.VMEM((4, blocks, 8, 128), f32),
            pltpu.VMEM((x_blocks, cells, cells), f32),
            pltpu.VMEM((cells, cells), f32),
            pltpu.VMEM((x_blocks, cells, cells), bf16),
            pltpu.VMEM((x_blocks, cells, cells), bf16),
            pltpu.VMEM((2 * cells, cells), bf16),
            pltpu.VMEM((2, cells, 128), f32),
            pltpu.VMEM((2, x_blocks + 1, 8, cells), f32),
            pltpu.VMEM((kinds, 8, 128), f32),
            pltpu.VMEM((2 * x_blocks, cols, 8, 128), f32),
            pltpu.VMEM((2 * x_blocks, kinds, 8, 128), f32),
            pltpu.VMEM((2, rows, 8, 128), f32),
            pltpu.VMEM((8, 128), f32),
            pltpu.VMEM((2 * cols, 8, width), f32),
            pltpu.VMEM((kinds, 8, cells), f32),
            pltpu.VMEM((cells, 128), f32),
            pltpu.VMEM((cols, 8, 128), f32),
            pltpu.VMEM((2, 8, cells), f32),
            pltpu.VMEM((ITERS, 8, cells), f32),
            pltpu.VMEM((ITERS, cols, 8, cells), f32),
            pltpu.VMEM((ITERS, 2, 8, cells), f32),
            pltpu.VMEM((ITERS, rows, 8, cells), f32),
            pltpu.VMEM((8, 128), f32),
            pltpu.VMEM((rows - 1, 8, 128), f32),
            pltpu.VMEM((8, 128), f32),
            pltpu.VMEM((cols - 1, 8, 128), f32),
            pltpu.SMEM((cols, cols), f32),
            dma((x_blocks + 10,)),
            dma((cols - 1,)),
            dma((cols - 1,)),
            dma((5, cols - 1)),
            dma((5, cols - 1)),
            dma((5, cols - 1)),
            dma((5, cols - 1)),
            dma((pieces, cols - 1)),
            dma((pieces, cols - 1)),
            dma((ITERS, cols - 1)),
            dma((ITERS, cols - 1)),
            dma((ITERS, 2)),
            dma((ITERS, 2)),
            dma((ITERS, rows - 1)),
            dma((ITERS, rows - 1)),
            dma((cols - 1,)),
            dma((cols - 1,)),
            dma((rows - 1,)),
            dma((rows - 1,)),
        ],
        compiler_params=pltpu.CompilerParams(
            has_side_effects=True, collective_id=0, vmem_limit_bytes=60 * 1024 * 1024
        ),
        name="line_iterations",
    )(
        z_inverse,
        energy[0],
        damage_old[0],
        crack_seeds[0],
        irreversible[0],
        line_inverses,
    )
    return damage[None], norms


def solution(mesh):
    def local_any(energy, damage_old, crack_seeds, irreversible, line_inverses, z_inverse):
        rows, cols = mesh.shape["row"], mesh.shape["col"]
        block_cells = line_inverses.shape[1]
        width = energy.shape[2] // cols
        whole_blocks = (
            energy.shape[0] == 1
            and energy.shape[1] == block_cells
            and width == 2 * block_cells
            and block_cells % 256 == 0
            and 2 * cols == 8
            and 2 * rows <= 128
            and min(rows, cols) > 2
        )
        chosen = local if whole_blocks else local_turned
        return chosen(energy, damage_old, crack_seeds, irreversible, line_inverses, z_inverse)

    return jax.shard_map(
        local_any,
        mesh=mesh,
        in_specs=(
            P("col", "row", None),
            P("col", "row", None),
            P("col", "row", None),
            P("col", "row", None),
            P(),
            P(),
        ),
        out_specs=(P("col", "row", None), P()),
        check_vma=False,
    )
```

```python
import functools

import jax
import jax.numpy as jnp
from jax import lax
from jax.experimental import pallas as pl
from jax.experimental.pallas import tpu as pltpu
from jax.sharding import PartitionSpec as P

ITERS = 2


KAPPA = 2.0
STEP = 0.02
COUPLE = 0.5
EPSILON = 1e-06
HIGHEST = lax.Precision.HIGHEST


def second_difference(grid_field, along):
    extent = grid_field.shape[along]
    forward_diff = lax.slice_in_dim(grid_field, 1, extent, axis=along) - lax.slice_in_dim(
        grid_field, 0, extent - 1, axis=along
    )
    zero_shape = list(grid_field.shape)
    zero_shape[along] = 1
    zero_rim = jnp.zeros(zero_shape, grid_field.dtype)
    ahead = jnp.concatenate([forward_diff, zero_rim], axis=along)
    behind = jnp.concatenate([zero_rim, forward_diff], axis=along)
    return ahead - behind


def line_solve(line_rows, inverses):
    block_count, block_cells, _ = inverses.shape
    line_count = line_rows.shape[0]
    blocks = line_rows.reshape(line_count, block_count, block_cells)
    products = jnp.einsum("rkb,kcb->rkc", blocks, inverses, precision=lax.Precision.HIGHEST)
    first_col = inverses[:, :, 0]
    last_col = inverses[:, :, block_cells - 1]
    incoming = [jnp.zeros((line_count,), line_rows.dtype)]
    for block_index in range(block_count - 1):
        incoming.append(
            products[:, block_index, block_cells - 1]
            + COUPLE * incoming[block_index] * inverses[block_index, block_cells - 1, 0]
        )
    inflow = jnp.stack(incoming, axis=1)
    forward = products + COUPLE * inflow[:, :, None] * first_col[None]
    head_terms = [jnp.zeros((line_count,), line_rows.dtype) for block_index in range(block_count)]
    carried = forward[:, block_count - 1, 0]
    for block_index in range(block_count - 2, -1, -1):
        head_terms[block_index] = carried
        carried = (
            forward[:, block_index, 0]
            + COUPLE * carried * inverses[block_index, 0, block_cells - 1]
        )
    outflow = jnp.stack(head_terms, axis=1)
    solved = forward + COUPLE * outflow[:, :, None] * last_col[None]
    return solved.reshape(line_count, block_count * block_cells)


def local_turned(energy, damage_old, crack_seeds, irreversible, line_inverses, z_inverse):
    planes, rows_here, line_length = energy.shape
    row_count = lax.axis_size("row")
    col_count = lax.axis_size("col")
    total_planes = planes * col_count
    cell_count = total_planes * rows_here * row_count * line_length
    seeded = crack_seeds == 1
    damage = jnp.where(seeded, 1.0, damage_old)
    lower_bound = jnp.where(irreversible == 1, damage_old, 0.0)
    own_sums = []
    for sweep_index in range(ITERS):
        local_lap = second_difference(damage, 2)
        partial_value = energy - (1.0 + energy) * damage + KAPPA * local_lap
        moved_part, moved_damage = (
            lax.all_to_all(
                lax.all_to_all(
                    jnp.swapaxes(partial_value, 1, 2),
                    "row",
                    split_axis=1,
                    concat_axis=2,
                    tiled=True,
                ),
                "col",
                split_axis=1,
                concat_axis=0,
                tiled=True,
            ),
            lax.all_to_all(
                lax.all_to_all(
                    jnp.swapaxes(damage, 1, 2), "row", split_axis=1, concat_axis=2, tiled=True
                ),
                "col",
                split_axis=1,
                concat_axis=0,
                tiled=True,
            ),
        )
        lap_rest = second_difference(moved_damage, 2) + second_difference(moved_damage, 0)
        turned = moved_part + KAPPA * lap_rest
        turned_shape = turned.shape
        along_y = line_solve(turned.reshape(-1, turned_shape[2]), line_inverses).reshape(
            turned_shape
        )
        along_z = jnp.einsum("zk,kxy->zxy", z_inverse, along_y, precision=lax.Precision.HIGHEST)
        gathered = lax.all_to_all(
            lax.all_to_all(along_z, "row", split_axis=2, concat_axis=1, tiled=True),
            "col",
            split_axis=0,
            concat_axis=1,
            tiled=True,
        )
        piece_cells = gathered.shape[1] // (row_count * col_count)
        reordered = gathered.reshape(planes, col_count, row_count, piece_cells, rows_here)
        restored = jnp.transpose(reordered, (0, 4, 2, 1, 3)).reshape(planes, rows_here, line_length)
        update = STEP * line_solve(restored.reshape(-1, line_length), line_inverses).reshape(
            restored.shape
        )
        clamped = jnp.minimum(jnp.maximum(damage + update, lower_bound), 1.0)
        renewed = jnp.where(seeded, 1.0, clamped)
        own_sum = jnp.sum((renewed - damage) ** 2)
        own_sums.append(own_sum)
        damage = renewed
    global_sums = lax.psum(jnp.stack(own_sums), ("row", "col"))
    update_norms = jnp.sqrt(global_sums / cell_count + EPSILON) / STEP
    return (damage, update_norms)


def line_kernel(
    shape,
    z_hbm,
    energy,
    damage_hbm,
    seeds_hbm,
    irreversible_hbm,
    inverses,
    out,
    norms,
    damage_old,
    crack_seeds,
    irreversible,
    start,
    bound,
    ez,
    ec,
    fz,
    landing,
    dz,
    final,
    w_high,
    w_low,
    a_high,
    a_low,
    mix,
    corner,
    gx,
    gy,
    gx_high,
    gx_low,
    gy_both,
    gy_ends,
    gend,
    wx_send,
    wx_in,
    wx_own,
    wy_in,
    wy_turn,
    carry_rows,
    own_rows,
    packed,
    w_mix,
    y_base,
    strips,
    g_all,
    word_send,
    word_all,
    x_cols,
    y_lines,
    x_send,
    x_all,
    y_send,
    y_all,
    s_send,
    s_row,
    s_col_send,
    s_col,
    z_inv,
    local_sems,
    e_ssem,
    e_rsem,
    d_ssem,
    d_rsem,
    f_ssem,
    f_rsem,
    back_ssem,
    back_rsem,
    w_ssem,
    w_rsem,
    x_ssem,
    x_rsem,
    v_ssem,
    v_rsem,
    y_ssem,
    y_rsem,
    sc_ssem,
    sc_rsem,
    sr_ssem,
    sr_rsem,
):
    rows, cols, cells, width, x_blocks, blocks, cell_count, cuts, backs_at = shape
    planes = cols
    last = cells - 1
    groups = width // 128
    kinds = 2 * x_blocks + 2
    f32 = jnp.float32
    row, col = lax.axis_index("row"), lax.axis_index("col")
    row_peers = [lax.rem(row + o, rows) for o in range(1, rows)]
    col_peers = [lax.rem(col + o, cols) for o in range(1, cols)]

    def slab(who):
        return pl.ds(pl.multiple_of(who * width, width), width)

    def eight(at):
        return pl.ds(pl.multiple_of(at, 8), 8)

    def send(src, dst, ssem, rsem, **where):
        copy = pltpu.make_async_remote_copy(
            src_ref=src, dst_ref=dst, send_sem=ssem, recv_sem=rsem,
            device_id=where, device_id_type=pl.DeviceIdType.MESH,
        )
        copy.start()
        return copy

    def finish(sent):
        for copy in sent:
            copy.wait()

    def split(a):
        high = a.astype(jnp.bfloat16)
        return high, (a - high.astype(f32)).astype(jnp.bfloat16)

    def dot(a, b):
        return jnp.dot(a, b, preferred_element_type=f32)

    barrier = pltpu.get_barrier_semaphore()
    for peer in col_peers:
        pl.semaphore_signal(
            barrier, inc=1, device_id={"col": peer}, device_id_type=pl.DeviceIdType.MESH
        )
    for peer in row_peers:
        pl.semaphore_signal(
            barrier, inc=1, device_id={"row": peer}, device_id_type=pl.DeviceIdType.MESH
        )

    pulls = [
        pltpu.make_async_copy(damage_hbm, damage_old, local_sems.at[0]),
        pltpu.make_async_copy(seeds_hbm, crack_seeds, local_sems.at[1]),
        pltpu.make_async_copy(irreversible_hbm, irreversible, local_sems.at[2]),
    ]
    fetch = [
        pltpu.make_async_copy(energy.at[:, slab(col)], ez.at[col], local_sems.at[3]),
        pltpu.make_async_copy(inverses.at[row], gy, local_sems.at[4]),
        pltpu.make_async_copy(z_hbm, z_inv, local_sems.at[9 + x_blocks]),
    ]
    for n in range(4):
        down, over = (cells - 8) * (n // 2), (cells - 128) * (n % 2)
        fetch.append(
            pltpu.make_async_copy(
                inverses.at[:, pl.ds(down, 8), pl.ds(over, 128)], corner.at[n], local_sems.at[5 + n]
            )
        )
    for j in range(x_blocks):
        fetch.append(
            pltpu.make_async_copy(inverses.at[col * x_blocks + j], gx.at[j], local_sems.at[9 + j])
        )
    for side, at in ((0, 0), (1, cells - 128)):
        fetch.append(
            pltpu.make_async_copy(
                inverses.at[:, :, pl.ds(at, 128)], strips.at[side], local_sems.at[10 + x_blocks + side]
            )
        )
    for copy in pulls + fetch:
        copy.start()
    pl.semaphore_wait(barrier, rows + cols - 2)

    def move_piece(src, target, index, ssem, rsem):
        at = pl.ds(cuts[index], cuts[index + 1] - cuts[index])
        return [
            send(src.at[at, slab(peer)], target.at[col, at, :], ssem.at[index, n],
                 rsem.at[index, n], col=peer)
            for n, peer in enumerate(col_peers)
        ]

    moved_e = [
        send(energy.at[:, slab(peer)], ez.at[col], e_ssem.at[n], e_rsem.at[n], col=peer)
        for n, peer in enumerate(col_peers)
    ]
    finish(pulls)

    @pl.loop(0, cells // 16)
    def _(i):
        at = pl.ds(pl.multiple_of(i * 16, 16), 16)
        old = damage_old[at, :]
        seeded = crack_seeds[at, :] == 1
        start[at, :] = jnp.where(seeded, 1.0, old)
        bound[at, :] = jnp.where(seeded, 1.0, jnp.where(irreversible[at, :] == 1, old, 0.0))

    order = (0, 4, 1, 2, 3)
    moved_d = {n: move_piece(start, landing, n, d_ssem, d_rsem) for n in order}
    moved_f = {n: move_piece(bound, fz, n, f_ssem, f_rsem) for n in order[:2]}
    landing[col] = start[:, slab(col)]
    fz[col] = bound[:, slab(col)]

    lane = lax.broadcasted_iota(jnp.int32, (8, 128), 1)
    sub = lax.broadcasted_iota(jnp.int32, (8, 128), 0)
    upper_half = sub < planes
    zero = jnp.zeros((8, 128), f32)
    finish(fetch)

    def lane_of(a, n):
        return jnp.broadcast_to(a[:, n : n + 1], (8, 128))

    def corner_of(down, over, k):
        tile = corner[2 * down + over, k]
        at = (7 if down else 0, 127 if over else 0)
        return jnp.broadcast_to(tile[at[0] : at[0] + 1, at[1] : at[1] + 1], (8, 128))

    def hot(index):
        return jnp.where(lane == index, 1.0, 0.0)

    def carries(first, final_of, lower=None, upper=None):
        firsts, finals = [], []
        low = [None if lower is None else lower(k) for k in range(blocks)]
        high = [None if upper is None else upper(k) for k in range(blocks)]
        for k in range(blocks):
            begin, end = hot(first(k)), hot(final_of(k))
            if low[k] is not None:
                begin = begin + corner_of(0, 0, k) * hot(low[k])
                end = end + corner_of(1, 0, k) * hot(low[k])
            if high[k] is not None:
                begin = begin + corner_of(0, 1, k) * hot(high[k])
                end = end + corner_of(1, 1, k) * hot(high[k])
            firsts.append(begin)
            finals.append(end)
        incoming = [zero]
        for k in range(blocks - 1):
            incoming.append(finals[k] + COUPLE * corner_of(1, 0, k) * incoming[k])
        heads = [
            firsts[k] + COUPLE * corner_of(0, 0, k) * incoming[k] for k in range(blocks)
        ]
        carried = heads[blocks - 1]
        outgoing = [zero] * blocks
        for k in range(blocks - 2, -1, -1):
            outgoing[k] = carried
            carried = heads[k] + COUPLE * corner_of(0, 1, k) * carried
        enter, leave = [], []
        for k in range(blocks):
            enter.append(COUPLE * incoming[k] + (zero if low[k] is None else hot(low[k])))
            leave.append(COUPLE * outgoing[k] + (zero if high[k] is None else hot(high[k])))
        return incoming, outgoing, enter, leave

    def picked(which, options):
        total = zero
        for n, option in enumerate(options):
            if option is not None:
                total = total + jnp.where(which == n, option, 0.0)
        return total

    def at_own(c, weights):
        return pltpu.roll(weights, 128 - 8 * c, 1) if c > 0 else weights

    def left_of(k):
        c = k // x_blocks
        return 8 * (c - 1) + 2 * x_blocks + 1 if k % x_blocks == 0 and c > 0 else None

    def right_of(k):
        c = k // x_blocks
        return 8 * (c + 1) + 2 * x_blocks if k % x_blocks == x_blocks - 1 and c < cols - 1 else None

    incoming, outgoing, enter, leave = carries(
        lambda k: 8 * (k // x_blocks) + k % x_blocks,
        lambda k: 8 * (k // x_blocks) + x_blocks + k % x_blocks,
        left_of,
        right_of,
    )
    to_right = picked(col, [
        at_own(c, incoming[(c + 1) * x_blocks] + hot(8 * c + 2 * x_blocks + 1) / COUPLE)
        if c < cols - 1 else None
        for c in range(cols)
    ])
    to_left = picked(col, [
        at_own(c, leave[c * x_blocks - 1] / COUPLE) if c > 0 else None for c in range(cols)
    ])
    for n in range(kinds):
        wx_send[n] = jnp.where(upper_half, lane_of(to_right, n), lane_of(to_left, n))
    for m in range(2 * x_blocks):
        table = (enter, leave)[m % 2]
        everywhere = picked(col, [table[c * x_blocks + m // 2] for c in range(cols)])
        here = picked(col, [at_own(c, table[c * x_blocks + m // 2]) for c in range(cols)])
        for c in range(cols):
            from_left = jnp.where(col > c, lane_of(everywhere, 8 * c + 2 * x_blocks - 1), 0.0)
            from_right = jnp.where(col < c, lane_of(everywhere, 8 * c), 0.0)
            wx_in[m, c] = jnp.where(upper_half, from_left, from_right)
        for n in range(kinds):
            wx_own[m, n] = lane_of(here, n)

    incoming, outgoing, enter, leave = carries(lambda k: 2 * k, lambda k: 2 * k + 1)
    enters, leaves = picked(row, enter), picked(row, leave)
    for k in range(rows):
        wy_in[0, k] = lane_of(enters, 2 * k + 1)
        wy_in[1, k] = jnp.where(row >= k, lane_of(leaves, 2 * k + 1), lane_of(leaves, 2 * k))
    wy_turn[...] = picked(
        row, [lane_of(outgoing[k - 1], 2 * k + 1) if k > 0 else None for k in range(rows)]
    )

    upper_wide = lax.broadcasted_iota(jnp.int32, (8, cells), 0) < planes
    for j in range(x_blocks):
        turned = gx[j].T
        gx_high[j], gx_low[j] = split(turned)
        for side, at in ((0, 0), (1, last)):
            line = jnp.broadcast_to(turned[at : at + 1], (8, cells))
            gend[side, j] = line
            if j == 0:
                gend[side, x_blocks] = line
            else:
                gend[side, x_blocks] = jnp.where(upper_wide, gend[side, x_blocks], line)
    gy_both[:cells], gy_both[cells:] = split(gy[...])
    gy_ends[0] = jnp.broadcast_to(gy[:, :1], (cells, 128))
    gy_ends[1] = jnp.broadcast_to(gy[:, last:], (cells, 128))

    for k in range(blocks):
        for side, at in ((0, 0), (1, 127)):
            line = strips[side, k].T[at : at + 1]
            g_all[side, k] = jnp.broadcast_to(line, (8, cells))

    first_col = jnp.where(col == 0, 1.0, 0.0)
    last_col = jnp.where(col == cols - 1, 1.0, 0.0)
    lane16 = lax.broadcasted_iota(jnp.int32, (16, 128), 1)
    at_first, at_last = lane16 == 0, lane16 == 127

    mixing = [[KAPPA * z_inv[z, k] for k in range(planes)] for z in range(planes)]
    for k in range(planes):
        weights = zero
        for z in range(planes):
            weights = jnp.where(lax.rem(sub, planes) == z, mixing[z][k], weights)
        w_mix[k] = weights

    def scale_energy():
        @pl.loop(0, cells // 8)
        def _(i):
            for z in range(planes):
                sides = 4 + (z > 0) + (z < planes - 1)
                scaled = ez[z, eight(i * 8), :] * (1.0 / KAPPA)
                ez[z, eight(i * 8), :] = scaled
                ec[z, eight(i * 8), :] = scaled + (1.0 / KAPPA + sides)

    def regroup(low, high):
        @pl.loop(low // 8, high // 8)
        def _(i):
            for z in range(planes):
                tile = landing[z, eight(i * 8), :]
                for g in range(groups):
                    dz[0, z, g, eight(i * 8 + 8), :] = tile[:, g * 128 : (g + 1) * 128]

    def share_rows(it):
        return [
            send(dz.at[it, :, :, pl.ds(cells, 8), :], dz.at[it, :, :, pl.ds(0, 8), :],
                 v_ssem.at[it, 0], v_rsem.at[it, 0], row=lax.rem(row + 1, rows)),
            send(dz.at[it, :, :, pl.ds(8, 8), :], dz.at[it, :, :, pl.ds(cells + 8, 8), :],
                 v_ssem.at[it, 1], v_rsem.at[it, 1], row=lax.rem(row + rows - 1, rows)),
        ]

    def mirror(it):
        for z in range(planes):
            for g in range(groups):
                dz[it, z, g, 7:8, :] = jnp.where(
                    row == 0, dz[it, z, g, 8:9, :], dz[it, z, g, 7:8, :]
                )
                dz[it, z, g, cells + 8 : cells + 9, :] = jnp.where(
                    row == rows - 1,
                    dz[it, z, g, cells + 7 : cells + 8, :],
                    dz[it, z, g, cells + 8 : cells + 9, :],
                )

    def residual(it, low, high):
        @pl.loop(low // 16, high // 16)
        def _(i):
            base = pl.multiple_of(i * 16, 16)
            here = pl.ds(base, 16)
            padded = pl.ds(pl.multiple_of(base + 8, 8), 16)
            for g in range(groups):
                lanes = slice(g * 128, (g + 1) * 128)
                mids = [dz[it, z, g, padded, :] for z in range(planes)]
                value = []
                for z in range(planes):
                    d = mids[z]
                    near = dz[it, z, g, pl.ds(base + 7, 16), :] + dz[it, z, g, pl.ds(base + 9, 16), :]
                    before = d * first_col
                    if g > 0:
                        before = pltpu.roll(dz[it, z, g - 1, padded, :], 1, 1)
                    after = d * last_col
                    if g < groups - 1:
                        after = pltpu.roll(dz[it, z, g + 1, padded, :], 127, 1)
                    near = near + jnp.where(at_first, before, pltpu.roll(d, 1, 1))
                    near = near + jnp.where(at_last, after, pltpu.roll(d, 127, 1))
                    if z > 0:
                        near = near + mids[z - 1]
                    if z < planes - 1:
                        near = near + mids[z + 1]
                    value.append(near + (ez[z, here, lanes] - ec[z, here, lanes] * d))
                for z in range(planes):
                    total = mixing[z][0] * value[0]
                    for k in range(1, planes):
                        total = total + mixing[z][k] * value[k]
                    w_high[z, here, lanes], w_low[z, here, lanes] = split(total)

    def x_product(it, ranges):
        packs = [jnp.zeros((b - a, 128), f32) for a, b in ranges]
        spots = [lax.broadcasted_iota(jnp.int32, (b - a, 128), 1) for a, b in ranges]

        def place(n, tile, lane_from, lane_to):
            if lane_from != lane_to:
                tile = pltpu.roll(tile, (lane_to - lane_from) % 128, 1)
            packs[n] = jnp.where(spots[n] == lane_to, tile, packs[n])

        for j in range(x_blocks):
            block = slice(j * cells, (j + 1) * cells)
            parts = [(z, n) for z in range(planes) for n in range(len(ranges))]
            cut = [slice(*ranges[n]) for _, n in parts]
            high_rows = jnp.concatenate(
                [w_high[z, c, block] for (z, _), c in zip(parts, cut)], axis=0
            )
            low_rows = jnp.concatenate(
                [w_low[z, c, block] for (z, _), c in zip(parts, cut)], axis=0
            )
            count = high_rows.shape[0]
            twice = dot(jnp.concatenate([high_rows, low_rows], axis=0), gx_high[j])
            along = twice[:count] + (twice[count:] + dot(high_rows, gx_low[j]))
            at = 0
            for (z, n), c in zip(parts, cut):
                part = along[at : at + c.stop - c.start]
                at += c.stop - c.start
                a_high[z, c, block], a_low[z, c, block] = split(part)
                place(n, part[:, :128], 0, j * planes + z)
                place(n, part[:, cells - 128 :], 127, (x_blocks + j) * planes + z)
        for n, (a, b) in enumerate(ranges):
            for z in range(planes):
                near = pl.ds(8 + a, b - a)
                place(n, dz[it, z, 0, near, :], 0, 2 * x_blocks * planes + z)
                place(n, dz[it, z, groups - 1, near, :], 127, (2 * x_blocks + 1) * planes + z)
            packed[a:b, :] = packs[n]

    def y_times(high, low):
        twice = dot(gy_both[...], high)
        return twice[:cells] + (twice[cells:] + dot(gy_both[:cells], low))

    def y_product(it, z):
        both = y_times(a_high[z], a_low[z])
        mix[z] = both
        for side, at in ((0, 0), (1, last)):
            for j in range(x_blocks):
                y_base[side, z, j : j + 1, :] = both[at : at + 1, j * cells : (j + 1) * cells]
        if it + 1 == ITERS:
            d = jnp.concatenate([dz[it, z, g, pl.ds(8, cells), :] for g in range(groups)], axis=1)
            final[z] = d + STEP * both

    def x_ends():
        turned = y_times(*split(packed[...])).T

        def keep(n, tile):
            other = pltpu.roll(tile, planes, 0)
            pair = (tile, other) if n % 2 == 0 else (other, tile)
            own_rows[n] = jnp.where(upper_wide, pair[0], pair[1])

        for n in range(2 * x_blocks):
            keep(n, turned[8 * (n // 2) : 8 * (n // 2) + 8])
        tile = turned[8 * x_blocks : 8 * x_blocks + 8]
        total = None
        for k in range(planes):
            line = jnp.where(
                upper_wide,
                jnp.broadcast_to(tile[k : k + 1], (8, cells)),
                jnp.broadcast_to(tile[planes + k : planes + k + 1], (8, cells)),
            )
            term = wide(w_mix[k]) * line
            total = term if total is None else total + term
        for n in range(2):
            keep(2 * x_blocks + n, total)

    def wide(weights):
        return jnp.concatenate([weights] * (cells // 128), axis=1)

    def x_share(it):
        total = None
        for n in range(kinds):
            term = wide(wx_send[n]) * own_rows[n]
            total = term if total is None else total + term
        x_send[it] = total
        x_all[it, col] = total
        return [
            send(x_send.at[it], x_all.at[it, col], x_ssem.at[it, n], x_rsem.at[it, n], col=peer)
            for n, peer in enumerate(col_peers)
        ]

    def y_share(it):
        sides = []
        for side in range(2):
            parts = []
            for j in range(x_blocks):
                m = 2 * j + side
                total = wide(wx_in[m, 0]) * x_all[it, 0]
                for c in range(1, cols):
                    total = total + wide(wx_in[m, c]) * x_all[it, c]
                total = total + pltpu.roll(total, planes, 0)
                for n in range(kinds):
                    total = total + wide(wx_own[m, n]) * own_rows[n]
                parts.append(total)
            sides.append(jnp.where(upper_wide, parts[0], parts[1]))
        lines = []
        for side, at in ((0, 0), (1, last)):
            line = jnp.concatenate(
                [y_base[side, z, j : j + 1, :] for j in range(x_blocks) for z in range(planes)],
                axis=0,
            )
            for n in range(2):
                scale = jnp.broadcast_to(sides[n][:, at : at + 1], (8, cells))
                line = line + scale * gend[n, x_blocks]
            lines.append(line)
        y_send[it, 0] = lines[1]
        y_send[it, 1] = lines[0] + wide(wy_turn[...]) * lines[1]
        y_all[it, row] = lines[1]
        sent = [
            send(y_send.at[it, lax.div(row + n + 1, rows)], y_all.at[it, row], y_ssem.at[it, n],
                 y_rsem.at[it, n], row=peer)
            for n, peer in enumerate(row_peers)
        ]
        stacked = jnp.concatenate(sides + [jnp.zeros((112, cells), f32)], axis=0).T
        for t in range(cells // 8):
            here = slice(t * 8, t * 8 + 8)
            tile = stacked[here]
            for z in range(planes):
                for j in range(x_blocks):
                    block = slice(j * cells, (j + 1) * cells)
                    n = j * planes + z
                    mix[z, here, block] = (
                        mix[z, here, block]
                        + tile[:, n : n + 1] * gend[0, j]
                        + tile[:, 8 + n : 9 + n] * gend[1, j]
                    )
        finish(sent)
        carried = []
        for side in range(2):
            total = wide(wy_in[side, 0]) * y_all[it, 0]
            for k in range(1, rows):
                total = total + wide(wy_in[side, k]) * y_all[it, k]
            for z in range(planes):
                for j in range(x_blocks):
                    n = j * planes + z
                    carry_rows[2 * z + side, :, j * cells : (j + 1) * cells] = jnp.broadcast_to(
                        total[n : n + 1], (8, cells)
                    )
            carried.append(total)
        return sides, carried

    def settle(it, low, high, squares):
        def step(i, acc):
            here, padded = eight(i * 8), eight(i * 8 + 8)
            g_first = jnp.concatenate([gy_ends[0, here, :]] * groups, axis=1)
            g_last = jnp.concatenate([gy_ends[1, here, :]] * groups, axis=1)
            for z in range(planes):
                solved = mix[z, here, :] + g_first * carry_rows[2 * z] + g_last * carry_rows[2 * z + 1]
                d = jnp.concatenate([dz[it, z, g, padded, :] for g in range(groups)], axis=1)
                renewed = jnp.minimum(jnp.maximum(d + STEP * solved, fz[z, here, :]), 1.0)
                if it + 1 < ITERS:
                    for g in range(groups):
                        dz[it + 1, z, g, padded, :] = renewed[:, g * 128 : (g + 1) * 128]
                change = renewed - d
                acc = acc + change * change
            return acc

        return lax.fori_loop(low // 8, high // 8, step, squares)

    def stream(it, ready):
        ready(order[0])
        ready(order[1])
        shared = share_rows(it)
        finish(shared)
        mirror(it)
        ranges = [(0, cuts[1] - 16), (cuts[4] + 16, cells)]
        for a, b in ranges:
            residual(it, a, b)
        x_product(it, ranges)
        for n in order[2:]:
            ready(n)
            a, b = cuts[n] - 16, cuts[n + 1] - 16
            if n == order[-1]:
                b += 32
            residual(it, a, b)
            x_product(it, [(a, b)])
        x_ends()

    def arrived(n):
        finish(moved_d[n])
        regroup(cuts[n], cuts[n + 1])

    finish(moved_e)
    scale_energy()
    stream(0, arrived)
    sent = x_share(0)
    for n in order[2:]:
        moved_f[n] = move_piece(bound, fz, n, f_ssem, f_rsem)
    for z in range(planes):
        y_product(0, z)
    finish(sent)
    y_share(0)

    totals = []
    blank = jnp.zeros((8, width), f32)
    held = [blank]

    def settled(n):
        finish(moved_f[n])
        held.append(settle(0, cuts[n], cuts[n + 1], held.pop()))

    stream(1, settled)
    def give_back(n, m):
        at = pl.ds(backs_at[n], backs_at[n + 1] - backs_at[n])
        return send(final.at[col_peers[m], at, :], out.at[at, slab(col)], back_ssem.at[n, m],
                    back_rsem.at[n, m], col=col_peers[m])

    backs = [[] for _ in backs_at[1:]]

    def give_all(n):
        for m in range(cols - 1):
            backs[n].append(give_back(n, m))

    def complete(low, high):
        @pl.loop(low // 8, high // 8)
        def _(i):
            here = eight(i * 8)
            tile = x_cols[here, :]
            ends_of = [
                jnp.concatenate([gy_ends[n, here, :]] * (cells // 128), axis=1) for n in range(2)
            ]
            for k in range(blocks):
                block = slice(k * cells, (k + 1) * cells)
                n = 8 * (k // x_blocks) + 2 * (k % x_blocks)
                value = (
                    out[here, block]
                    + tile[:, n : n + 1] * g_all[0, k]
                    + tile[:, n + 1 : n + 2] * g_all[1, k]
                    + (ends_of[0] * y_lines[0, k] + ends_of[1] * y_lines[1, k])
                )
                out[here, block] = jnp.minimum(jnp.maximum(value, bound[here, block]), 1.0)

    sent = x_share(1)
    for m in range(cols - 1):
        y_product(1, col_peers[m])
        for n in range(2):
            backs[n].append(give_back(n, m))
    y_product(1, col)
    out[:, slab(col)] = final[col]
    finish(sent)
    sides, carried = y_share(1)
    for z in range(planes):
        for j in range(x_blocks):
            n = j * planes + z
            for side in range(2):
                at = 2 * j + side
                word_send[z, at : at + 1, :] = STEP * sides[side][n : n + 1]
                at += 2 * x_blocks
                word_send[z, at : at + 1, :] = STEP * carried[side][n : n + 1]
    words = [
        send(word_send.at[peer], word_all.at[col], w_ssem.at[n], w_rsem.at[n], col=peer)
        for n, peer in enumerate(col_peers)
    ]
    give_all(2)
    word_all[col] = word_send[col]
    totals.append(jnp.sum(held[0]))
    totals.append(jnp.sum(settle(ITERS - 1, 0, cells, blank)))
    s_send[...] = jnp.where(sub == 0, totals[0], jnp.where(sub == 1, totals[1], 0.0))
    shares = [
        send(s_send, s_row.at[n], sr_ssem.at[n], sr_rsem.at[n], row=peer)
        for n, peer in enumerate(row_peers)
    ]
    finish(shares)
    total = s_send[...]
    for n in range(rows - 1):
        total = total + s_row[n]
    s_col_send[...] = total
    shares = [
        send(s_col_send, s_col.at[n], sc_ssem.at[n], sc_rsem.at[n], col=peer)
        for n, peer in enumerate(col_peers)
    ]
    for n in range(3, len(backs_at) - 1):
        give_all(n)
    finish(words)
    x_cols[...] = jnp.concatenate(
        [word_all[c] for c in range(cols)] + [jnp.zeros((128 - 8 * cols, cells), f32)], axis=0
    ).T
    for k in range(blocks):
        for side in range(2):
            at = 2 * x_blocks + 2 * (k % x_blocks) + side
            y_lines[side, k] = jnp.broadcast_to(
                word_all[k // x_blocks, at : at + 1, :], (8, cells)
            )
    for n in range(len(backs_at) - 2):
        finish(backs[n])
        complete(backs_at[n], backs_at[n + 1])
    finish(shares)
    for n in range(cols - 1):
        total = total + s_col[n]
    sizes = jnp.sqrt(total / cell_count + EPSILON) / STEP
    norms[...] = jnp.where(lane == 0, sizes[:1, :], sizes[1:2, :])[0, :ITERS]
    finish(backs[-1])
    complete(backs_at[-2], backs_at[-1])


def local(energy, damage_old, crack_seeds, irreversible, line_inverses, z_inverse):
    planes, cells, line_length = energy.shape
    rows, cols = lax.axis_size("row"), lax.axis_size("col")
    blocks, _, _ = line_inverses.shape
    width = line_length // cols
    x_blocks = width // cells
    kinds = 2 * x_blocks + 2
    step = cells // 16
    cuts = (0, 3 * step, 8 * step, 12 * step, 13 * step, cells)
    backs_at = (0, 4 * step, 8 * step, 11 * step, 14 * step, cells)
    cell_count = float(cols * rows * cells * line_length)
    shape = (rows, cols, cells, width, x_blocks, blocks, cell_count, cuts, backs_at)
    f32 = jnp.float32
    bf16 = jnp.bfloat16
    dma = pltpu.SemaphoreType.DMA
    vmem = pl.BlockSpec(memory_space=pltpu.VMEM)
    damage, norms = pl.pallas_call(
        functools.partial(line_kernel, shape),
        out_shape=(
            pltpu.VMEM((cells, line_length), f32),
            pltpu.VMEM((ITERS,), f32),
        ),
        in_specs=[pl.BlockSpec(memory_space=pl.ANY)] * 6,
        out_specs=(vmem, vmem),
        scratch_shapes=[
            pltpu.VMEM((cells, line_length), f32),
            pltpu.VMEM((cells, line_length), jnp.int32),
            pltpu.VMEM((cells, line_length), jnp.int32),
            pltpu.VMEM((cells, line_length), f32),
            pltpu.VMEM((cells, line_length), f32),
            pltpu.VMEM((cols, cells, width), f32),
            pltpu.VMEM((cols, cells, width), f32),
            pltpu.VMEM((cols, cells, width), f32),
            pltpu.VMEM((cols, cells, width), f32),
            pltpu.VMEM((ITERS, cols, width // 128, cells + 16, 128), f32),
            pltpu.VMEM((cols, cells, width), f32),
            pltpu.VMEM((cols, cells, width), bf16),
            pltpu.VMEM((cols, cells, width), bf16),
            pltpu.VMEM((cols, cells, width), bf16),
            pltpu.VMEM((cols, cells, width), bf16),
            pltpu.VMEM((cols, cells, width), f32),
            pltpu.VMEM((4, blocks, 8, 128), f32),
            pltpu.VMEM((x_blocks, cells, cells), f32),
            pltpu.VMEM((cells, cells), f32),
            pltpu.VMEM((x_blocks, cells, cells), bf16),
            pltpu.VMEM((x_blocks, cells, cells), bf16),
            pltpu.VMEM((2 * cells, cells), bf16),
            pltpu.VMEM((2, cells, 128), f32),
            pltpu.VMEM((2, x_blocks + 1, 8, cells), f32),
            pltpu.VMEM((kinds, 8, 128), f32),
            pltpu.VMEM((2 * x_blocks, cols, 8, 128), f32),
            pltpu.VMEM((2 * x_blocks, kinds, 8, 128), f32),
            pltpu.VMEM((2, rows, 8, 128), f32),
            pltpu.VMEM((8, 128), f32),
            pltpu.VMEM((2 * cols, 8, width), f32),
            pltpu.VMEM((kinds, 8, cells), f32),
            pltpu.VMEM((cells, 128), f32),
            pltpu.VMEM((cols, 8, 128), f32),
            pltpu.VMEM((2, cols, 8, cells), f32),
            pltpu.VMEM((2, blocks, cells, 128), f32),
            pltpu.VMEM((2, blocks, 8, cells), f32),
            pltpu.VMEM((cols, 8, cells), f32),
            pltpu.VMEM((cols, 8, cells), f32),
            pltpu.VMEM((cells, 128), f32),
            pltpu.VMEM((2, blocks, 8, cells), f32),
            pltpu.VMEM((ITERS, 8, cells), f32),
            pltpu.VMEM((ITERS, cols, 8, cells), f32),
            pltpu.VMEM((ITERS, 2, 8, cells), f32),
            pltpu.VMEM((ITERS, rows, 8, cells), f32),
            pltpu.VMEM((8, 128), f32),
            pltpu.VMEM((rows - 1, 8, 128), f32),
            pltpu.VMEM((8, 128), f32),
            pltpu.VMEM((cols - 1, 8, 128), f32),
            pltpu.SMEM((cols, cols), f32),
            dma((x_blocks + 12,)),
            dma((cols - 1,)),
            dma((cols - 1,)),
            dma((5, cols - 1)),
            dma((5, cols - 1)),
            dma((5, cols - 1)),
            dma((5, cols - 1)),
            dma((5, cols - 1)),
            dma((5, cols - 1)),
            dma((cols - 1,)),
            dma((cols - 1,)),
            dma((ITERS, cols - 1)),
            dma((ITERS, cols - 1)),
            dma((ITERS, 2)),
            dma((ITERS, 2)),
            dma((ITERS, rows - 1)),
            dma((ITERS, rows - 1)),
            dma((cols - 1,)),
            dma((cols - 1,)),
            dma((rows - 1,)),
            dma((rows - 1,)),
        ],
        compiler_params=pltpu.CompilerParams(
            has_side_effects=True, collective_id=0, vmem_limit_bytes=60 * 1024 * 1024
        ),
        name="line_iterations",
    )(
        z_inverse,
        energy[0],
        damage_old[0],
        crack_seeds[0],
        irreversible[0],
        line_inverses,
    )
    return damage[None], norms


def solution(mesh):
    def local_any(energy, damage_old, crack_seeds, irreversible, line_inverses, z_inverse):
        rows, cols = mesh.shape["row"], mesh.shape["col"]
        block_cells = line_inverses.shape[1]
        width = energy.shape[2] // cols
        whole_blocks = (
            energy.shape[0] == 1
            and energy.shape[1] == block_cells
            and width == 2 * block_cells
            and block_cells % 256 == 0
            and 2 * cols == 8
            and 2 * rows <= 128
            and min(rows, cols) > 2
        )
        chosen = local if whole_blocks else local_turned
        return chosen(energy, damage_old, crack_seeds, irreversible, line_inverses, z_inverse)

    return jax.shard_map(
        local_any,
        mesh=mesh,
        in_specs=(
            P("col", "row", None),
            P("col", "row", None),
            P("col", "row", None),
            P("col", "row", None),
            P(),
            P(),
        ),
        out_specs=(P("col", "row", None), P()),
        check_vma=False,
    )
```

```python
import functools

import jax
import jax.numpy as jnp
from jax import lax
from jax.experimental import pallas as pl
from jax.experimental.pallas import tpu as pltpu
from jax.sharding import PartitionSpec as P

ITERS = 2


KAPPA = 2.0
STEP = 0.02
COUPLE = 0.5
EPSILON = 1e-06
HIGHEST = lax.Precision.HIGHEST


def second_difference(grid_field, along):
    extent = grid_field.shape[along]
    forward_diff = lax.slice_in_dim(grid_field, 1, extent, axis=along) - lax.slice_in_dim(
        grid_field, 0, extent - 1, axis=along
    )
    zero_shape = list(grid_field.shape)
    zero_shape[along] = 1
    zero_rim = jnp.zeros(zero_shape, grid_field.dtype)
    ahead = jnp.concatenate([forward_diff, zero_rim], axis=along)
    behind = jnp.concatenate([zero_rim, forward_diff], axis=along)
    return ahead - behind


def line_solve(line_rows, inverses):
    block_count, block_cells, _ = inverses.shape
    line_count = line_rows.shape[0]
    blocks = line_rows.reshape(line_count, block_count, block_cells)
    products = jnp.einsum("rkb,kcb->rkc", blocks, inverses, precision=lax.Precision.HIGHEST)
    first_col = inverses[:, :, 0]
    last_col = inverses[:, :, block_cells - 1]
    incoming = [jnp.zeros((line_count,), line_rows.dtype)]
    for block_index in range(block_count - 1):
        incoming.append(
            products[:, block_index, block_cells - 1]
            + COUPLE * incoming[block_index] * inverses[block_index, block_cells - 1, 0]
        )
    inflow = jnp.stack(incoming, axis=1)
    forward = products + COUPLE * inflow[:, :, None] * first_col[None]
    head_terms = [jnp.zeros((line_count,), line_rows.dtype) for block_index in range(block_count)]
    carried = forward[:, block_count - 1, 0]
    for block_index in range(block_count - 2, -1, -1):
        head_terms[block_index] = carried
        carried = (
            forward[:, block_index, 0]
            + COUPLE * carried * inverses[block_index, 0, block_cells - 1]
        )
    outflow = jnp.stack(head_terms, axis=1)
    solved = forward + COUPLE * outflow[:, :, None] * last_col[None]
    return solved.reshape(line_count, block_count * block_cells)


def local_turned(energy, damage_old, crack_seeds, irreversible, line_inverses, z_inverse):
    planes, rows_here, line_length = energy.shape
    row_count = lax.axis_size("row")
    col_count = lax.axis_size("col")
    total_planes = planes * col_count
    cell_count = total_planes * rows_here * row_count * line_length
    seeded = crack_seeds == 1
    damage = jnp.where(seeded, 1.0, damage_old)
    lower_bound = jnp.where(irreversible == 1, damage_old, 0.0)
    own_sums = []
    for sweep_index in range(ITERS):
        local_lap = second_difference(damage, 2)
        partial_value = energy - (1.0 + energy) * damage + KAPPA * local_lap
        moved_part, moved_damage = (
            lax.all_to_all(
                lax.all_to_all(
                    jnp.swapaxes(partial_value, 1, 2),
                    "row",
                    split_axis=1,
                    concat_axis=2,
                    tiled=True,
                ),
                "col",
                split_axis=1,
                concat_axis=0,
                tiled=True,
            ),
            lax.all_to_all(
                lax.all_to_all(
                    jnp.swapaxes(damage, 1, 2), "row", split_axis=1, concat_axis=2, tiled=True
                ),
                "col",
                split_axis=1,
                concat_axis=0,
                tiled=True,
            ),
        )
        lap_rest = second_difference(moved_damage, 2) + second_difference(moved_damage, 0)
        turned = moved_part + KAPPA * lap_rest
        turned_shape = turned.shape
        along_y = line_solve(turned.reshape(-1, turned_shape[2]), line_inverses).reshape(
            turned_shape
        )
        along_z = jnp.einsum("zk,kxy->zxy", z_inverse, along_y, precision=lax.Precision.HIGHEST)
        gathered = lax.all_to_all(
            lax.all_to_all(along_z, "row", split_axis=2, concat_axis=1, tiled=True),
            "col",
            split_axis=0,
            concat_axis=1,
            tiled=True,
        )
        piece_cells = gathered.shape[1] // (row_count * col_count)
        reordered = gathered.reshape(planes, col_count, row_count, piece_cells, rows_here)
        restored = jnp.transpose(reordered, (0, 4, 2, 1, 3)).reshape(planes, rows_here, line_length)
        update = STEP * line_solve(restored.reshape(-1, line_length), line_inverses).reshape(
            restored.shape
        )
        clamped = jnp.minimum(jnp.maximum(damage + update, lower_bound), 1.0)
        renewed = jnp.where(seeded, 1.0, clamped)
        own_sum = jnp.sum((renewed - damage) ** 2)
        own_sums.append(own_sum)
        damage = renewed
    global_sums = lax.psum(jnp.stack(own_sums), ("row", "col"))
    update_norms = jnp.sqrt(global_sums / cell_count + EPSILON) / STEP
    return (damage, update_norms)


def line_kernel(
    shape,
    z_hbm,
    energy,
    damage_hbm,
    seeds_hbm,
    irreversible_hbm,
    inverses,
    out,
    norms,
    damage_old,
    crack_seeds,
    irreversible,
    start,
    bound,
    ez,
    ec,
    fz,
    landing,
    dz,
    final,
    w_high,
    w_low,
    a_high,
    a_low,
    mix,
    inverse,
    gx_high,
    gx_low,
    gy_both,
    gy_ends,
    gend,
    wx_send,
    wx_in,
    wx_own,
    wy_in,
    wy_turn,
    carry_rows,
    own_rows,
    packed,
    w_mix,
    y_base,
    g_all,
    word_send,
    word_all,
    x_cols,
    y_lines,
    x_send,
    x_all,
    y_send,
    y_all,
    s_send,
    s_row,
    s_col_send,
    s_col,
    z_inv,
    local_sems,
    greet,
    e_sems,
    d_ssem,
    d_rsem,
    f_ssem,
    f_rsem,
    back_ssem,
    back_rsem,
    w_sems,
    x_sems,
    v_sems,
    y_sems,
    s_sems,
):
    rows, cols, cells, width, x_blocks, blocks, cell_count, cuts, backs_at = shape
    planes = cols
    last = cells - 1
    groups = width // 128
    kinds = 2 * x_blocks + 2
    f32 = jnp.float32
    row, col = lax.axis_index("row"), lax.axis_index("col")
    row_peers = [lax.rem(row + o, rows) for o in range(1, rows)]
    col_peers = [lax.rem(col + o, cols) for o in range(1, cols)]

    def slab(who):
        return pl.ds(pl.multiple_of(who * width, width), width)

    def eight(at):
        return pl.ds(pl.multiple_of(at, 8), 8)

    def send(src, dst, ssem, rsem, **where):
        copy = pltpu.make_async_remote_copy(
            src_ref=src, dst_ref=dst, send_sem=ssem, recv_sem=rsem,
            device_id=where, device_id_type=pl.DeviceIdType.MESH,
        )
        copy.start()
        return copy

    def finish(sem, sized):
        pltpu.make_async_copy(sized, sized, sem).wait()

    def split(a):
        high = a.astype(jnp.bfloat16)
        return high, (a - high.astype(f32)).astype(jnp.bfloat16)

    def dot(a, b):
        return jnp.dot(a, b, preferred_element_type=f32)

    barrier = pltpu.get_barrier_semaphore()
    for peer in col_peers:
        pl.semaphore_signal(
            barrier, inc=1, device_id={"col": peer}, device_id_type=pl.DeviceIdType.MESH
        )
    above, below = row > 0, row < rows - 1

    def signal_row(sem, who):
        pl.semaphore_signal(
            sem, inc=1, device_id={"row": who}, device_id_type=pl.DeviceIdType.MESH
        )

    @pl.when(above)
    def _():
        signal_row(barrier, row - 1)

    @pl.when(below)
    def _():
        signal_row(barrier, row + 1)

    pulls = [
        pltpu.make_async_copy(damage_hbm, damage_old, local_sems.at[0]),
        pltpu.make_async_copy(seeds_hbm, crack_seeds, local_sems.at[1]),
        pltpu.make_async_copy(irreversible_hbm, irreversible, local_sems.at[2]),
    ]
    fetch = [
        pltpu.make_async_copy(energy.at[:, slab(col)], ez.at[col], local_sems.at[3]),
        pltpu.make_async_copy(inverses, inverse, local_sems.at[4]),
        pltpu.make_async_copy(z_hbm, z_inv, local_sems.at[5]),
    ]
    for copy in pulls + fetch:
        copy.start()
    neighbours = jnp.where(above, 1, 0) + jnp.where(below, 1, 0)
    pl.semaphore_wait(barrier, cols - 1 + neighbours)

    def move_piece(src, target, index, ssem, rsem):
        at = pl.ds(cuts[index], cuts[index + 1] - cuts[index])
        for peer in col_peers:
            send(src.at[at, slab(peer)], target.at[col, at, :], ssem, rsem.at[index], col=peer)

    others = pl.ds(0, cols - 1)

    def piece_of(target, marks, index):
        return target.at[others, pl.ds(marks[index], marks[index + 1] - marks[index]), :]

    for peer in col_peers:
        send(energy.at[:, slab(peer)], ez.at[col], e_sems.at[0], e_sems.at[1], col=peer)
    for copy in pulls:
        copy.wait()

    @pl.loop(0, cells // 16)
    def _(i):
        at = pl.ds(pl.multiple_of(i * 16, 16), 16)
        old = damage_old[at, :]
        seeded = crack_seeds[at, :] == 1
        start[at, :] = jnp.where(seeded, 1.0, old)
        bound[at, :] = jnp.where(seeded, 1.0, jnp.where(irreversible[at, :] == 1, old, 0.0))

    order = (0, 4, 1, 2, 3)
    for n in order:
        move_piece(start, landing, n, d_ssem.at[0], d_rsem)
    for n in order[:2]:
        move_piece(bound, fz, n, f_ssem.at[0], f_rsem)
    landing[col] = start[:, slab(col)]
    fz[col] = bound[:, slab(col)]

    lane = lax.broadcasted_iota(jnp.int32, (8, 128), 1)
    sub = lax.broadcasted_iota(jnp.int32, (8, 128), 0)
    upper_half = sub < planes
    zero = jnp.zeros((8, 128), f32)
    for copy in fetch:
        copy.wait()

    def lane_of(a, n):
        return jnp.broadcast_to(a[:, n : n + 1], (8, 128))

    def corner_of(down, over, k):
        tile = inverse[k, (cells - 8) * down : (cells - 8) * down + 8, (cells - 128) * over : (cells - 128) * over + 128]
        at = (7 if down else 0, 127 if over else 0)
        return jnp.broadcast_to(tile[at[0] : at[0] + 1, at[1] : at[1] + 1], (8, 128))

    def hot(index):
        return jnp.where(lane == index, 1.0, 0.0)

    def carries(first, final_of, lower=None, upper=None):
        firsts, finals = [], []
        low = [None if lower is None else lower(k) for k in range(blocks)]
        high = [None if upper is None else upper(k) for k in range(blocks)]
        for k in range(blocks):
            begin, end = hot(first(k)), hot(final_of(k))
            if low[k] is not None:
                begin = begin + corner_of(0, 0, k) * hot(low[k])
                end = end + corner_of(1, 0, k) * hot(low[k])
            if high[k] is not None:
                begin = begin + corner_of(0, 1, k) * hot(high[k])
                end = end + corner_of(1, 1, k) * hot(high[k])
            firsts.append(begin)
            finals.append(end)
        incoming = [zero]
        for k in range(blocks - 1):
            incoming.append(finals[k] + COUPLE * corner_of(1, 0, k) * incoming[k])
        heads = [
            firsts[k] + COUPLE * corner_of(0, 0, k) * incoming[k] for k in range(blocks)
        ]
        carried = heads[blocks - 1]
        outgoing = [zero] * blocks
        for k in range(blocks - 2, -1, -1):
            outgoing[k] = carried
            carried = heads[k] + COUPLE * corner_of(0, 1, k) * carried
        enter, leave = [], []
        for k in range(blocks):
            enter.append(COUPLE * incoming[k] + (zero if low[k] is None else hot(low[k])))
            leave.append(COUPLE * outgoing[k] + (zero if high[k] is None else hot(high[k])))
        return incoming, outgoing, enter, leave

    def picked(which, options):
        total = zero
        for n, option in enumerate(options):
            if option is not None:
                total = total + jnp.where(which == n, option, 0.0)
        return total

    def at_own(c, weights):
        return pltpu.roll(weights, 128 - 8 * c, 1) if c > 0 else weights

    def left_of(k):
        c = k // x_blocks
        return 8 * (c - 1) + 2 * x_blocks + 1 if k % x_blocks == 0 and c > 0 else None

    def right_of(k):
        c = k // x_blocks
        return 8 * (c + 1) + 2 * x_blocks if k % x_blocks == x_blocks - 1 and c < cols - 1 else None

    incoming, outgoing, enter, leave = carries(
        lambda k: 8 * (k // x_blocks) + k % x_blocks,
        lambda k: 8 * (k // x_blocks) + x_blocks + k % x_blocks,
        left_of,
        right_of,
    )
    to_right = picked(col, [
        at_own(c, incoming[(c + 1) * x_blocks] + hot(8 * c + 2 * x_blocks + 1) / COUPLE)
        if c < cols - 1 else None
        for c in range(cols)
    ])
    to_left = picked(col, [
        at_own(c, leave[c * x_blocks - 1] / COUPLE) if c > 0 else None for c in range(cols)
    ])
    for n in range(kinds):
        wx_send[n] = jnp.where(upper_half, lane_of(to_right, n), lane_of(to_left, n))
    for m in range(2 * x_blocks):
        table = (enter, leave)[m % 2]
        everywhere = picked(col, [table[c * x_blocks + m // 2] for c in range(cols)])
        here = picked(col, [at_own(c, table[c * x_blocks + m // 2]) for c in range(cols)])
        for c in range(cols):
            from_left = jnp.where(col > c, lane_of(everywhere, 8 * c + 2 * x_blocks - 1), 0.0)
            from_right = jnp.where(col < c, lane_of(everywhere, 8 * c), 0.0)
            wx_in[m, c] = jnp.where(upper_half, from_left, from_right)
        for n in range(kinds):
            wx_own[m, n] = lane_of(here, n)

    incoming, outgoing, enter, leave = carries(lambda k: 2 * k, lambda k: 2 * k + 1)
    enters, leaves = picked(row, enter), picked(row, leave)
    for k in range(rows):
        wy_in[0, k] = lane_of(enters, 2 * k + 1)
        wy_in[1, k] = jnp.where(row >= k, lane_of(leaves, 2 * k + 1), lane_of(leaves, 2 * k))
    wy_turn[...] = picked(
        row, [lane_of(outgoing[k - 1], 2 * k + 1) if k > 0 else None for k in range(rows)]
    )

    upper_wide = lax.broadcasted_iota(jnp.int32, (8, cells), 0) < planes
    for j in range(x_blocks):
        turned = inverse[col * x_blocks + j].T
        gx_high[j], gx_low[j] = split(turned)
        for side, at in ((0, 0), (1, last)):
            line = jnp.broadcast_to(turned[at : at + 1], (8, cells))
            gend[side, j] = line
            if j == 0:
                gend[side, x_blocks] = line
            else:
                gend[side, x_blocks] = jnp.where(upper_wide, gend[side, x_blocks], line)
    gy = inverse[row]
    gy_both[:cells], gy_both[cells:] = split(gy)
    gy_ends[0] = jnp.broadcast_to(gy[:, :1], (cells, 128))
    gy_ends[1] = jnp.broadcast_to(gy[:, last:], (cells, 128))

    for k in range(blocks):
        for side, at in ((0, 0), (1, 127)):
            strip = inverse[k, :, (cells - 128) * side : (cells - 128) * side + 128]
            line = strip.T[at : at + 1]
            g_all[side, k] = jnp.broadcast_to(line, (8, cells))

    @pl.when(above)
    def _():
        pl.semaphore_wait(greet.at[0], 1)

    @pl.when(below)
    def _():
        signal_row(greet.at[0], row + 1)
        pl.semaphore_wait(greet.at[1], 1)

    @pl.when(above)
    def _():
        signal_row(greet.at[1], row - 1)

    first_col = jnp.where(col == 0, 1.0, 0.0)
    last_col = jnp.where(col == cols - 1, 1.0, 0.0)
    lane16 = lax.broadcasted_iota(jnp.int32, (16, 128), 1)
    at_first, at_last = lane16 == 0, lane16 == 127

    mixing = [[KAPPA * z_inv[z, k] for k in range(planes)] for z in range(planes)]
    for k in range(planes):
        weights = zero
        for z in range(planes):
            weights = jnp.where(lax.rem(sub, planes) == z, mixing[z][k], weights)
        w_mix[k] = weights

    def scale_energy():
        @pl.loop(0, cells // 8)
        def _(i):
            for z in range(planes):
                sides = 4 + (z > 0) + (z < planes - 1)
                scaled = ez[z, eight(i * 8), :] * (1.0 / KAPPA)
                ez[z, eight(i * 8), :] = scaled
                ec[z, eight(i * 8), :] = scaled + (1.0 / KAPPA + sides)

    def regroup(low, high):
        @pl.loop(low // 8, high // 8)
        def _(i):
            for z in range(planes):
                tile = landing[z, eight(i * 8), :]
                for g in range(groups):
                    dz[0, z, g, eight(i * 8 + 8), :] = tile[:, g * 128 : (g + 1) * 128]

    def share_rows(it):
        send(dz.at[it, :, :, pl.ds(cells, 8), :], dz.at[it, :, :, pl.ds(0, 8), :],
             v_sems.at[0, it], v_sems.at[1, it], row=lax.rem(row + 1, rows))
        send(dz.at[it, :, :, pl.ds(8, 8), :], dz.at[it, :, :, pl.ds(cells + 8, 8), :],
             v_sems.at[0, it], v_sems.at[1, it], row=lax.rem(row + rows - 1, rows))

    def two_rows(it):
        return dz.at[it, :, :, pl.ds(0, 16), :]

    def mirror(it):
        for z in range(planes):
            for g in range(groups):
                dz[it, z, g, 7:8, :] = jnp.where(
                    row == 0, dz[it, z, g, 8:9, :], dz[it, z, g, 7:8, :]
                )
                dz[it, z, g, cells + 8 : cells + 9, :] = jnp.where(
                    row == rows - 1,
                    dz[it, z, g, cells + 7 : cells + 8, :],
                    dz[it, z, g, cells + 8 : cells + 9, :],
                )

    def residual(it, low, high):
        @pl.loop(low // 16, high // 16)
        def _(i):
            base = pl.multiple_of(i * 16, 16)
            here = pl.ds(base, 16)
            padded = pl.ds(pl.multiple_of(base + 8, 8), 16)
            for g in range(groups):
                lanes = slice(g * 128, (g + 1) * 128)
                mids = [dz[it, z, g, padded, :] for z in range(planes)]
                value = []
                for z in range(planes):
                    d = mids[z]
                    near = dz[it, z, g, pl.ds(base + 7, 16), :] + dz[it, z, g, pl.ds(base + 9, 16), :]
                    before = d * first_col
                    if g > 0:
                        before = pltpu.roll(dz[it, z, g - 1, padded, :], 1, 1)
                    after = d * last_col
                    if g < groups - 1:
                        after = pltpu.roll(dz[it, z, g + 1, padded, :], 127, 1)
                    near = near + jnp.where(at_first, before, pltpu.roll(d, 1, 1))
                    near = near + jnp.where(at_last, after, pltpu.roll(d, 127, 1))
                    if z > 0:
                        near = near + mids[z - 1]
                    if z < planes - 1:
                        near = near + mids[z + 1]
                    value.append(near + (ez[z, here, lanes] - ec[z, here, lanes] * d))
                for z in range(planes):
                    total = mixing[z][0] * value[0]
                    for k in range(1, planes):
                        total = total + mixing[z][k] * value[k]
                    w_high[z, here, lanes], w_low[z, here, lanes] = split(total)

    def x_product(it, ranges):
        packs = [jnp.zeros((b - a, 128), f32) for a, b in ranges]
        spots = [lax.broadcasted_iota(jnp.int32, (b - a, 128), 1) for a, b in ranges]

        def place(n, tile, lane_from, lane_to):
            if lane_from != lane_to:
                tile = pltpu.roll(tile, (lane_to - lane_from) % 128, 1)
            packs[n] = jnp.where(spots[n] == lane_to, tile, packs[n])

        for j in range(x_blocks):
            block = slice(j * cells, (j + 1) * cells)
            parts = [(z, n) for z in range(planes) for n in range(len(ranges))]
            cut = [slice(*ranges[n]) for _, n in parts]
            high_rows = jnp.concatenate(
                [w_high[z, c, block] for (z, _), c in zip(parts, cut)], axis=0
            )
            low_rows = jnp.concatenate(
                [w_low[z, c, block] for (z, _), c in zip(parts, cut)], axis=0
            )
            count = high_rows.shape[0]
            twice = dot(jnp.concatenate([high_rows, low_rows], axis=0), gx_high[j])
            along = twice[:count] + (twice[count:] + dot(high_rows, gx_low[j]))
            at = 0
            for (z, n), c in zip(parts, cut):
                part = along[at : at + c.stop - c.start]
                at += c.stop - c.start
                a_high[z, c, block], a_low[z, c, block] = split(part)
                place(n, part[:, :128], 0, j * planes + z)
                place(n, part[:, cells - 128 :], 127, (x_blocks + j) * planes + z)
        for n, (a, b) in enumerate(ranges):
            for z in range(planes):
                near = pl.ds(8 + a, b - a)
                place(n, dz[it, z, 0, near, :], 0, 2 * x_blocks * planes + z)
                place(n, dz[it, z, groups - 1, near, :], 127, (2 * x_blocks + 1) * planes + z)
            packed[a:b, :] = packs[n]

    def y_times(high, low):
        twice = dot(gy_both[...], high)
        return twice[:cells] + (twice[cells:] + dot(gy_both[:cells], low))

    def y_product(it, z):
        both = y_times(a_high[z], a_low[z])
        mix[z] = both
        for side, at in ((0, 0), (1, last)):
            for j in range(x_blocks):
                y_base[side, z, j : j + 1, :] = both[at : at + 1, j * cells : (j + 1) * cells]
        if it + 1 == ITERS:
            d = jnp.concatenate([dz[it, z, g, pl.ds(8, cells), :] for g in range(groups)], axis=1)
            final[z] = d + STEP * both

    def x_ends():
        turned = y_times(*split(packed[...])).T

        def keep(n, tile):
            other = pltpu.roll(tile, planes, 0)
            pair = (tile, other) if n % 2 == 0 else (other, tile)
            own_rows[n] = jnp.where(upper_wide, pair[0], pair[1])

        for n in range(2 * x_blocks):
            keep(n, turned[8 * (n // 2) : 8 * (n // 2) + 8])
        tile = turned[8 * x_blocks : 8 * x_blocks + 8]
        total = None
        for k in range(planes):
            line = jnp.where(
                upper_wide,
                jnp.broadcast_to(tile[k : k + 1], (8, cells)),
                jnp.broadcast_to(tile[planes + k : planes + k + 1], (8, cells)),
            )
            term = wide(w_mix[k]) * line
            total = term if total is None else total + term
        for n in range(2):
            keep(2 * x_blocks + n, total)

    def wide(weights):
        return jnp.concatenate([weights] * (cells // 128), axis=1)

    def x_share(it):
        total = None
        for n in range(kinds):
            term = wide(wx_send[n]) * own_rows[n]
            total = term if total is None else total + term
        x_send[it] = total
        x_all[it, col] = total
        for peer in col_peers:
            send(x_send.at[it], x_all.at[it, col], x_sems.at[0, it], x_sems.at[1, it], col=peer)

    def y_share(it):
        sides = []
        for side in range(2):
            parts = []
            for j in range(x_blocks):
                m = 2 * j + side
                total = wide(wx_in[m, 0]) * x_all[it, 0]
                for c in range(1, cols):
                    total = total + wide(wx_in[m, c]) * x_all[it, c]
                total = total + pltpu.roll(total, planes, 0)
                for n in range(kinds):
                    total = total + wide(wx_own[m, n]) * own_rows[n]
                parts.append(total)
            sides.append(jnp.where(upper_wide, parts[0], parts[1]))
        lines = []
        for side, at in ((0, 0), (1, last)):
            line = jnp.concatenate(
                [y_base[side, z, j : j + 1, :] for j in range(x_blocks) for z in range(planes)],
                axis=0,
            )
            for n in range(2):
                scale = jnp.broadcast_to(sides[n][:, at : at + 1], (8, cells))
                line = line + scale * gend[n, x_blocks]
            lines.append(line)
        y_send[it, 0] = lines[1]
        y_send[it, 1] = lines[0] + wide(wy_turn[...]) * lines[1]
        y_all[it, row] = lines[1]
        for n, peer in enumerate(row_peers):
            send(y_send.at[it, lax.div(row + n + 1, rows)], y_all.at[it, row], y_sems.at[0, it],
                 y_sems.at[1, it], row=peer)
        stacked = jnp.concatenate(sides + [jnp.zeros((112, cells), f32)], axis=0).T
        for t in range(cells // 8):
            here = slice(t * 8, t * 8 + 8)
            tile = stacked[here]
            for z in range(planes):
                for j in range(x_blocks):
                    block = slice(j * cells, (j + 1) * cells)
                    n = j * planes + z
                    mix[z, here, block] = (
                        mix[z, here, block]
                        + tile[:, n : n + 1] * gend[0, j]
                        + tile[:, 8 + n : 9 + n] * gend[1, j]
                    )
        finish(y_sems.at[1, it], y_all.at[it, pl.ds(0, rows - 1)])
        carried = []
        for side in range(2):
            total = wide(wy_in[side, 0]) * y_all[it, 0]
            for k in range(1, rows):
                total = total + wide(wy_in[side, k]) * y_all[it, k]
            for z in range(planes):
                for j in range(x_blocks):
                    n = j * planes + z
                    carry_rows[2 * z + side, :, j * cells : (j + 1) * cells] = jnp.broadcast_to(
                        total[n : n + 1], (8, cells)
                    )
            carried.append(total)
        return sides, carried

    def settle(it, low, high, squares):
        def step(i, acc):
            here, padded = eight(i * 8), eight(i * 8 + 8)
            g_first = jnp.concatenate([gy_ends[0, here, :]] * groups, axis=1)
            g_last = jnp.concatenate([gy_ends[1, here, :]] * groups, axis=1)
            for z in range(planes):
                solved = mix[z, here, :] + g_first * carry_rows[2 * z] + g_last * carry_rows[2 * z + 1]
                d = jnp.concatenate([dz[it, z, g, padded, :] for g in range(groups)], axis=1)
                renewed = jnp.minimum(jnp.maximum(d + STEP * solved, fz[z, here, :]), 1.0)
                if it + 1 < ITERS:
                    for g in range(groups):
                        dz[it + 1, z, g, padded, :] = renewed[:, g * 128 : (g + 1) * 128]
                change = renewed - d
                acc = acc + change * change
            return acc

        return lax.fori_loop(low // 8, high // 8, step, squares)

    def stream(it, ready):
        ready(order[0])
        ready(order[1])
        share_rows(it)
        a = 16
        for n in order[2:]:
            ready(n)
            b = cuts[n + 1] - 16
            if n == order[-1]:
                b += 32
            residual(it, a, b)
            x_product(it, [(a, b)])
            a = b
            if n == order[2]:
                finish(v_sems.at[1, it], two_rows(it))
                mirror(it)
                residual(it, 0, 16)
                residual(it, cuts[4] + 16, cells)
                x_product(it, [(0, 16), (cuts[4] + 16, cells)])

    def arrived(n):
        finish(d_rsem.at[n], piece_of(landing, cuts, n))
        regroup(cuts[n], cuts[n + 1])

    finish(e_sems.at[1], ez.at[others])
    scale_energy()
    stream(0, arrived)
    x_ends()
    x_share(0)
    for n in order[2:]:
        move_piece(bound, fz, n, f_ssem.at[0], f_rsem)
    for z in range(planes):
        y_product(0, z)
    finish(x_sems.at[1, 0], x_all.at[0, others])
    y_share(0)

    totals = []
    blank = jnp.zeros((8, width), f32)
    held = [blank]

    def settled(n):
        finish(f_rsem.at[n], piece_of(fz, cuts, n))
        held.append(settle(0, cuts[n], cuts[n + 1], held.pop()))

    stream(1, settled)
    def give_back(n, m):
        at = pl.ds(backs_at[n], backs_at[n + 1] - backs_at[n])
        send(final.at[col_peers[m], at, :], out.at[at, slab(col)], back_ssem.at[0],
             back_rsem.at[n], col=col_peers[m])

    def give_all(n):
        for m in range(cols - 1):
            give_back(n, m)

    def complete(low, high):
        @pl.loop(low // 8, high // 8)
        def _(i):
            here = eight(i * 8)
            tile = x_cols[here, :]
            ends_of = [
                jnp.concatenate([gy_ends[n, here, :]] * (cells // 128), axis=1) for n in range(2)
            ]
            for k in range(blocks):
                block = slice(k * cells, (k + 1) * cells)
                n = 8 * (k // x_blocks) + 2 * (k % x_blocks)
                value = (
                    out[here, block]
                    + tile[:, n : n + 1] * g_all[0, k]
                    + tile[:, n + 1 : n + 2] * g_all[1, k]
                    + (ends_of[0] * y_lines[0, k] + ends_of[1] * y_lines[1, k])
                )
                out[here, block] = jnp.minimum(jnp.maximum(value, bound[here, block]), 1.0)

    for m in range(cols - 1):
        y_product(1, col_peers[m])
        give_back(0, m)
    x_ends()
    x_share(1)
    give_all(1)
    y_product(1, col)
    out[:, slab(col)] = final[col]
    finish(x_sems.at[1, 1], x_all.at[1, others])
    sides, carried = y_share(1)
    for z in range(planes):
        for j in range(x_blocks):
            n = j * planes + z
            for side in range(2):
                at = 2 * j + side
                word_send[z, at : at + 1, :] = STEP * sides[side][n : n + 1]
                at += 2 * x_blocks
                word_send[z, at : at + 1, :] = STEP * carried[side][n : n + 1]
    for peer in col_peers:
        send(word_send.at[peer], word_all.at[col], w_sems.at[0], w_sems.at[1], col=peer)
    give_all(2)
    word_all[col] = word_send[col]
    totals.append(jnp.sum(held[0]))
    totals.append(jnp.sum(settle(ITERS - 1, 0, cells, blank)))
    s_send[...] = jnp.where(sub == 0, totals[0], jnp.where(sub == 1, totals[1], 0.0))
    for n, peer in enumerate(row_peers):
        send(s_send, s_row.at[n], s_sems.at[0], s_sems.at[1], row=peer)
    finish(s_sems.at[1], s_row)
    total = s_send[...]
    for n in range(rows - 1):
        total = total + s_row[n]
    s_col_send[...] = total
    for n, peer in enumerate(col_peers):
        send(s_col_send, s_col.at[n], s_sems.at[2], s_sems.at[3], col=peer)
    for n in range(3, len(backs_at) - 1):
        give_all(n)
    finish(w_sems.at[1], word_all.at[others])
    x_cols[...] = jnp.concatenate(
        [word_all[c] for c in range(cols)] + [jnp.zeros((128 - 8 * cols, cells), f32)], axis=0
    ).T
    for k in range(blocks):
        for side in range(2):
            at = 2 * x_blocks + 2 * (k % x_blocks) + side
            y_lines[side, k] = jnp.broadcast_to(
                word_all[k // x_blocks, at : at + 1, :], (8, cells)
            )
    for n in range(len(backs_at) - 2):
        finish(back_rsem.at[n], piece_of(final, backs_at, n))
        complete(backs_at[n], backs_at[n + 1])
    finish(s_sems.at[3], s_col)
    for n in range(cols - 1):
        total = total + s_col[n]
    sizes = jnp.sqrt(total / cell_count + EPSILON) / STEP
    norms[...] = jnp.where(lane == 0, sizes[:1, :], sizes[1:2, :])[0, :ITERS]
    for it in range(ITERS):
        finish(x_sems.at[0, it], x_all.at[it, others])
        finish(y_sems.at[0, it], y_all.at[it, pl.ds(0, rows - 1)])
        finish(v_sems.at[0, it], two_rows(it))
    finish(e_sems.at[0], ez.at[others])
    finish(d_ssem.at[0], landing.at[others])
    finish(f_ssem.at[0], fz.at[others])
    finish(w_sems.at[0], word_all.at[others])
    finish(s_sems.at[0], s_row)
    finish(s_sems.at[2], s_col)
    n = len(backs_at) - 2
    finish(back_rsem.at[n], piece_of(final, backs_at, n))
    complete(backs_at[n], backs_at[n + 1])
    finish(back_ssem.at[0], final.at[others])


def local(energy, damage_old, crack_seeds, irreversible, line_inverses, z_inverse):
    planes, cells, line_length = energy.shape
    rows, cols = lax.axis_size("row"), lax.axis_size("col")
    blocks, _, _ = line_inverses.shape
    width = line_length // cols
    x_blocks = width // cells
    kinds = 2 * x_blocks + 2
    step = cells // 16
    cuts = (0, 3 * step, 8 * step, 12 * step, 13 * step, cells)
    backs_at = (0, 2 * step, 8 * step, 12 * step, 15 * step, cells)
    cell_count = float(cols * rows * cells * line_length)
    shape = (rows, cols, cells, width, x_blocks, blocks, cell_count, cuts, backs_at)
    f32 = jnp.float32
    bf16 = jnp.bfloat16
    dma = pltpu.SemaphoreType.DMA
    vmem = pl.BlockSpec(memory_space=pltpu.VMEM)
    damage, norms = pl.pallas_call(
        functools.partial(line_kernel, shape),
        out_shape=(
            pltpu.VMEM((cells, line_length), f32),
            pltpu.VMEM((ITERS,), f32),
        ),
        in_specs=[pl.BlockSpec(memory_space=pl.ANY)] * 6,
        out_specs=(vmem, vmem),
        scratch_shapes=[
            pltpu.VMEM((cells, line_length), f32),
            pltpu.VMEM((cells, line_length), jnp.int32),
            pltpu.VMEM((cells, line_length), jnp.int32),
            pltpu.VMEM((cells, line_length), f32),
            pltpu.VMEM((cells, line_length), f32),
            pltpu.VMEM((cols, cells, width), f32),
            pltpu.VMEM((cols, cells, width), f32),
            pltpu.VMEM((cols, cells, width), f32),
            pltpu.VMEM((cols, cells, width), f32),
            pltpu.VMEM((ITERS, cols, width // 128, cells + 16, 128), f32),
            pltpu.VMEM((cols, cells, width), f32),
            pltpu.VMEM((cols, cells, width), bf16),
            pltpu.VMEM((cols, cells, width), bf16),
            pltpu.VMEM((cols, cells, width), bf16),
            pltpu.VMEM((cols, cells, width), bf16),
            pltpu.VMEM((cols, cells, width), f32),
            pltpu.VMEM((blocks, cells, cells), f32),
            pltpu.VMEM((x_blocks, cells, cells), bf16),
            pltpu.VMEM((x_blocks, cells, cells), bf16),
            pltpu.VMEM((2 * cells, cells), bf16),
            pltpu.VMEM((2, cells, 128), f32),
            pltpu.VMEM((2, x_blocks + 1, 8, cells), f32),
            pltpu.VMEM((kinds, 8, 128), f32),
            pltpu.VMEM((2 * x_blocks, cols, 8, 128), f32),
            pltpu.VMEM((2 * x_blocks, kinds, 8, 128), f32),
            pltpu.VMEM((2, rows, 8, 128), f32),
            pltpu.VMEM((8, 128), f32),
            pltpu.VMEM((2 * cols, 8, width), f32),
            pltpu.VMEM((kinds, 8, cells), f32),
            pltpu.VMEM((cells, 128), f32),
            pltpu.VMEM((cols, 8, 128), f32),
            pltpu.VMEM((2, cols, 8, cells), f32),
            pltpu.VMEM((2, blocks, 8, cells), f32),
            pltpu.VMEM((cols, 8, cells), f32),
            pltpu.VMEM((cols, 8, cells), f32),
            pltpu.VMEM((cells, 128), f32),
            pltpu.VMEM((2, blocks, 8, cells), f32),
            pltpu.VMEM((ITERS, 8, cells), f32),
            pltpu.VMEM((ITERS, cols, 8, cells), f32),
            pltpu.VMEM((ITERS, 2, 8, cells), f32),
            pltpu.VMEM((ITERS, rows, 8, cells), f32),
            pltpu.VMEM((8, 128), f32),
            pltpu.VMEM((rows - 1, 8, 128), f32),
            pltpu.VMEM((8, 128), f32),
            pltpu.VMEM((cols - 1, 8, 128), f32),
            pltpu.SMEM((cols, cols), f32),
            dma((6,)),
            pltpu.SemaphoreType.REGULAR((2,)),
            dma((2,)),
            dma((1,)),
            dma((5,)),
            dma((1,)),
            dma((5,)),
            dma((1,)),
            dma((5,)),
            dma((2,)),
            dma((2, ITERS)),
            dma((2, ITERS)),
            dma((2, ITERS)),
            dma((4,)),
        ],
        compiler_params=pltpu.CompilerParams(
            has_side_effects=True, collective_id=0, vmem_limit_bytes=60 * 1024 * 1024
        ),
        name="line_iterations",
    )(
        z_inverse,
        energy[0],
        damage_old[0],
        crack_seeds[0],
        irreversible[0],
        line_inverses,
    )
    return damage[None], norms


def solution(mesh):
    def local_any(energy, damage_old, crack_seeds, irreversible, line_inverses, z_inverse):
        rows, cols = mesh.shape["row"], mesh.shape["col"]
        block_cells = line_inverses.shape[1]
        width = energy.shape[2] // cols
        whole_blocks = (
            energy.shape[0] == 1
            and energy.shape[1] == block_cells
            and width == 2 * block_cells
            and block_cells % 256 == 0
            and 2 * cols == 8
            and 2 * rows <= 128
            and min(rows, cols) > 2
        )
        chosen = local if whole_blocks else local_turned
        return chosen(energy, damage_old, crack_seeds, irreversible, line_inverses, z_inverse)

    return jax.shard_map(
        local_any,
        mesh=mesh,
        in_specs=(
            P("col", "row", None),
            P("col", "row", None),
            P("col", "row", None),
            P("col", "row", None),
            P(),
            P(),
        ),
        out_specs=(P("col", "row", None), P()),
        check_vma=False,
    )
```

```python
import functools

import jax
import jax.numpy as jnp
from jax import lax
from jax.experimental import pallas as pl
from jax.experimental.pallas import tpu as pltpu
from jax.sharding import PartitionSpec as P

ITERS = 2


KAPPA = 2.0
STEP = 0.02
COUPLE = 0.5
EPSILON = 1e-06
HIGHEST = lax.Precision.HIGHEST


def second_difference(grid_field, along):
    extent = grid_field.shape[along]
    forward_diff = lax.slice_in_dim(grid_field, 1, extent, axis=along) - lax.slice_in_dim(
        grid_field, 0, extent - 1, axis=along
    )
    zero_shape = list(grid_field.shape)
    zero_shape[along] = 1
    zero_rim = jnp.zeros(zero_shape, grid_field.dtype)
    ahead = jnp.concatenate([forward_diff, zero_rim], axis=along)
    behind = jnp.concatenate([zero_rim, forward_diff], axis=along)
    return ahead - behind


def line_solve(line_rows, inverses):
    block_count, block_cells, _ = inverses.shape
    line_count = line_rows.shape[0]
    blocks = line_rows.reshape(line_count, block_count, block_cells)
    products = jnp.einsum("rkb,kcb->rkc", blocks, inverses, precision=lax.Precision.HIGHEST)
    first_col = inverses[:, :, 0]
    last_col = inverses[:, :, block_cells - 1]
    incoming = [jnp.zeros((line_count,), line_rows.dtype)]
    for block_index in range(block_count - 1):
        incoming.append(
            products[:, block_index, block_cells - 1]
            + COUPLE * incoming[block_index] * inverses[block_index, block_cells - 1, 0]
        )
    inflow = jnp.stack(incoming, axis=1)
    forward = products + COUPLE * inflow[:, :, None] * first_col[None]
    head_terms = [jnp.zeros((line_count,), line_rows.dtype) for block_index in range(block_count)]
    carried = forward[:, block_count - 1, 0]
    for block_index in range(block_count - 2, -1, -1):
        head_terms[block_index] = carried
        carried = (
            forward[:, block_index, 0]
            + COUPLE * carried * inverses[block_index, 0, block_cells - 1]
        )
    outflow = jnp.stack(head_terms, axis=1)
    solved = forward + COUPLE * outflow[:, :, None] * last_col[None]
    return solved.reshape(line_count, block_count * block_cells)


def local_turned(energy, damage_old, crack_seeds, irreversible, line_inverses, z_inverse):
    planes, rows_here, line_length = energy.shape
    row_count = lax.axis_size("row")
    col_count = lax.axis_size("col")
    total_planes = planes * col_count
    cell_count = total_planes * rows_here * row_count * line_length
    seeded = crack_seeds == 1
    damage = jnp.where(seeded, 1.0, damage_old)
    lower_bound = jnp.where(irreversible == 1, damage_old, 0.0)
    own_sums = []
    for sweep_index in range(ITERS):
        local_lap = second_difference(damage, 2)
        partial_value = energy - (1.0 + energy) * damage + KAPPA * local_lap
        moved_part, moved_damage = (
            lax.all_to_all(
                lax.all_to_all(
                    jnp.swapaxes(partial_value, 1, 2),
                    "row",
                    split_axis=1,
                    concat_axis=2,
                    tiled=True,
                ),
                "col",
                split_axis=1,
                concat_axis=0,
                tiled=True,
            ),
            lax.all_to_all(
                lax.all_to_all(
                    jnp.swapaxes(damage, 1, 2), "row", split_axis=1, concat_axis=2, tiled=True
                ),
                "col",
                split_axis=1,
                concat_axis=0,
                tiled=True,
            ),
        )
        lap_rest = second_difference(moved_damage, 2) + second_difference(moved_damage, 0)
        turned = moved_part + KAPPA * lap_rest
        turned_shape = turned.shape
        along_y = line_solve(turned.reshape(-1, turned_shape[2]), line_inverses).reshape(
            turned_shape
        )
        along_z = jnp.einsum("zk,kxy->zxy", z_inverse, along_y, precision=lax.Precision.HIGHEST)
        gathered = lax.all_to_all(
            lax.all_to_all(along_z, "row", split_axis=2, concat_axis=1, tiled=True),
            "col",
            split_axis=0,
            concat_axis=1,
            tiled=True,
        )
        piece_cells = gathered.shape[1] // (row_count * col_count)
        reordered = gathered.reshape(planes, col_count, row_count, piece_cells, rows_here)
        restored = jnp.transpose(reordered, (0, 4, 2, 1, 3)).reshape(planes, rows_here, line_length)
        update = STEP * line_solve(restored.reshape(-1, line_length), line_inverses).reshape(
            restored.shape
        )
        clamped = jnp.minimum(jnp.maximum(damage + update, lower_bound), 1.0)
        renewed = jnp.where(seeded, 1.0, clamped)
        own_sum = jnp.sum((renewed - damage) ** 2)
        own_sums.append(own_sum)
        damage = renewed
    global_sums = lax.psum(jnp.stack(own_sums), ("row", "col"))
    update_norms = jnp.sqrt(global_sums / cell_count + EPSILON) / STEP
    return (damage, update_norms)


def line_kernel(
    shape,
    z_hbm,
    energy,
    damage_hbm,
    seeds_hbm,
    irreversible_hbm,
    inverses,
    out,
    norms,
    damage_old,
    crack_seeds,
    irreversible,
    start,
    bound,
    ez,
    ec,
    fz,
    landing,
    dz,
    final,
    w_high,
    w_low,
    a_high,
    a_low,
    mix,
    inverse,
    gx_high,
    gx_low,
    gy_both,
    gy_ends,
    gend,
    wx_send,
    wx_in,
    wx_own,
    wy_in,
    wy_turn,
    carry_rows,
    own_rows,
    w_mix,
    y_base,
    g_all,
    word_send,
    word_all,
    x_cols,
    y_lines,
    x_send,
    x_all,
    y_send,
    y_all,
    s_send,
    s_row,
    s_col_send,
    s_col,
    z_inv,
    local_sems,
    greet,
    e_sems,
    d_ssem,
    d_rsem,
    f_ssem,
    f_rsem,
    back_ssem,
    back_rsem,
    w_sems,
    x_sems,
    v_sems,
    y_sems,
    s_sems,
):
    rows, cols, cells, width, x_blocks, blocks, cell_count, cuts, backs_at = shape
    planes = cols
    last = cells - 1
    groups = width // 128
    kinds = 2 * x_blocks + 2
    f32 = jnp.float32
    row, col = lax.axis_index("row"), lax.axis_index("col")
    row_peers = [lax.rem(row + o, rows) for o in range(1, rows)]
    col_peers = [lax.rem(col + o, cols) for o in range(1, cols)]

    def slab(who):
        return pl.ds(pl.multiple_of(who * width, width), width)

    def eight(at):
        return pl.ds(pl.multiple_of(at, 8), 8)

    def send(src, dst, ssem, rsem, **where):
        copy = pltpu.make_async_remote_copy(
            src_ref=src, dst_ref=dst, send_sem=ssem, recv_sem=rsem,
            device_id=where, device_id_type=pl.DeviceIdType.MESH,
        )
        copy.start()
        return copy

    def finish(sem, sized):
        pltpu.make_async_copy(sized, sized, sem).wait()

    def split(a):
        high = a.astype(jnp.bfloat16)
        return high, (a - high.astype(f32)).astype(jnp.bfloat16)

    def dot(a, b):
        return jnp.dot(a, b, preferred_element_type=f32)

    barrier = pltpu.get_barrier_semaphore()
    for peer in col_peers:
        pl.semaphore_signal(
            barrier, inc=1, device_id={"col": peer}, device_id_type=pl.DeviceIdType.MESH
        )
    above, below = row > 0, row < rows - 1

    def signal_row(sem, who):
        pl.semaphore_signal(
            sem, inc=1, device_id={"row": who}, device_id_type=pl.DeviceIdType.MESH
        )

    @pl.when(above)
    def _():
        signal_row(barrier, row - 1)

    @pl.when(below)
    def _():
        signal_row(barrier, row + 1)

    pulls = [
        pltpu.make_async_copy(damage_hbm, damage_old, local_sems.at[0]),
        pltpu.make_async_copy(seeds_hbm, crack_seeds, local_sems.at[1]),
        pltpu.make_async_copy(irreversible_hbm, irreversible, local_sems.at[2]),
    ]
    fetch = [
        pltpu.make_async_copy(energy.at[:, slab(col)], ez.at[col], local_sems.at[3]),
        pltpu.make_async_copy(inverses, inverse, local_sems.at[4]),
        pltpu.make_async_copy(z_hbm, z_inv, local_sems.at[5]),
    ]
    for copy in pulls + fetch:
        copy.start()
    neighbours = jnp.where(above, 1, 0) + jnp.where(below, 1, 0)
    pl.semaphore_wait(barrier, cols - 1 + neighbours)

    def move_piece(src, target, index, ssem, rsem):
        at = pl.ds(cuts[index], cuts[index + 1] - cuts[index])
        for peer in col_peers:
            send(src.at[at, slab(peer)], target.at[col, at, :], ssem, rsem.at[index], col=peer)

    others = pl.ds(0, cols - 1)

    def piece_of(target, marks, index):
        return target.at[others, pl.ds(marks[index], marks[index + 1] - marks[index]), :]

    for peer in col_peers:
        send(energy.at[:, slab(peer)], ez.at[col], e_sems.at[0], e_sems.at[1], col=peer)
    for copy in pulls:
        copy.wait()

    @pl.loop(0, cells // 16)
    def _(i):
        at = pl.ds(pl.multiple_of(i * 16, 16), 16)
        old = damage_old[at, :]
        seeded = crack_seeds[at, :] == 1
        start[at, :] = jnp.where(seeded, 1.0, old)
        bound[at, :] = jnp.where(seeded, 1.0, jnp.where(irreversible[at, :] == 1, old, 0.0))

    order = (0, 4, 1, 2, 3)
    for n in order:
        move_piece(start, landing, n, d_ssem.at[0], d_rsem)
    for n in order[:2]:
        move_piece(bound, fz, n, f_ssem.at[0], f_rsem)
    landing[col] = start[:, slab(col)]
    fz[col] = bound[:, slab(col)]

    lane = lax.broadcasted_iota(jnp.int32, (8, 128), 1)
    sub = lax.broadcasted_iota(jnp.int32, (8, 128), 0)
    upper_half = sub < planes
    zero = jnp.zeros((8, 128), f32)
    for copy in fetch:
        copy.wait()

    def lane_of(a, n):
        return jnp.broadcast_to(a[:, n : n + 1], (8, 128))

    def corner_of(down, over, k):
        tile = inverse[k, (cells - 8) * down : (cells - 8) * down + 8, (cells - 128) * over : (cells - 128) * over + 128]
        at = (7 if down else 0, 127 if over else 0)
        return jnp.broadcast_to(tile[at[0] : at[0] + 1, at[1] : at[1] + 1], (8, 128))

    def hot(index):
        return jnp.where(lane == index, 1.0, 0.0)

    def carries(first, final_of, lower=None, upper=None):
        firsts, finals = [], []
        low = [None if lower is None else lower(k) for k in range(blocks)]
        high = [None if upper is None else upper(k) for k in range(blocks)]
        for k in range(blocks):
            begin, end = hot(first(k)), hot(final_of(k))
            if low[k] is not None:
                begin = begin + corner_of(0, 0, k) * hot(low[k])
                end = end + corner_of(1, 0, k) * hot(low[k])
            if high[k] is not None:
                begin = begin + corner_of(0, 1, k) * hot(high[k])
                end = end + corner_of(1, 1, k) * hot(high[k])
            firsts.append(begin)
            finals.append(end)
        incoming = [zero]
        for k in range(blocks - 1):
            incoming.append(finals[k] + COUPLE * corner_of(1, 0, k) * incoming[k])
        heads = [
            firsts[k] + COUPLE * corner_of(0, 0, k) * incoming[k] for k in range(blocks)
        ]
        carried = heads[blocks - 1]
        outgoing = [zero] * blocks
        for k in range(blocks - 2, -1, -1):
            outgoing[k] = carried
            carried = heads[k] + COUPLE * corner_of(0, 1, k) * carried
        enter, leave = [], []
        for k in range(blocks):
            enter.append(COUPLE * incoming[k] + (zero if low[k] is None else hot(low[k])))
            leave.append(COUPLE * outgoing[k] + (zero if high[k] is None else hot(high[k])))
        return incoming, outgoing, enter, leave

    def picked(which, options):
        total = zero
        for n, option in enumerate(options):
            if option is not None:
                total = total + jnp.where(which == n, option, 0.0)
        return total

    def at_own(c, weights):
        return pltpu.roll(weights, 128 - 8 * c, 1) if c > 0 else weights

    def left_of(k):
        c = k // x_blocks
        return 8 * (c - 1) + 2 * x_blocks + 1 if k % x_blocks == 0 and c > 0 else None

    def right_of(k):
        c = k // x_blocks
        return 8 * (c + 1) + 2 * x_blocks if k % x_blocks == x_blocks - 1 and c < cols - 1 else None

    incoming, outgoing, enter, leave = carries(
        lambda k: 8 * (k // x_blocks) + k % x_blocks,
        lambda k: 8 * (k // x_blocks) + x_blocks + k % x_blocks,
        left_of,
        right_of,
    )
    to_right = picked(col, [
        at_own(c, incoming[(c + 1) * x_blocks] + hot(8 * c + 2 * x_blocks + 1) / COUPLE)
        if c < cols - 1 else None
        for c in range(cols)
    ])
    to_left = picked(col, [
        at_own(c, leave[c * x_blocks - 1] / COUPLE) if c > 0 else None for c in range(cols)
    ])
    for n in range(kinds):
        wx_send[n] = jnp.where(upper_half, lane_of(to_right, n), lane_of(to_left, n))
    for m in range(2 * x_blocks):
        table = (enter, leave)[m % 2]
        everywhere = picked(col, [table[c * x_blocks + m // 2] for c in range(cols)])
        here = picked(col, [at_own(c, table[c * x_blocks + m // 2]) for c in range(cols)])
        for c in range(cols):
            from_left = jnp.where(col > c, lane_of(everywhere, 8 * c + 2 * x_blocks - 1), 0.0)
            from_right = jnp.where(col < c, lane_of(everywhere, 8 * c), 0.0)
            wx_in[m, c] = jnp.where(upper_half, from_left, from_right)
        for n in range(kinds):
            wx_own[m, n] = lane_of(here, n)

    incoming, outgoing, enter, leave = carries(lambda k: 2 * k, lambda k: 2 * k + 1)
    enters, leaves = picked(row, enter), picked(row, leave)
    for k in range(rows):
        wy_in[0, k] = lane_of(enters, 2 * k + 1)
        wy_in[1, k] = jnp.where(row >= k, lane_of(leaves, 2 * k + 1), lane_of(leaves, 2 * k))
    wy_turn[...] = picked(
        row, [lane_of(outgoing[k - 1], 2 * k + 1) if k > 0 else None for k in range(rows)]
    )

    upper_wide = lax.broadcasted_iota(jnp.int32, (8, cells), 0) < planes
    for j in range(x_blocks):
        turned = inverse[col * x_blocks + j].T
        gx_high[j], gx_low[j] = split(turned)
        for side, at in ((0, 0), (1, last)):
            line = jnp.broadcast_to(turned[at : at + 1], (8, cells))
            gend[side, j] = line
            if j == 0:
                gend[side, x_blocks] = line
            else:
                gend[side, x_blocks] = jnp.where(upper_wide, gend[side, x_blocks], line)
    gy = inverse[row]
    gy_both[:cells], gy_both[cells:] = split(gy)
    gy_ends[0] = jnp.broadcast_to(gy[:, :1], (cells, 128))
    gy_ends[1] = jnp.broadcast_to(gy[:, last:], (cells, 128))

    for k in range(blocks):
        for side, at in ((0, 0), (1, 127)):
            strip = inverse[k, :, (cells - 128) * side : (cells - 128) * side + 128]
            line = strip.T[at : at + 1]
            g_all[side, k] = jnp.broadcast_to(line, (8, cells))

    @pl.when(above)
    def _():
        pl.semaphore_wait(greet.at[0], 1)

    @pl.when(below)
    def _():
        signal_row(greet.at[0], row + 1)
        pl.semaphore_wait(greet.at[1], 1)

    @pl.when(above)
    def _():
        signal_row(greet.at[1], row - 1)

    first_col = jnp.where(col == 0, 1.0, 0.0)
    last_col = jnp.where(col == cols - 1, 1.0, 0.0)
    lane16 = lax.broadcasted_iota(jnp.int32, (16, 128), 1)
    at_first, at_last = lane16 == 0, lane16 == 127

    mixing = [[KAPPA * z_inv[z, k] for k in range(planes)] for z in range(planes)]
    for k in range(planes):
        weights = zero
        for z in range(planes):
            weights = jnp.where(lax.rem(sub, planes) == z, mixing[z][k], weights)
        w_mix[k] = weights

    def scale_energy():
        @pl.loop(0, cells // 8)
        def _(i):
            for z in range(planes):
                sides = 4 + (z > 0) + (z < planes - 1)
                scaled = ez[z, eight(i * 8), :] * (1.0 / KAPPA)
                ez[z, eight(i * 8), :] = scaled
                ec[z, eight(i * 8), :] = scaled + (1.0 / KAPPA + sides)

    def regroup(low, high):
        @pl.loop(low // 8, high // 8)
        def _(i):
            for z in range(planes):
                tile = landing[z, eight(i * 8), :]
                for g in range(groups):
                    dz[0, z, g, eight(i * 8 + 8), :] = tile[:, g * 128 : (g + 1) * 128]

    def share_rows(it):
        send(dz.at[it, :, :, pl.ds(cells, 8), :], dz.at[it, :, :, pl.ds(0, 8), :],
             v_sems.at[0, it], v_sems.at[1, it], row=lax.rem(row + 1, rows))
        send(dz.at[it, :, :, pl.ds(8, 8), :], dz.at[it, :, :, pl.ds(cells + 8, 8), :],
             v_sems.at[0, it], v_sems.at[1, it], row=lax.rem(row + rows - 1, rows))

    def two_rows(it):
        return dz.at[it, :, :, pl.ds(0, 16), :]

    def mirror(it):
        for z in range(planes):
            for g in range(groups):
                dz[it, z, g, 7:8, :] = jnp.where(
                    row == 0, dz[it, z, g, 8:9, :], dz[it, z, g, 7:8, :]
                )
                dz[it, z, g, cells + 8 : cells + 9, :] = jnp.where(
                    row == rows - 1,
                    dz[it, z, g, cells + 7 : cells + 8, :],
                    dz[it, z, g, cells + 8 : cells + 9, :],
                )

    def residual(it, low, high):
        @pl.loop(low // 16, high // 16)
        def _(i):
            base = pl.multiple_of(i * 16, 16)
            here = pl.ds(base, 16)
            padded = pl.ds(pl.multiple_of(base + 8, 8), 16)
            for g in range(groups):
                lanes = slice(g * 128, (g + 1) * 128)
                mids = [dz[it, z, g, padded, :] for z in range(planes)]
                value = []
                for z in range(planes):
                    d = mids[z]
                    near = dz[it, z, g, pl.ds(base + 7, 16), :] + dz[it, z, g, pl.ds(base + 9, 16), :]
                    before = d * first_col
                    if g > 0:
                        before = pltpu.roll(dz[it, z, g - 1, padded, :], 1, 1)
                    after = d * last_col
                    if g < groups - 1:
                        after = pltpu.roll(dz[it, z, g + 1, padded, :], 127, 1)
                    near = near + jnp.where(at_first, before, pltpu.roll(d, 1, 1))
                    near = near + jnp.where(at_last, after, pltpu.roll(d, 127, 1))
                    if z > 0:
                        near = near + mids[z - 1]
                    if z < planes - 1:
                        near = near + mids[z + 1]
                    value.append(near + (ez[z, here, lanes] - ec[z, here, lanes] * d))
                for z in range(planes):
                    total = mixing[z][0] * value[0]
                    for k in range(1, planes):
                        total = total + mixing[z][k] * value[k]
                    w_high[z, here, lanes], w_low[z, here, lanes] = split(total)

    def x_product(ranges):
        for j in range(x_blocks):
            block = slice(j * cells, (j + 1) * cells)
            parts = [(z, n) for z in range(planes) for n in range(len(ranges))]
            cut = [slice(*ranges[n]) for _, n in parts]
            high_rows = jnp.concatenate(
                [w_high[z, c, block] for (z, _), c in zip(parts, cut)], axis=0
            )
            low_rows = jnp.concatenate(
                [w_low[z, c, block] for (z, _), c in zip(parts, cut)], axis=0
            )
            count = high_rows.shape[0]
            twice = dot(jnp.concatenate([high_rows, low_rows], axis=0), gx_high[j])
            along = twice[:count] + (twice[count:] + dot(high_rows, gx_low[j]))
            at = 0
            for (z, n), c in zip(parts, cut):
                part = along[at : at + c.stop - c.start]
                at += c.stop - c.start
                a_high[z, c, block], a_low[z, c, block] = split(part)

    def y_times(high, low):
        twice = dot(gy_both[...], high)
        return twice[:cells] + (twice[cells:] + dot(gy_both[:cells], low))

    def y_product(it, z):
        both = y_times(a_high[z], a_low[z])
        mix[z] = both
        for side, at in ((0, 0), (1, last)):
            for j in range(x_blocks):
                y_base[side, z, j : j + 1, :] = both[at : at + 1, j * cells : (j + 1) * cells]
        if it + 1 == ITERS:
            low = backs_at[1]
            rest = pl.ds(8 + low, cells - low)
            d = jnp.concatenate([dz[it, z, g, rest, :] for g in range(groups)], axis=1)
            final[z, low:, :] = d + STEP * both[low:]

    def y_first(it, z):
        count = backs_at[1]
        pair = jnp.concatenate([gy_both[:count], gy_both[cells : cells + count]], axis=0)
        twice = dot(pair, a_high[z])
        both = twice[:count] + (twice[count:] + dot(gy_both[:count], a_low[z]))
        d = jnp.concatenate([dz[it, z, g, pl.ds(8, count), :] for g in range(groups)], axis=1)
        final[z, :count, :] = d + STEP * both

    def x_ends(it):
        tile_lane = lax.broadcasted_iota(jnp.int32, (cells, 128), 1)
        near = pl.ds(8, cells)
        pack = jnp.zeros((cells, 128), f32)
        for z in range(planes):
            tiles = []
            for j in range(x_blocks):
                for spot, at, start_lane in (
                    (j, j * cells, 0), (x_blocks + j, (j + 1) * cells - 128, 127)
                ):
                    lanes = slice(at, at + 128)
                    tile = a_high[z, :, lanes].astype(f32) + a_low[z, :, lanes].astype(f32)
                    tiles.append((tile, start_lane, spot * planes + z))
            tiles.append((dz[it, z, 0, near, :], 0, 2 * x_blocks * planes + z))
            tiles.append((dz[it, z, groups - 1, near, :], 127, (2 * x_blocks + 1) * planes + z))
            for tile, lane_from, lane_to in tiles:
                if lane_from != lane_to:
                    tile = pltpu.roll(tile, (lane_to - lane_from) % 128, 1)
                pack = jnp.where(tile_lane == lane_to, tile, pack)
        turned = y_times(*split(pack)).T

        def keep(n, tile):
            other = pltpu.roll(tile, planes, 0)
            pair = (tile, other) if n % 2 == 0 else (other, tile)
            own_rows[n] = jnp.where(upper_wide, pair[0], pair[1])

        for n in range(2 * x_blocks):
            keep(n, turned[8 * (n // 2) : 8 * (n // 2) + 8])
        tile = turned[8 * x_blocks : 8 * x_blocks + 8]
        total = None
        for k in range(planes):
            line = jnp.where(
                upper_wide,
                jnp.broadcast_to(tile[k : k + 1], (8, cells)),
                jnp.broadcast_to(tile[planes + k : planes + k + 1], (8, cells)),
            )
            term = wide(w_mix[k]) * line
            total = term if total is None else total + term
        for n in range(2):
            keep(2 * x_blocks + n, total)

    def wide(weights):
        return jnp.concatenate([weights] * (cells // 128), axis=1)

    def x_share(it):
        total = None
        for n in range(kinds):
            term = wide(wx_send[n]) * own_rows[n]
            total = term if total is None else total + term
        x_send[it] = total
        x_all[it, col] = total
        for peer in col_peers:
            send(x_send.at[it], x_all.at[it, col], x_sems.at[0, it], x_sems.at[1, it], col=peer)

    def y_share(it):
        sides = []
        for side in range(2):
            parts = []
            for j in range(x_blocks):
                m = 2 * j + side
                total = wide(wx_in[m, 0]) * x_all[it, 0]
                for c in range(1, cols):
                    total = total + wide(wx_in[m, c]) * x_all[it, c]
                total = total + pltpu.roll(total, planes, 0)
                for n in range(kinds):
                    total = total + wide(wx_own[m, n]) * own_rows[n]
                parts.append(total)
            sides.append(jnp.where(upper_wide, parts[0], parts[1]))
        lines = []
        for side, at in ((0, 0), (1, last)):
            line = jnp.concatenate(
                [y_base[side, z, j : j + 1, :] for j in range(x_blocks) for z in range(planes)],
                axis=0,
            )
            for n in range(2):
                scale = jnp.broadcast_to(sides[n][:, at : at + 1], (8, cells))
                line = line + scale * gend[n, x_blocks]
            lines.append(line)
        y_send[it, 0] = lines[1]
        y_send[it, 1] = lines[0] + wide(wy_turn[...]) * lines[1]
        y_all[it, row] = lines[1]
        for n, peer in enumerate(row_peers):
            send(y_send.at[it, lax.div(row + n + 1, rows)], y_all.at[it, row], y_sems.at[0, it],
                 y_sems.at[1, it], row=peer)
        stacked = jnp.concatenate(sides + [jnp.zeros((112, cells), f32)], axis=0).T
        for t in range(cells // 8):
            here = slice(t * 8, t * 8 + 8)
            tile = stacked[here]
            for z in range(planes):
                for j in range(x_blocks):
                    block = slice(j * cells, (j + 1) * cells)
                    n = j * planes + z
                    mix[z, here, block] = (
                        mix[z, here, block]
                        + tile[:, n : n + 1] * gend[0, j]
                        + tile[:, 8 + n : 9 + n] * gend[1, j]
                    )
        finish(y_sems.at[1, it], y_all.at[it, pl.ds(0, rows - 1)])
        carried = []
        for side in range(2):
            total = wide(wy_in[side, 0]) * y_all[it, 0]
            for k in range(1, rows):
                total = total + wide(wy_in[side, k]) * y_all[it, k]
            for z in range(planes):
                for j in range(x_blocks):
                    n = j * planes + z
                    carry_rows[2 * z + side, :, j * cells : (j + 1) * cells] = jnp.broadcast_to(
                        total[n : n + 1], (8, cells)
                    )
            carried.append(total)
        return sides, carried

    def settle(it, low, high, squares):
        def step(i, acc):
            here, padded = eight(i * 8), eight(i * 8 + 8)
            g_first = jnp.concatenate([gy_ends[0, here, :]] * groups, axis=1)
            g_last = jnp.concatenate([gy_ends[1, here, :]] * groups, axis=1)
            for z in range(planes):
                solved = mix[z, here, :] + g_first * carry_rows[2 * z] + g_last * carry_rows[2 * z + 1]
                d = jnp.concatenate([dz[it, z, g, padded, :] for g in range(groups)], axis=1)
                renewed = jnp.minimum(jnp.maximum(d + STEP * solved, fz[z, here, :]), 1.0)
                if it + 1 < ITERS:
                    for g in range(groups):
                        dz[it + 1, z, g, padded, :] = renewed[:, g * 128 : (g + 1) * 128]
                change = renewed - d
                acc = acc + change * change
            return acc

        return lax.fori_loop(low // 8, high // 8, step, squares)

    def stream(it, ready):
        ready(order[0])
        ready(order[1])
        share_rows(it)
        a = 16
        for n in order[2:]:
            ready(n)
            b = cuts[n + 1] - 16 if n != order[-1] else cuts[4] + 16
            residual(it, a, b)
            x_product([(a, b)])
            a = b
            if n == order[2]:
                finish(v_sems.at[1, it], two_rows(it))
                mirror(it)
                residual(it, 0, 16)
                residual(it, cuts[4] + 16, cells)
                x_product([(0, 16), (cuts[4] + 16, cells)])

    def arrived(n):
        finish(d_rsem.at[n], piece_of(landing, cuts, n))
        regroup(cuts[n], cuts[n + 1])

    finish(e_sems.at[1], ez.at[others])
    scale_energy()
    stream(0, arrived)
    x_ends(0)
    x_share(0)
    for n in order[2:]:
        move_piece(bound, fz, n, f_ssem.at[0], f_rsem)
    for z in range(planes):
        y_product(0, z)
    finish(x_sems.at[1, 0], x_all.at[0, others])
    y_share(0)

    totals = []
    blank = jnp.zeros((8, width), f32)
    held = [blank]

    def settled(n):
        finish(f_rsem.at[n], piece_of(fz, cuts, n))
        held.append(settle(0, cuts[n], cuts[n + 1], held.pop()))

    stream(1, settled)
    def give_back(n, m):
        at = pl.ds(backs_at[n], backs_at[n + 1] - backs_at[n])
        send(final.at[col_peers[m], at, :], out.at[at, slab(col)], back_ssem.at[0],
             back_rsem.at[n], col=col_peers[m])

    def give_all(n):
        for m in range(cols - 1):
            give_back(n, m)

    def complete(low, high):
        @pl.loop(low // 8, high // 8)
        def _(i):
            here = eight(i * 8)
            tile = x_cols[here, :]
            ends_of = [
                jnp.concatenate([gy_ends[n, here, :]] * (cells // 128), axis=1) for n in range(2)
            ]
            for k in range(blocks):
                block = slice(k * cells, (k + 1) * cells)
                n = 8 * (k // x_blocks) + 2 * (k % x_blocks)
                value = (
                    out[here, block]
                    + tile[:, n : n + 1] * g_all[0, k]
                    + tile[:, n + 1 : n + 2] * g_all[1, k]
                    + (ends_of[0] * y_lines[0, k] + ends_of[1] * y_lines[1, k])
                )
                out[here, block] = jnp.minimum(jnp.maximum(value, bound[here, block]), 1.0)

    for m in range(cols - 1):
        y_first(1, col_peers[m])
        give_back(0, m)
    x_ends(1)
    x_share(1)
    for m in range(cols - 1):
        y_product(1, col_peers[m])
        give_back(1, m)
    y_first(1, col)
    y_product(1, col)
    out[:, slab(col)] = final[col]
    finish(x_sems.at[1, 1], x_all.at[1, others])
    sides, carried = y_share(1)
    for z in range(planes):
        for j in range(x_blocks):
            n = j * planes + z
            for side in range(2):
                at = 2 * j + side
                word_send[z, at : at + 1, :] = STEP * sides[side][n : n + 1]
                at += 2 * x_blocks
                word_send[z, at : at + 1, :] = STEP * carried[side][n : n + 1]
    for peer in col_peers:
        send(word_send.at[peer], word_all.at[col], w_sems.at[0], w_sems.at[1], col=peer)
    give_all(2)
    word_all[col] = word_send[col]
    totals.append(jnp.sum(held[0]))
    totals.append(jnp.sum(settle(ITERS - 1, 0, cells, blank)))
    s_send[...] = jnp.where(sub == 0, totals[0], jnp.where(sub == 1, totals[1], 0.0))
    for n, peer in enumerate(row_peers):
        send(s_send, s_row.at[n], s_sems.at[0], s_sems.at[1], row=peer)
    finish(s_sems.at[1], s_row)
    total = s_send[...]
    for n in range(rows - 1):
        total = total + s_row[n]
    s_col_send[...] = total
    for n, peer in enumerate(col_peers):
        send(s_col_send, s_col.at[n], s_sems.at[2], s_sems.at[3], col=peer)
    for n in range(3, len(backs_at) - 1):
        give_all(n)
    finish(w_sems.at[1], word_all.at[others])
    x_cols[...] = jnp.concatenate(
        [word_all[c] for c in range(cols)] + [jnp.zeros((128 - 8 * cols, cells), f32)], axis=0
    ).T
    for k in range(blocks):
        for side in range(2):
            at = 2 * x_blocks + 2 * (k % x_blocks) + side
            y_lines[side, k] = jnp.broadcast_to(
                word_all[k // x_blocks, at : at + 1, :], (8, cells)
            )
    for n in range(len(backs_at) - 2):
        finish(back_rsem.at[n], piece_of(final, backs_at, n))
        complete(backs_at[n], backs_at[n + 1])
    finish(s_sems.at[3], s_col)
    for n in range(cols - 1):
        total = total + s_col[n]
    sizes = jnp.sqrt(total / cell_count + EPSILON) / STEP
    norms[...] = jnp.where(lane == 0, sizes[:1, :], sizes[1:2, :])[0, :ITERS]
    for it in range(ITERS):
        finish(x_sems.at[0, it], x_all.at[it, others])
        finish(y_sems.at[0, it], y_all.at[it, pl.ds(0, rows - 1)])
        finish(v_sems.at[0, it], two_rows(it))
    finish(e_sems.at[0], ez.at[others])
    finish(d_ssem.at[0], landing.at[others])
    finish(f_ssem.at[0], fz.at[others])
    finish(w_sems.at[0], word_all.at[others])
    finish(s_sems.at[0], s_row)
    finish(s_sems.at[2], s_col)
    n = len(backs_at) - 2
    finish(back_rsem.at[n], piece_of(final, backs_at, n))
    complete(backs_at[n], backs_at[n + 1])
    finish(back_ssem.at[0], final.at[others])


def hand_over(damage, norms, damage_out, norms_out, sems):
    parts = 4
    part = damage.shape[0] // parts
    copies = [pltpu.make_async_copy(norms, norms_out, sems.at[parts])]
    for n in range(parts):
        at = pl.ds(n * part, part)
        copies.append(pltpu.make_async_copy(damage.at[at], damage_out.at[0, at], sems.at[n]))
    for copy in copies:
        copy.start()
    for copy in copies:
        copy.wait()


def local(energy, damage_old, crack_seeds, irreversible, line_inverses, z_inverse):
    planes, cells, line_length = energy.shape
    rows, cols = lax.axis_size("row"), lax.axis_size("col")
    blocks, _, _ = line_inverses.shape
    width = line_length // cols
    x_blocks = width // cells
    kinds = 2 * x_blocks + 2
    step = cells // 16
    cuts = (0, 3 * step, 8 * step, 12 * step, 13 * step, cells)
    backs_at = (0, 2 * step, 10 * step, 13 * step, 15 * step, cells)
    cell_count = float(cols * rows * cells * line_length)
    shape = (rows, cols, cells, width, x_blocks, blocks, cell_count, cuts, backs_at)
    f32 = jnp.float32
    bf16 = jnp.bfloat16
    dma = pltpu.SemaphoreType.DMA
    vmem = pl.BlockSpec(memory_space=pltpu.VMEM)
    damage, norms = pl.pallas_call(
        functools.partial(line_kernel, shape),
        out_shape=(
            pltpu.VMEM((cells, line_length), f32),
            pltpu.VMEM((ITERS,), f32),
        ),
        in_specs=[pl.BlockSpec(memory_space=pl.ANY)] * 6,
        out_specs=(vmem, vmem),
        scratch_shapes=[
            pltpu.VMEM((cells, line_length), f32),
            pltpu.VMEM((cells, line_length), jnp.int32),
            pltpu.VMEM((cells, line_length), jnp.int32),
            pltpu.VMEM((cells, line_length), f32),
            pltpu.VMEM((cells, line_length), f32),
            pltpu.VMEM((cols, cells, width), f32),
            pltpu.VMEM((cols, cells, width), f32),
            pltpu.VMEM((cols, cells, width), f32),
            pltpu.VMEM((cols, cells, width), f32),
            pltpu.VMEM((ITERS, cols, width // 128, cells + 16, 128), f32),
            pltpu.VMEM((cols, cells, width), f32),
            pltpu.VMEM((cols, cells, width), bf16),
            pltpu.VMEM((cols, cells, width), bf16),
            pltpu.VMEM((cols, cells, width), bf16),
            pltpu.VMEM((cols, cells, width), bf16),
            pltpu.VMEM((cols, cells, width), f32),
            pltpu.VMEM((blocks, cells, cells), f32),
            pltpu.VMEM((x_blocks, cells, cells), bf16),
            pltpu.VMEM((x_blocks, cells, cells), bf16),
            pltpu.VMEM((2 * cells, cells), bf16),
            pltpu.VMEM((2, cells, 128), f32),
            pltpu.VMEM((2, x_blocks + 1, 8, cells), f32),
            pltpu.VMEM((kinds, 8, 128), f32),
            pltpu.VMEM((2 * x_blocks, cols, 8, 128), f32),
            pltpu.VMEM((2 * x_blocks, kinds, 8, 128), f32),
            pltpu.VMEM((2, rows, 8, 128), f32),
            pltpu.VMEM((8, 128), f32),
            pltpu.VMEM((2 * cols, 8, width), f32),
            pltpu.VMEM((kinds, 8, cells), f32),
            pltpu.VMEM((cols, 8, 128), f32),
            pltpu.VMEM((2, cols, 8, cells), f32),
            pltpu.VMEM((2, blocks, 8, cells), f32),
            pltpu.VMEM((cols, 8, cells), f32),
            pltpu.VMEM((cols, 8, cells), f32),
            pltpu.VMEM((cells, 128), f32),
            pltpu.VMEM((2, blocks, 8, cells), f32),
            pltpu.VMEM((ITERS, 8, cells), f32),
            pltpu.VMEM((ITERS, cols, 8, cells), f32),
            pltpu.VMEM((ITERS, 2, 8, cells), f32),
            pltpu.VMEM((ITERS, rows, 8, cells), f32),
            pltpu.VMEM((8, 128), f32),
            pltpu.VMEM((rows - 1, 8, 128), f32),
            pltpu.VMEM((8, 128), f32),
            pltpu.VMEM((cols - 1, 8, 128), f32),
            pltpu.SMEM((cols, cols), f32),
            dma((6,)),
            pltpu.SemaphoreType.REGULAR((2,)),
            dma((2,)),
            dma((1,)),
            dma((5,)),
            dma((1,)),
            dma((5,)),
            dma((1,)),
            dma((5,)),
            dma((2,)),
            dma((2, ITERS)),
            dma((2, ITERS)),
            dma((2, ITERS)),
            dma((4,)),
        ],
        compiler_params=pltpu.CompilerParams(
            has_side_effects=True, collective_id=0, vmem_limit_bytes=60 * 1024 * 1024
        ),
        name="line_iterations",
    )(
        z_inverse,
        energy[0],
        damage_old[0],
        crack_seeds[0],
        irreversible[0],
        line_inverses,
    )
    return pl.pallas_call(
        hand_over,
        out_shape=(
            jax.ShapeDtypeStruct((1, cells, line_length), f32),
            jax.ShapeDtypeStruct((ITERS,), f32),
        ),
        in_specs=[vmem, vmem],
        out_specs=(pl.BlockSpec(memory_space=pl.ANY), pl.BlockSpec(memory_space=pl.ANY)),
        scratch_shapes=[dma((5,))],
        compiler_params=pltpu.CompilerParams(vmem_limit_bytes=1024 * 1024),
        name="hand_over",
    )(
        pltpu.with_memory_space_constraint(damage, pltpu.VMEM),
        pltpu.with_memory_space_constraint(norms, pltpu.VMEM),
    )


def solution(mesh):
    def local_any(energy, damage_old, crack_seeds, irreversible, line_inverses, z_inverse):
        rows, cols = mesh.shape["row"], mesh.shape["col"]
        block_cells = line_inverses.shape[1]
        width = energy.shape[2] // cols
        whole_blocks = (
            energy.shape[0] == 1
            and energy.shape[1] == block_cells
            and width == 2 * block_cells
            and block_cells % 256 == 0
            and 2 * cols == 8
            and 2 * rows <= 128
            and min(rows, cols) > 2
        )
        chosen = local if whole_blocks else local_turned
        return chosen(energy, damage_old, crack_seeds, irreversible, line_inverses, z_inverse)

    return jax.shard_map(
        local_any,
        mesh=mesh,
        in_specs=(
            P("col", "row", None),
            P("col", "row", None),
            P("col", "row", None),
            P("col", "row", None),
            P(),
            P(),
        ),
        out_specs=(P("col", "row", None), P()),
        check_vma=False,
    )
```

```python
import functools

import jax
import jax.numpy as jnp
from jax import lax
from jax.experimental import pallas as pl
from jax.experimental.pallas import tpu as pltpu
from jax.sharding import PartitionSpec as P

ITERS = 2


KAPPA = 2.0
STEP = 0.02
COUPLE = 0.5
EPSILON = 1e-06
HIGHEST = lax.Precision.HIGHEST


def second_difference(grid_field, along):
    extent = grid_field.shape[along]
    forward_diff = lax.slice_in_dim(grid_field, 1, extent, axis=along) - lax.slice_in_dim(
        grid_field, 0, extent - 1, axis=along
    )
    zero_shape = list(grid_field.shape)
    zero_shape[along] = 1
    zero_rim = jnp.zeros(zero_shape, grid_field.dtype)
    ahead = jnp.concatenate([forward_diff, zero_rim], axis=along)
    behind = jnp.concatenate([zero_rim, forward_diff], axis=along)
    return ahead - behind


def line_solve(line_rows, inverses):
    block_count, block_cells, _ = inverses.shape
    line_count = line_rows.shape[0]
    blocks = line_rows.reshape(line_count, block_count, block_cells)
    products = jnp.einsum("rkb,kcb->rkc", blocks, inverses, precision=lax.Precision.HIGHEST)
    first_col = inverses[:, :, 0]
    last_col = inverses[:, :, block_cells - 1]
    incoming = [jnp.zeros((line_count,), line_rows.dtype)]
    for block_index in range(block_count - 1):
        incoming.append(
            products[:, block_index, block_cells - 1]
            + COUPLE * incoming[block_index] * inverses[block_index, block_cells - 1, 0]
        )
    inflow = jnp.stack(incoming, axis=1)
    forward = products + COUPLE * inflow[:, :, None] * first_col[None]
    head_terms = [jnp.zeros((line_count,), line_rows.dtype) for block_index in range(block_count)]
    carried = forward[:, block_count - 1, 0]
    for block_index in range(block_count - 2, -1, -1):
        head_terms[block_index] = carried
        carried = (
            forward[:, block_index, 0]
            + COUPLE * carried * inverses[block_index, 0, block_cells - 1]
        )
    outflow = jnp.stack(head_terms, axis=1)
    solved = forward + COUPLE * outflow[:, :, None] * last_col[None]
    return solved.reshape(line_count, block_count * block_cells)


def local_turned(energy, damage_old, crack_seeds, irreversible, line_inverses, z_inverse):
    planes, rows_here, line_length = energy.shape
    row_count = lax.axis_size("row")
    col_count = lax.axis_size("col")
    total_planes = planes * col_count
    cell_count = total_planes * rows_here * row_count * line_length
    seeded = crack_seeds == 1
    damage = jnp.where(seeded, 1.0, damage_old)
    lower_bound = jnp.where(irreversible == 1, damage_old, 0.0)
    own_sums = []
    for sweep_index in range(ITERS):
        local_lap = second_difference(damage, 2)
        partial_value = energy - (1.0 + energy) * damage + KAPPA * local_lap
        moved_part, moved_damage = (
            lax.all_to_all(
                lax.all_to_all(
                    jnp.swapaxes(partial_value, 1, 2),
                    "row",
                    split_axis=1,
                    concat_axis=2,
                    tiled=True,
                ),
                "col",
                split_axis=1,
                concat_axis=0,
                tiled=True,
            ),
            lax.all_to_all(
                lax.all_to_all(
                    jnp.swapaxes(damage, 1, 2), "row", split_axis=1, concat_axis=2, tiled=True
                ),
                "col",
                split_axis=1,
                concat_axis=0,
                tiled=True,
            ),
        )
        lap_rest = second_difference(moved_damage, 2) + second_difference(moved_damage, 0)
        turned = moved_part + KAPPA * lap_rest
        turned_shape = turned.shape
        along_y = line_solve(turned.reshape(-1, turned_shape[2]), line_inverses).reshape(
            turned_shape
        )
        along_z = jnp.einsum("zk,kxy->zxy", z_inverse, along_y, precision=lax.Precision.HIGHEST)
        gathered = lax.all_to_all(
            lax.all_to_all(along_z, "row", split_axis=2, concat_axis=1, tiled=True),
            "col",
            split_axis=0,
            concat_axis=1,
            tiled=True,
        )
        piece_cells = gathered.shape[1] // (row_count * col_count)
        reordered = gathered.reshape(planes, col_count, row_count, piece_cells, rows_here)
        restored = jnp.transpose(reordered, (0, 4, 2, 1, 3)).reshape(planes, rows_here, line_length)
        update = STEP * line_solve(restored.reshape(-1, line_length), line_inverses).reshape(
            restored.shape
        )
        clamped = jnp.minimum(jnp.maximum(damage + update, lower_bound), 1.0)
        renewed = jnp.where(seeded, 1.0, clamped)
        own_sum = jnp.sum((renewed - damage) ** 2)
        own_sums.append(own_sum)
        damage = renewed
    global_sums = lax.psum(jnp.stack(own_sums), ("row", "col"))
    update_norms = jnp.sqrt(global_sums / cell_count + EPSILON) / STEP
    return (damage, update_norms)


def line_kernel(
    shape,
    z_hbm,
    energy,
    damage_hbm,
    seeds_hbm,
    irreversible_hbm,
    inverses,
    out,
    norms,
    damage_old,
    crack_seeds,
    irreversible,
    e_home,
    start,
    bound,
    ez,
    ec,
    fz,
    landing,
    dx,
    dz,
    final,
    w_high,
    w_low,
    a_high,
    a_low,
    mix,
    inverse,
    gx_high,
    gx_low,
    gy_both,
    gy_ends,
    gend,
    wx_send,
    wx_in,
    wx_own,
    wy_in,
    wy_turn,
    carry_rows,
    own_rows,
    w_mix,
    y_base,
    g_all,
    word_send,
    word_all,
    x_cols,
    y_lines,
    x_send,
    x_all,
    y_send,
    y_all,
    s_send,
    s_row,
    s_col_send,
    s_col,
    z_inv,
    local_sems,
    greet,
    e_sems,
    d_ssem,
    d_rsem,
    f_ssem,
    f_rsem,
    back_ssem,
    back_rsem,
    w_sems,
    x_sems,
    v_sems,
    y_sems,
    s_sems,
):
    rows, cols, cells, width, x_blocks, blocks, cell_count, cuts, backs_at = shape
    planes = cols
    last = cells - 1
    groups = width // 128
    kinds = 2 * x_blocks + 2
    f32 = jnp.float32
    row, col = lax.axis_index("row"), lax.axis_index("col")
    row_peers = [lax.rem(row + o, rows) for o in range(1, rows)]
    col_peers = [lax.rem(col + o, cols) for o in range(1, cols)]

    def slab(who):
        return pl.ds(pl.multiple_of(who * width, width), width)

    def eight(at):
        return pl.ds(pl.multiple_of(at, 8), 8)

    def send(src, dst, ssem, rsem, **where):
        copy = pltpu.make_async_remote_copy(
            src_ref=src, dst_ref=dst, send_sem=ssem, recv_sem=rsem,
            device_id=where, device_id_type=pl.DeviceIdType.MESH,
        )
        copy.start()
        return copy

    def finish(sem, sized):
        pltpu.make_async_copy(sized, sized, sem).wait()

    def split(a):
        high = a.astype(jnp.bfloat16)
        return high, (a - high.astype(f32)).astype(jnp.bfloat16)

    def dot(a, b):
        return jnp.dot(a, b, preferred_element_type=f32)

    barrier = pltpu.get_barrier_semaphore()
    for peer in col_peers:
        pl.semaphore_signal(
            barrier, inc=1, device_id={"col": peer}, device_id_type=pl.DeviceIdType.MESH
        )
    above, below = row > 0, row < rows - 1

    def signal_row(sem, who):
        pl.semaphore_signal(
            sem, inc=1, device_id={"row": who}, device_id_type=pl.DeviceIdType.MESH
        )

    @pl.when(above)
    def _():
        signal_row(barrier, row - 1)

    @pl.when(below)
    def _():
        signal_row(barrier, row + 1)

    pulls = [
        pltpu.make_async_copy(damage_hbm, damage_old, local_sems.at[0]),
        pltpu.make_async_copy(seeds_hbm, crack_seeds, local_sems.at[1]),
        pltpu.make_async_copy(irreversible_hbm, irreversible, local_sems.at[2]),
    ]
    fetch = [
        pltpu.make_async_copy(inverses, inverse, local_sems.at[4]),
        pltpu.make_async_copy(z_hbm, z_inv, local_sems.at[5]),
    ]
    e_cuts = (0, cells // 8, cells)
    e_parts = [pl.ds(a, b - a) for a, b in zip(e_cuts, e_cuts[1:])]
    loads = [
        pltpu.make_async_copy(energy.at[at], e_home.at[at], local_sems.at[(3, 6)[n]])
        for n, at in enumerate(e_parts)
    ]
    for copy in loads + pulls + fetch:
        copy.start()
    neighbours = jnp.where(above, 1, 0) + jnp.where(below, 1, 0)
    pl.semaphore_wait(barrier, cols - 1 + neighbours)

    def move_piece(src, target, index, ssem, rsem):
        at = pl.ds(cuts[index], cuts[index + 1] - cuts[index])
        for peer in col_peers:
            send(src.at[at, slab(peer)], target.at[col, at, :], ssem, rsem.at[index], col=peer)

    others = pl.ds(0, cols - 1)

    def piece_of(target, marks, index):
        return target.at[others, pl.ds(marks[index], marks[index + 1] - marks[index]), :]

    for copy, at in zip(loads, e_parts):
        copy.wait()
        for peer in col_peers:
            send(e_home.at[at, slab(peer)], ez.at[col, at, :], e_sems.at[0], e_sems.at[1], col=peer)
    for copy in pulls:
        copy.wait()

    @pl.loop(0, cells // 16)
    def _(i):
        at = pl.ds(pl.multiple_of(i * 16, 16), 16)
        old = damage_old[at, :]
        seeded = crack_seeds[at, :] == 1
        start[at, :] = jnp.where(seeded, 1.0, old)
        bound[at, :] = jnp.where(seeded, 1.0, jnp.where(irreversible[at, :] == 1, old, 0.0))

    order = (0, 4, 1, 2, 3)
    for n in order:
        move_piece(start, landing, n, d_ssem.at[0], d_rsem)
    for n in order[:2]:
        move_piece(bound, fz, n, f_ssem.at[0], f_rsem)
    ez[col] = e_home[:, slab(col)]
    landing[col] = start[:, slab(col)]
    fz[col] = bound[:, slab(col)]

    lane = lax.broadcasted_iota(jnp.int32, (8, 128), 1)
    sub = lax.broadcasted_iota(jnp.int32, (8, 128), 0)
    upper_half = sub < planes
    zero = jnp.zeros((8, 128), f32)
    for copy in fetch:
        copy.wait()

    def lane_of(a, n):
        return jnp.broadcast_to(a[:, n : n + 1], (8, 128))

    def corner_of(down, over, k):
        tile = inverse[k, (cells - 8) * down : (cells - 8) * down + 8, (cells - 128) * over : (cells - 128) * over + 128]
        at = (7 if down else 0, 127 if over else 0)
        return jnp.broadcast_to(tile[at[0] : at[0] + 1, at[1] : at[1] + 1], (8, 128))

    def hot(index):
        return jnp.where(lane == index, 1.0, 0.0)

    def carries(first, final_of, lower=None, upper=None):
        firsts, finals = [], []
        low = [None if lower is None else lower(k) for k in range(blocks)]
        high = [None if upper is None else upper(k) for k in range(blocks)]
        for k in range(blocks):
            begin, end = hot(first(k)), hot(final_of(k))
            if low[k] is not None:
                begin = begin + corner_of(0, 0, k) * hot(low[k])
                end = end + corner_of(1, 0, k) * hot(low[k])
            if high[k] is not None:
                begin = begin + corner_of(0, 1, k) * hot(high[k])
                end = end + corner_of(1, 1, k) * hot(high[k])
            firsts.append(begin)
            finals.append(end)
        incoming = [zero]
        for k in range(blocks - 1):
            incoming.append(finals[k] + COUPLE * corner_of(1, 0, k) * incoming[k])
        heads = [
            firsts[k] + COUPLE * corner_of(0, 0, k) * incoming[k] for k in range(blocks)
        ]
        carried = heads[blocks - 1]
        outgoing = [zero] * blocks
        for k in range(blocks - 2, -1, -1):
            outgoing[k] = carried
            carried = heads[k] + COUPLE * corner_of(0, 1, k) * carried
        enter, leave = [], []
        for k in range(blocks):
            enter.append(COUPLE * incoming[k] + (zero if low[k] is None else hot(low[k])))
            leave.append(COUPLE * outgoing[k] + (zero if high[k] is None else hot(high[k])))
        return incoming, outgoing, enter, leave

    def picked(which, options):
        total = zero
        for n, option in enumerate(options):
            if option is not None:
                total = total + jnp.where(which == n, option, 0.0)
        return total

    def at_own(c, weights):
        return pltpu.roll(weights, 128 - 8 * c, 1) if c > 0 else weights

    def left_of(k):
        c = k // x_blocks
        return 8 * (c - 1) + 2 * x_blocks + 1 if k % x_blocks == 0 and c > 0 else None

    def right_of(k):
        c = k // x_blocks
        return 8 * (c + 1) + 2 * x_blocks if k % x_blocks == x_blocks - 1 and c < cols - 1 else None

    incoming, outgoing, enter, leave = carries(
        lambda k: 8 * (k // x_blocks) + k % x_blocks,
        lambda k: 8 * (k // x_blocks) + x_blocks + k % x_blocks,
        left_of,
        right_of,
    )
    to_right = picked(col, [
        at_own(c, incoming[(c + 1) * x_blocks] + hot(8 * c + 2 * x_blocks + 1) / COUPLE)
        if c < cols - 1 else None
        for c in range(cols)
    ])
    to_left = picked(col, [
        at_own(c, leave[c * x_blocks - 1] / COUPLE) if c > 0 else None for c in range(cols)
    ])
    for n in range(kinds):
        wx_send[n] = jnp.where(upper_half, lane_of(to_right, n), lane_of(to_left, n))
    for m in range(2 * x_blocks):
        table = (enter, leave)[m % 2]
        everywhere = picked(col, [table[c * x_blocks + m // 2] for c in range(cols)])
        here = picked(col, [at_own(c, table[c * x_blocks + m // 2]) for c in range(cols)])
        for c in range(cols):
            from_left = jnp.where(col > c, lane_of(everywhere, 8 * c + 2 * x_blocks - 1), 0.0)
            from_right = jnp.where(col < c, lane_of(everywhere, 8 * c), 0.0)
            wx_in[m, c] = jnp.where(upper_half, from_left, from_right)
        for n in range(kinds):
            wx_own[m, n] = lane_of(here, n)

    incoming, outgoing, enter, leave = carries(lambda k: 2 * k, lambda k: 2 * k + 1)
    enters, leaves = picked(row, enter), picked(row, leave)
    for k in range(rows):
        wy_in[0, k] = lane_of(enters, 2 * k + 1)
        wy_in[1, k] = jnp.where(row >= k, lane_of(leaves, 2 * k + 1), lane_of(leaves, 2 * k))
    wy_turn[...] = picked(
        row, [lane_of(outgoing[k - 1], 2 * k + 1) if k > 0 else None for k in range(rows)]
    )

    upper_wide = lax.broadcasted_iota(jnp.int32, (8, cells), 0) < planes
    for j in range(x_blocks):
        turned = inverse[col * x_blocks + j].T
        gx_high[j], gx_low[j] = split(turned)
        for side, at in ((0, 0), (1, last)):
            line = jnp.broadcast_to(turned[at : at + 1], (8, cells))
            gend[side, j] = line
            if j == 0:
                gend[side, x_blocks] = line
            else:
                gend[side, x_blocks] = jnp.where(upper_wide, gend[side, x_blocks], line)
    gy = inverse[row]
    gy_both[:cells], gy_both[cells:] = split(gy)
    gy_ends[0] = jnp.broadcast_to(gy[:, :1], (cells, 128))
    gy_ends[1] = jnp.broadcast_to(gy[:, last:], (cells, 128))

    for k in range(blocks):
        for side, at in ((0, 0), (1, 127)):
            strip = inverse[k, :, (cells - 128) * side : (cells - 128) * side + 128]
            line = strip.T[at : at + 1]
            g_all[side, k] = jnp.broadcast_to(line, (8, cells))

    @pl.when(above)
    def _():
        pl.semaphore_wait(greet.at[0], 1)

    @pl.when(below)
    def _():
        signal_row(greet.at[0], row + 1)
        pl.semaphore_wait(greet.at[1], 1)

    @pl.when(above)
    def _():
        signal_row(greet.at[1], row - 1)

    first_col = jnp.where(col == 0, 1.0, 0.0)
    last_col = jnp.where(col == cols - 1, 1.0, 0.0)
    at_first, at_last = lane == 0, lane == 127

    def keep_damage(it, z, at, row_of):
        tiles = [row_of[:, g * 128 : (g + 1) * 128] for g in range(groups)]
        up = [pltpu.roll(tile, 1, 1) for tile in tiles]
        down = [pltpu.roll(tile, 127, 1) for tile in tiles]
        for g in range(groups):
            before = up[g - 1] if g > 0 else tiles[g] * first_col
            after = down[g + 1] if g < groups - 1 else tiles[g] * last_col
            dz[it, z, g, eight(at + 8), :] = tiles[g]
            dx[z, eight(at), g * 128 : (g + 1) * 128] = jnp.where(
                at_first, before, up[g]
            ) + jnp.where(at_last, after, down[g])

    mixing = [[KAPPA * z_inv[z, k] for k in range(planes)] for z in range(planes)]
    for k in range(planes):
        weights = zero
        for z in range(planes):
            weights = jnp.where(lax.rem(sub, planes) == z, mixing[z][k], weights)
        w_mix[k] = weights

    def scale_energy():
        @pl.loop(0, cells // 8)
        def _(i):
            for z in range(planes):
                sides = 4 + (z > 0) + (z < planes - 1)
                scaled = ez[z, eight(i * 8), :] * (1.0 / KAPPA)
                ez[z, eight(i * 8), :] = scaled
                ec[z, eight(i * 8), :] = scaled + (1.0 / KAPPA + sides)

    def regroup(low, high):
        @pl.loop(low // 8, high // 8)
        def _(i):
            for z in range(planes):
                keep_damage(0, z, i * 8, landing[z, eight(i * 8), :])

    def share_rows(it):
        send(dz.at[it, :, :, pl.ds(cells, 8), :], dz.at[it, :, :, pl.ds(0, 8), :],
             v_sems.at[0, it], v_sems.at[1, it], row=lax.rem(row + 1, rows))
        send(dz.at[it, :, :, pl.ds(8, 8), :], dz.at[it, :, :, pl.ds(cells + 8, 8), :],
             v_sems.at[0, it], v_sems.at[1, it], row=lax.rem(row + rows - 1, rows))

    def two_rows(it):
        return dz.at[it, :, :, pl.ds(0, 16), :]

    def mirror(it):
        for z in range(planes):
            for g in range(groups):
                dz[it, z, g, 7:8, :] = jnp.where(
                    row == 0, dz[it, z, g, 8:9, :], dz[it, z, g, 7:8, :]
                )
                dz[it, z, g, cells + 8 : cells + 9, :] = jnp.where(
                    row == rows - 1,
                    dz[it, z, g, cells + 7 : cells + 8, :],
                    dz[it, z, g, cells + 8 : cells + 9, :],
                )

    def residual(it, low, high):
        @pl.loop(low // 16, high // 16)
        def _(i):
            base = pl.multiple_of(i * 16, 16)
            here = pl.ds(base, 16)
            padded = pl.ds(pl.multiple_of(base + 8, 8), 16)
            for g in range(groups):
                lanes = slice(g * 128, (g + 1) * 128)
                mids = [dz[it, z, g, padded, :] for z in range(planes)]
                value = []
                for z in range(planes):
                    d = mids[z]
                    near = dz[it, z, g, pl.ds(base + 7, 16), :] + dz[it, z, g, pl.ds(base + 9, 16), :]
                    near = near + dx[z, here, lanes]
                    if z > 0:
                        near = near + mids[z - 1]
                    if z < planes - 1:
                        near = near + mids[z + 1]
                    value.append(near + (ez[z, here, lanes] - ec[z, here, lanes] * d))
                for z in range(planes):
                    total = mixing[z][0] * value[0]
                    for k in range(1, planes):
                        total = total + mixing[z][k] * value[k]
                    w_high[z, here, lanes], w_low[z, here, lanes] = split(total)

    def x_product(ranges):
        for j in range(x_blocks):
            block = slice(j * cells, (j + 1) * cells)
            parts = [(z, n) for z in range(planes) for n in range(len(ranges))]
            cut = [slice(*ranges[n]) for _, n in parts]
            high_rows = jnp.concatenate(
                [w_high[z, c, block] for (z, _), c in zip(parts, cut)], axis=0
            )
            low_rows = jnp.concatenate(
                [w_low[z, c, block] for (z, _), c in zip(parts, cut)], axis=0
            )
            count = high_rows.shape[0]
            twice = dot(jnp.concatenate([high_rows, low_rows], axis=0), gx_high[j])
            along = twice[:count] + (twice[count:] + dot(high_rows, gx_low[j]))
            at = 0
            for (z, n), c in zip(parts, cut):
                part = along[at : at + c.stop - c.start]
                at += c.stop - c.start
                a_high[z, c, block], a_low[z, c, block] = split(part)

    def y_times(high, low):
        twice = dot(gy_both[...], high)
        return twice[:cells] + (twice[cells:] + dot(gy_both[:cells], low))

    def y_product(it, z):
        both = y_times(a_high[z], a_low[z])
        mix[z] = both
        for side, at in ((0, 0), (1, last)):
            for j in range(x_blocks):
                y_base[side, z, j : j + 1, :] = both[at : at + 1, j * cells : (j + 1) * cells]
        if it + 1 == ITERS:
            low = backs_at[1]
            rest = pl.ds(8 + low, cells - low)
            d = jnp.concatenate([dz[it, z, g, rest, :] for g in range(groups)], axis=1)
            final[z, low:, :] = d + STEP * both[low:]

    def y_first(it, z):
        count = backs_at[1]
        pair = jnp.concatenate([gy_both[:count], gy_both[cells : cells + count]], axis=0)
        twice = dot(pair, a_high[z])
        both = twice[:count] + (twice[count:] + dot(gy_both[:count], a_low[z]))
        d = jnp.concatenate([dz[it, z, g, pl.ds(8, count), :] for g in range(groups)], axis=1)
        final[z, :count, :] = d + STEP * both

    def x_ends(it):
        tile_lane = lax.broadcasted_iota(jnp.int32, (cells, 128), 1)
        near = pl.ds(8, cells)
        pack = jnp.zeros((cells, 128), f32)
        for z in range(planes):
            tiles = []
            for j in range(x_blocks):
                for spot, at, start_lane in (
                    (j, j * cells, 0), (x_blocks + j, (j + 1) * cells - 128, 127)
                ):
                    lanes = slice(at, at + 128)
                    tile = a_high[z, :, lanes].astype(f32) + a_low[z, :, lanes].astype(f32)
                    tiles.append((tile, start_lane, spot * planes + z))
            tiles.append((dz[it, z, 0, near, :], 0, 2 * x_blocks * planes + z))
            tiles.append((dz[it, z, groups - 1, near, :], 127, (2 * x_blocks + 1) * planes + z))
            for tile, lane_from, lane_to in tiles:
                if lane_from != lane_to:
                    tile = pltpu.roll(tile, (lane_to - lane_from) % 128, 1)
                pack = jnp.where(tile_lane == lane_to, tile, pack)
        turned = y_times(*split(pack)).T

        def keep(n, tile):
            other = pltpu.roll(tile, planes, 0)
            pair = (tile, other) if n % 2 == 0 else (other, tile)
            own_rows[n] = jnp.where(upper_wide, pair[0], pair[1])

        for n in range(2 * x_blocks):
            keep(n, turned[8 * (n // 2) : 8 * (n // 2) + 8])
        tile = turned[8 * x_blocks : 8 * x_blocks + 8]
        total = None
        for k in range(planes):
            line = jnp.where(
                upper_wide,
                jnp.broadcast_to(tile[k : k + 1], (8, cells)),
                jnp.broadcast_to(tile[planes + k : planes + k + 1], (8, cells)),
            )
            term = wide(w_mix[k]) * line
            total = term if total is None else total + term
        for n in range(2):
            keep(2 * x_blocks + n, total)

    def wide(weights):
        return jnp.concatenate([weights] * (cells // 128), axis=1)

    def x_share(it):
        total = None
        for n in range(kinds):
            term = wide(wx_send[n]) * own_rows[n]
            total = term if total is None else total + term
        x_send[it] = total
        x_all[it, col] = total
        for peer in col_peers:
            send(x_send.at[it], x_all.at[it, col], x_sems.at[0, it], x_sems.at[1, it], col=peer)

    def y_share(it):
        sides = []
        for side in range(2):
            parts = []
            for j in range(x_blocks):
                m = 2 * j + side
                total = wide(wx_in[m, 0]) * x_all[it, 0]
                for c in range(1, cols):
                    total = total + wide(wx_in[m, c]) * x_all[it, c]
                total = total + pltpu.roll(total, planes, 0)
                for n in range(kinds):
                    total = total + wide(wx_own[m, n]) * own_rows[n]
                parts.append(total)
            sides.append(jnp.where(upper_wide, parts[0], parts[1]))
        lines = []
        for side, at in ((0, 0), (1, last)):
            line = jnp.concatenate(
                [y_base[side, z, j : j + 1, :] for j in range(x_blocks) for z in range(planes)],
                axis=0,
            )
            for n in range(2):
                scale = jnp.broadcast_to(sides[n][:, at : at + 1], (8, cells))
                line = line + scale * gend[n, x_blocks]
            lines.append(line)
        y_send[it, 0] = lines[1]
        y_send[it, 1] = lines[0] + wide(wy_turn[...]) * lines[1]
        y_all[it, row] = lines[1]
        for n, peer in enumerate(row_peers):
            send(y_send.at[it, lax.div(row + n + 1, rows)], y_all.at[it, row], y_sems.at[0, it],
                 y_sems.at[1, it], row=peer)
        stacked = jnp.concatenate(sides + [jnp.zeros((112, cells), f32)], axis=0).T
        for t in range(cells // 8):
            here = slice(t * 8, t * 8 + 8)
            tile = stacked[here]
            for z in range(planes):
                for j in range(x_blocks):
                    block = slice(j * cells, (j + 1) * cells)
                    n = j * planes + z
                    mix[z, here, block] = (
                        mix[z, here, block]
                        + tile[:, n : n + 1] * gend[0, j]
                        + tile[:, 8 + n : 9 + n] * gend[1, j]
                    )
        finish(y_sems.at[1, it], y_all.at[it, pl.ds(0, rows - 1)])
        carried = []
        for side in range(2):
            total = wide(wy_in[side, 0]) * y_all[it, 0]
            for k in range(1, rows):
                total = total + wide(wy_in[side, k]) * y_all[it, k]
            for z in range(planes):
                for j in range(x_blocks):
                    n = j * planes + z
                    carry_rows[2 * z + side, :, j * cells : (j + 1) * cells] = jnp.broadcast_to(
                        total[n : n + 1], (8, cells)
                    )
            carried.append(total)
        return sides, carried

    def settle(it, low, high, squares):
        def step(i, acc):
            here, padded = eight(i * 8), eight(i * 8 + 8)
            g_first = jnp.concatenate([gy_ends[0, here, :]] * groups, axis=1)
            g_last = jnp.concatenate([gy_ends[1, here, :]] * groups, axis=1)
            for z in range(planes):
                solved = mix[z, here, :] + g_first * carry_rows[2 * z] + g_last * carry_rows[2 * z + 1]
                d = jnp.concatenate([dz[it, z, g, padded, :] for g in range(groups)], axis=1)
                renewed = jnp.minimum(jnp.maximum(d + STEP * solved, fz[z, here, :]), 1.0)
                if it + 1 < ITERS:
                    keep_damage(it + 1, z, i * 8, renewed)
                change = renewed - d
                acc = acc + change * change
            return acc

        return lax.fori_loop(low // 8, high // 8, step, squares)

    def stream(it, ready):
        ready(order[0])
        ready(order[1])
        share_rows(it)
        a = 16
        for n in order[2:]:
            ready(n)
            b = cuts[n + 1] - 16 if n != order[-1] else cuts[4] + 16
            residual(it, a, b)
            x_product([(a, b)])
            a = b
            if n == order[2]:
                finish(v_sems.at[1, it], two_rows(it))
                mirror(it)
                residual(it, 0, 16)
                residual(it, cuts[4] + 16, cells)
                x_product([(0, 16), (cuts[4] + 16, cells)])

    def arrived(n):
        finish(d_rsem.at[n], piece_of(landing, cuts, n))
        regroup(cuts[n], cuts[n + 1])

    finish(e_sems.at[1], ez.at[others])
    scale_energy()
    stream(0, arrived)
    x_ends(0)
    x_share(0)
    for n in order[2:]:
        move_piece(bound, fz, n, f_ssem.at[0], f_rsem)
    for z in range(planes):
        y_product(0, z)
    finish(x_sems.at[1, 0], x_all.at[0, others])
    y_share(0)

    totals = []
    blank = jnp.zeros((8, width), f32)
    held = [blank]

    def settled(n):
        finish(f_rsem.at[n], piece_of(fz, cuts, n))
        held.append(settle(0, cuts[n], cuts[n + 1], held.pop()))

    stream(1, settled)
    def give_back(n, m):
        at = pl.ds(backs_at[n], backs_at[n + 1] - backs_at[n])
        send(final.at[col_peers[m], at, :], out.at[at, slab(col)], back_ssem.at[0],
             back_rsem.at[n], col=col_peers[m])

    def give_all(n):
        for m in range(cols - 1):
            give_back(n, m)

    def complete(low, high):
        @pl.loop(low // 8, high // 8)
        def _(i):
            here = eight(i * 8)
            tile = x_cols[here, :]
            ends_of = [
                jnp.concatenate([gy_ends[n, here, :]] * (cells // 128), axis=1) for n in range(2)
            ]
            for k in range(blocks):
                block = slice(k * cells, (k + 1) * cells)
                n = 8 * (k // x_blocks) + 2 * (k % x_blocks)
                value = (
                    out[here, block]
                    + tile[:, n : n + 1] * g_all[0, k]
                    + tile[:, n + 1 : n + 2] * g_all[1, k]
                    + (ends_of[0] * y_lines[0, k] + ends_of[1] * y_lines[1, k])
                )
                out[here, block] = jnp.minimum(jnp.maximum(value, bound[here, block]), 1.0)

    for m in range(cols - 1):
        y_first(1, col_peers[m])
        give_back(0, m)
    x_ends(1)
    x_share(1)
    for m in range(cols - 1):
        y_product(1, col_peers[m])
        give_back(1, m)
    y_first(1, col)
    y_product(1, col)
    out[:, slab(col)] = final[col]
    finish(x_sems.at[1, 1], x_all.at[1, others])
    sides, carried = y_share(1)
    for z in range(planes):
        for j in range(x_blocks):
            n = j * planes + z
            for side in range(2):
                at = 2 * j + side
                word_send[z, at : at + 1, :] = STEP * sides[side][n : n + 1]
                at += 2 * x_blocks
                word_send[z, at : at + 1, :] = STEP * carried[side][n : n + 1]
    for peer in col_peers:
        send(word_send.at[peer], word_all.at[col], w_sems.at[0], w_sems.at[1], col=peer)
    give_all(2)
    word_all[col] = word_send[col]
    totals.append(jnp.sum(held[0]))
    totals.append(jnp.sum(settle(ITERS - 1, 0, cells, blank)))
    s_send[...] = jnp.where(sub == 0, totals[0], jnp.where(sub == 1, totals[1], 0.0))
    for n, peer in enumerate(row_peers):
        send(s_send, s_row.at[n], s_sems.at[0], s_sems.at[1], row=peer)
    finish(s_sems.at[1], s_row)
    total = s_send[...]
    for n in range(rows - 1):
        total = total + s_row[n]
    s_col_send[...] = total
    for n, peer in enumerate(col_peers):
        send(s_col_send, s_col.at[n], s_sems.at[2], s_sems.at[3], col=peer)
    for n in range(3, len(backs_at) - 1):
        give_all(n)
    finish(w_sems.at[1], word_all.at[others])
    x_cols[...] = jnp.concatenate(
        [word_all[c] for c in range(cols)] + [jnp.zeros((128 - 8 * cols, cells), f32)], axis=0
    ).T
    for k in range(blocks):
        for side in range(2):
            at = 2 * x_blocks + 2 * (k % x_blocks) + side
            y_lines[side, k] = jnp.broadcast_to(
                word_all[k // x_blocks, at : at + 1, :], (8, cells)
            )
    for n in range(len(backs_at) - 2):
        finish(back_rsem.at[n], piece_of(final, backs_at, n))
        complete(backs_at[n], backs_at[n + 1])
    finish(s_sems.at[3], s_col)
    for n in range(cols - 1):
        total = total + s_col[n]
    sizes = jnp.sqrt(total / cell_count + EPSILON) / STEP
    norms[...] = jnp.where(lane == 0, sizes[:1, :], sizes[1:2, :])[0, :ITERS]
    for it in range(ITERS):
        finish(x_sems.at[0, it], x_all.at[it, others])
        finish(y_sems.at[0, it], y_all.at[it, pl.ds(0, rows - 1)])
        finish(v_sems.at[0, it], two_rows(it))
    finish(e_sems.at[0], ez.at[others])
    finish(d_ssem.at[0], landing.at[others])
    finish(f_ssem.at[0], fz.at[others])
    finish(w_sems.at[0], word_all.at[others])
    finish(s_sems.at[0], s_row)
    finish(s_sems.at[2], s_col)
    n = len(backs_at) - 2
    finish(back_rsem.at[n], piece_of(final, backs_at, n))
    complete(backs_at[n], backs_at[n + 1])
    finish(back_ssem.at[0], final.at[others])


def hand_over(damage, norms, damage_out, norms_out, sems):
    parts = 4
    part = damage.shape[0] // parts
    copies = [pltpu.make_async_copy(norms, norms_out, sems.at[parts])]
    for n in range(parts):
        at = pl.ds(n * part, part)
        copies.append(pltpu.make_async_copy(damage.at[at], damage_out.at[0, at], sems.at[n]))
    for copy in copies:
        copy.start()
    for copy in copies:
        copy.wait()


def local(energy, damage_old, crack_seeds, irreversible, line_inverses, z_inverse):
    planes, cells, line_length = energy.shape
    rows, cols = lax.axis_size("row"), lax.axis_size("col")
    blocks, _, _ = line_inverses.shape
    width = line_length // cols
    x_blocks = width // cells
    kinds = 2 * x_blocks + 2
    step = cells // 16
    cuts = (0, 3 * step, 8 * step, 12 * step, 13 * step, cells)
    backs_at = (0, 2 * step, 10 * step, 13 * step, 15 * step, cells)
    cell_count = float(cols * rows * cells * line_length)
    shape = (rows, cols, cells, width, x_blocks, blocks, cell_count, cuts, backs_at)
    f32 = jnp.float32
    bf16 = jnp.bfloat16
    dma = pltpu.SemaphoreType.DMA
    vmem = pl.BlockSpec(memory_space=pltpu.VMEM)
    damage, norms = pl.pallas_call(
        functools.partial(line_kernel, shape),
        out_shape=(
            pltpu.VMEM((cells, line_length), f32),
            pltpu.VMEM((ITERS,), f32),
        ),
        in_specs=[pl.BlockSpec(memory_space=pl.ANY)] * 6,
        out_specs=(vmem, vmem),
        scratch_shapes=[
            pltpu.VMEM((cells, line_length), f32),
            pltpu.VMEM((cells, line_length), jnp.int32),
            pltpu.VMEM((cells, line_length), jnp.int32),
            pltpu.VMEM((cells, line_length), f32),
            pltpu.VMEM((cells, line_length), f32),
            pltpu.VMEM((cells, line_length), f32),
            pltpu.VMEM((cols, cells, width), f32),
            pltpu.VMEM((cols, cells, width), f32),
            pltpu.VMEM((cols, cells, width), f32),
            pltpu.VMEM((cols, cells, width), f32),
            pltpu.VMEM((cols, cells, width), f32),
            pltpu.VMEM((ITERS, cols, width // 128, cells + 16, 128), f32),
            pltpu.VMEM((cols, cells, width), f32),
            pltpu.VMEM((cols, cells, width), bf16),
            pltpu.VMEM((cols, cells, width), bf16),
            pltpu.VMEM((cols, cells, width), bf16),
            pltpu.VMEM((cols, cells, width), bf16),
            pltpu.VMEM((cols, cells, width), f32),
            pltpu.VMEM((blocks, cells, cells), f32),
            pltpu.VMEM((x_blocks, cells, cells), bf16),
            pltpu.VMEM((x_blocks, cells, cells), bf16),
            pltpu.VMEM((2 * cells, cells), bf16),
            pltpu.VMEM((2, cells, 128), f32),
            pltpu.VMEM((2, x_blocks + 1, 8, cells), f32),
            pltpu.VMEM((kinds, 8, 128), f32),
            pltpu.VMEM((2 * x_blocks, cols, 8, 128), f32),
            pltpu.VMEM((2 * x_blocks, kinds, 8, 128), f32),
            pltpu.VMEM((2, rows, 8, 128), f32),
            pltpu.VMEM((8, 128), f32),
            pltpu.VMEM((2 * cols, 8, width), f32),
            pltpu.VMEM((kinds, 8, cells), f32),
            pltpu.VMEM((cols, 8, 128), f32),
            pltpu.VMEM((2, cols, 8, cells), f32),
            pltpu.VMEM((2, blocks, 8, cells), f32),
            pltpu.VMEM((cols, 8, cells), f32),
            pltpu.VMEM((cols, 8, cells), f32),
            pltpu.VMEM((cells, 128), f32),
            pltpu.VMEM((2, blocks, 8, cells), f32),
            pltpu.VMEM((ITERS, 8, cells), f32),
            pltpu.VMEM((ITERS, cols, 8, cells), f32),
            pltpu.VMEM((ITERS, 2, 8, cells), f32),
            pltpu.VMEM((ITERS, rows, 8, cells), f32),
            pltpu.VMEM((8, 128), f32),
            pltpu.VMEM((rows - 1, 8, 128), f32),
            pltpu.VMEM((8, 128), f32),
            pltpu.VMEM((cols - 1, 8, 128), f32),
            pltpu.SMEM((cols, cols), f32),
            dma((7,)),
            pltpu.SemaphoreType.REGULAR((2,)),
            dma((2,)),
            dma((1,)),
            dma((5,)),
            dma((1,)),
            dma((5,)),
            dma((1,)),
            dma((5,)),
            dma((2,)),
            dma((2, ITERS)),
            dma((2, ITERS)),
            dma((2, ITERS)),
            dma((4,)),
        ],
        compiler_params=pltpu.CompilerParams(
            has_side_effects=True, collective_id=0, vmem_limit_bytes=60 * 1024 * 1024
        ),
        name="line_iterations",
    )(
        z_inverse,
        energy[0],
        damage_old[0],
        crack_seeds[0],
        irreversible[0],
        line_inverses,
    )
    return pl.pallas_call(
        hand_over,
        out_shape=(
            jax.ShapeDtypeStruct((1, cells, line_length), f32),
            jax.ShapeDtypeStruct((ITERS,), f32),
        ),
        in_specs=[vmem, vmem],
        out_specs=(pl.BlockSpec(memory_space=pl.ANY), pl.BlockSpec(memory_space=pl.ANY)),
        scratch_shapes=[dma((5,))],
        compiler_params=pltpu.CompilerParams(vmem_limit_bytes=1024 * 1024),
        name="hand_over",
    )(
        pltpu.with_memory_space_constraint(damage, pltpu.VMEM),
        pltpu.with_memory_space_constraint(norms, pltpu.VMEM),
    )


def solution(mesh):
    def local_any(energy, damage_old, crack_seeds, irreversible, line_inverses, z_inverse):
        rows, cols = mesh.shape["row"], mesh.shape["col"]
        block_cells = line_inverses.shape[1]
        width = energy.shape[2] // cols
        whole_blocks = (
            energy.shape[0] == 1
            and energy.shape[1] == block_cells
            and width == 2 * block_cells
            and block_cells % 256 == 0
            and 2 * cols == 8
            and 2 * rows <= 128
            and min(rows, cols) > 2
        )
        chosen = local if whole_blocks else local_turned
        return chosen(energy, damage_old, crack_seeds, irreversible, line_inverses, z_inverse)

    return jax.shard_map(
        local_any,
        mesh=mesh,
        in_specs=(
            P("col", "row", None),
            P("col", "row", None),
            P("col", "row", None),
            P("col", "row", None),
            P(),
            P(),
        ),
        out_specs=(P("col", "row", None), P()),
        check_vma=False,
    )
```

```python
import functools

import jax
import jax.numpy as jnp
from jax import lax
from jax.experimental import pallas as pl
from jax.experimental.pallas import tpu as pltpu
from jax.sharding import PartitionSpec as P

ITERS = 2


KAPPA = 2.0
STEP = 0.02
COUPLE = 0.5
EPSILON = 1e-06
HIGHEST = lax.Precision.HIGHEST


def second_difference(grid_field, along):
    extent = grid_field.shape[along]
    forward_diff = lax.slice_in_dim(grid_field, 1, extent, axis=along) - lax.slice_in_dim(
        grid_field, 0, extent - 1, axis=along
    )
    zero_shape = list(grid_field.shape)
    zero_shape[along] = 1
    zero_rim = jnp.zeros(zero_shape, grid_field.dtype)
    ahead = jnp.concatenate([forward_diff, zero_rim], axis=along)
    behind = jnp.concatenate([zero_rim, forward_diff], axis=along)
    return ahead - behind


def line_solve(line_rows, inverses):
    block_count, block_cells, _ = inverses.shape
    line_count = line_rows.shape[0]
    blocks = line_rows.reshape(line_count, block_count, block_cells)
    products = jnp.einsum("rkb,kcb->rkc", blocks, inverses, precision=lax.Precision.HIGHEST)
    first_col = inverses[:, :, 0]
    last_col = inverses[:, :, block_cells - 1]
    incoming = [jnp.zeros((line_count,), line_rows.dtype)]
    for block_index in range(block_count - 1):
        incoming.append(
            products[:, block_index, block_cells - 1]
            + COUPLE * incoming[block_index] * inverses[block_index, block_cells - 1, 0]
        )
    inflow = jnp.stack(incoming, axis=1)
    forward = products + COUPLE * inflow[:, :, None] * first_col[None]
    head_terms = [jnp.zeros((line_count,), line_rows.dtype) for block_index in range(block_count)]
    carried = forward[:, block_count - 1, 0]
    for block_index in range(block_count - 2, -1, -1):
        head_terms[block_index] = carried
        carried = (
            forward[:, block_index, 0]
            + COUPLE * carried * inverses[block_index, 0, block_cells - 1]
        )
    outflow = jnp.stack(head_terms, axis=1)
    solved = forward + COUPLE * outflow[:, :, None] * last_col[None]
    return solved.reshape(line_count, block_count * block_cells)


def local_turned(energy, damage_old, crack_seeds, irreversible, line_inverses, z_inverse):
    planes, rows_here, line_length = energy.shape
    row_count = lax.axis_size("row")
    col_count = lax.axis_size("col")
    total_planes = planes * col_count
    cell_count = total_planes * rows_here * row_count * line_length
    seeded = crack_seeds == 1
    damage = jnp.where(seeded, 1.0, damage_old)
    lower_bound = jnp.where(irreversible == 1, damage_old, 0.0)
    own_sums = []
    for sweep_index in range(ITERS):
        local_lap = second_difference(damage, 2)
        partial_value = energy - (1.0 + energy) * damage + KAPPA * local_lap
        moved_part, moved_damage = (
            lax.all_to_all(
                lax.all_to_all(
                    jnp.swapaxes(partial_value, 1, 2),
                    "row",
                    split_axis=1,
                    concat_axis=2,
                    tiled=True,
                ),
                "col",
                split_axis=1,
                concat_axis=0,
                tiled=True,
            ),
            lax.all_to_all(
                lax.all_to_all(
                    jnp.swapaxes(damage, 1, 2), "row", split_axis=1, concat_axis=2, tiled=True
                ),
                "col",
                split_axis=1,
                concat_axis=0,
                tiled=True,
            ),
        )
        lap_rest = second_difference(moved_damage, 2) + second_difference(moved_damage, 0)
        turned = moved_part + KAPPA * lap_rest
        turned_shape = turned.shape
        along_y = line_solve(turned.reshape(-1, turned_shape[2]), line_inverses).reshape(
            turned_shape
        )
        along_z = jnp.einsum("zk,kxy->zxy", z_inverse, along_y, precision=lax.Precision.HIGHEST)
        gathered = lax.all_to_all(
            lax.all_to_all(along_z, "row", split_axis=2, concat_axis=1, tiled=True),
            "col",
            split_axis=0,
            concat_axis=1,
            tiled=True,
        )
        piece_cells = gathered.shape[1] // (row_count * col_count)
        reordered = gathered.reshape(planes, col_count, row_count, piece_cells, rows_here)
        restored = jnp.transpose(reordered, (0, 4, 2, 1, 3)).reshape(planes, rows_here, line_length)
        update = STEP * line_solve(restored.reshape(-1, line_length), line_inverses).reshape(
            restored.shape
        )
        clamped = jnp.minimum(jnp.maximum(damage + update, lower_bound), 1.0)
        renewed = jnp.where(seeded, 1.0, clamped)
        own_sum = jnp.sum((renewed - damage) ** 2)
        own_sums.append(own_sum)
        damage = renewed
    global_sums = lax.psum(jnp.stack(own_sums), ("row", "col"))
    update_norms = jnp.sqrt(global_sums / cell_count + EPSILON) / STEP
    return (damage, update_norms)


def line_kernel(
    shape,
    z_hbm,
    energy,
    damage_hbm,
    seeds_hbm,
    irreversible_hbm,
    inverses,
    out,
    norms,
    damage_old,
    crack_seeds,
    irreversible,
    e_home,
    start,
    bound,
    ez,
    ec,
    fz,
    landing,
    dx,
    dz,
    final,
    w_high,
    w_low,
    a_high,
    a_low,
    mix,
    inverse,
    gx_high,
    gx_low,
    gy_both,
    gy_ends,
    gend,
    wx_send,
    wx_in,
    wx_own,
    wy_in,
    wy_turn,
    carry_rows,
    own_rows,
    w_mix,
    y_base,
    g_all,
    word_send,
    word_all,
    x_cols,
    y_lines,
    x_send,
    x_all,
    y_send,
    y_all,
    s_send,
    s_row,
    s_col_send,
    s_col,
    z_inv,
    local_sems,
    greet,
    e_sems,
    d_ssem,
    d_rsem,
    f_ssem,
    f_rsem,
    back_ssem,
    back_rsem,
    w_sems,
    x_sems,
    v_sems,
    y_sems,
    s_sems,
):
    rows, cols, cells, width, x_blocks, blocks, cell_count, cuts, backs_at = shape
    planes = cols
    last = cells - 1
    groups = width // 128
    kinds = 2 * x_blocks + 2
    f32 = jnp.float32
    row, col = lax.axis_index("row"), lax.axis_index("col")
    row_peers = [lax.rem(row + o, rows) for o in range(1, rows)]
    col_peers = [lax.rem(col + o, cols) for o in range(1, cols)]

    def slab(who):
        return pl.ds(pl.multiple_of(who * width, width), width)

    def eight(at):
        return pl.ds(pl.multiple_of(at, 8), 8)

    def send(src, dst, ssem, rsem, **where):
        copy = pltpu.make_async_remote_copy(
            src_ref=src, dst_ref=dst, send_sem=ssem, recv_sem=rsem,
            device_id=where, device_id_type=pl.DeviceIdType.MESH,
        )
        copy.start()
        return copy

    def finish(sem, sized):
        pltpu.make_async_copy(sized, sized, sem).wait()

    def split(a):
        high = a.astype(jnp.bfloat16)
        return high, (a - high.astype(f32)).astype(jnp.bfloat16)

    def dot(a, b):
        return jnp.dot(a, b, preferred_element_type=f32)

    barrier = pltpu.get_barrier_semaphore()
    for peer in col_peers:
        pl.semaphore_signal(
            barrier, inc=1, device_id={"col": peer}, device_id_type=pl.DeviceIdType.MESH
        )
    above, below = row > 0, row < rows - 1

    def signal_row(sem, who):
        pl.semaphore_signal(
            sem, inc=1, device_id={"row": who}, device_id_type=pl.DeviceIdType.MESH
        )

    @pl.when(above)
    def _():
        signal_row(barrier, row - 1)

    @pl.when(below)
    def _():
        signal_row(barrier, row + 1)

    pulls = [
        pltpu.make_async_copy(damage_hbm, damage_old, local_sems.at[0]),
        pltpu.make_async_copy(seeds_hbm, crack_seeds, local_sems.at[1]),
        pltpu.make_async_copy(irreversible_hbm, irreversible, local_sems.at[2]),
    ]
    fetch = [
        pltpu.make_async_copy(inverses, inverse, local_sems.at[4]),
        pltpu.make_async_copy(z_hbm, z_inv, local_sems.at[5]),
    ]
    e_cuts = (0, cells // 8, cells)
    e_parts = [pl.ds(a, b - a) for a, b in zip(e_cuts, e_cuts[1:])]
    loads = [
        pltpu.make_async_copy(energy.at[at], e_home.at[at], local_sems.at[(3, 6)[n]])
        for n, at in enumerate(e_parts)
    ]
    for copy in loads + pulls + fetch:
        copy.start()
    neighbours = jnp.where(above, 1, 0) + jnp.where(below, 1, 0)
    pl.semaphore_wait(barrier, cols - 1 + neighbours)

    def move_piece(src, target, index, ssem, rsem):
        at = pl.ds(cuts[index], cuts[index + 1] - cuts[index])
        for peer in col_peers:
            send(src.at[at, slab(peer)], target.at[col, at, :], ssem, rsem.at[index], col=peer)

    others = pl.ds(0, cols - 1)

    def piece_of(target, marks, index):
        return target.at[others, pl.ds(marks[index], marks[index + 1] - marks[index]), :]

    for copy, at in zip(loads, e_parts):
        copy.wait()
        for peer in col_peers:
            send(e_home.at[at, slab(peer)], ez.at[col, at, :], e_sems.at[0], e_sems.at[1], col=peer)
    for copy in pulls:
        copy.wait()

    @pl.loop(0, cells // 16)
    def _(i):
        at = pl.ds(pl.multiple_of(i * 16, 16), 16)
        old = damage_old[at, :]
        seeded = crack_seeds[at, :] == 1
        start[at, :] = jnp.where(seeded, 1.0, old)
        bound[at, :] = jnp.where(seeded, 1.0, jnp.where(irreversible[at, :] == 1, old, 0.0))

    order = (0, 4, 1, 2, 3)
    for n in order:
        move_piece(start, landing, n, d_ssem.at[0], d_rsem)
    for n in order[:2]:
        move_piece(bound, fz, n, f_ssem.at[0], f_rsem)
    ez[col] = e_home[:, slab(col)]
    landing[col] = start[:, slab(col)]
    fz[col] = bound[:, slab(col)]

    lane = lax.broadcasted_iota(jnp.int32, (8, 128), 1)
    sub = lax.broadcasted_iota(jnp.int32, (8, 128), 0)
    upper_half = sub < planes
    zero = jnp.zeros((8, 128), f32)
    for copy in fetch:
        copy.wait()

    def lane_of(a, n):
        return jnp.broadcast_to(a[:, n : n + 1], (8, 128))

    def corner_of(down, over, k):
        tile = inverse[k, (cells - 8) * down : (cells - 8) * down + 8, (cells - 128) * over : (cells - 128) * over + 128]
        at = (7 if down else 0, 127 if over else 0)
        return jnp.broadcast_to(tile[at[0] : at[0] + 1, at[1] : at[1] + 1], (8, 128))

    def hot(index):
        return jnp.where(lane == index, 1.0, 0.0)

    def carries(first, final_of, lower=None, upper=None):
        firsts, finals = [], []
        low = [None if lower is None else lower(k) for k in range(blocks)]
        high = [None if upper is None else upper(k) for k in range(blocks)]
        for k in range(blocks):
            begin, end = hot(first(k)), hot(final_of(k))
            if low[k] is not None:
                begin = begin + corner_of(0, 0, k) * hot(low[k])
                end = end + corner_of(1, 0, k) * hot(low[k])
            if high[k] is not None:
                begin = begin + corner_of(0, 1, k) * hot(high[k])
                end = end + corner_of(1, 1, k) * hot(high[k])
            firsts.append(begin)
            finals.append(end)
        incoming = [zero]
        for k in range(blocks - 1):
            incoming.append(finals[k] + COUPLE * corner_of(1, 0, k) * incoming[k])
        heads = [
            firsts[k] + COUPLE * corner_of(0, 0, k) * incoming[k] for k in range(blocks)
        ]
        carried = heads[blocks - 1]
        outgoing = [zero] * blocks
        for k in range(blocks - 2, -1, -1):
            outgoing[k] = carried
            carried = heads[k] + COUPLE * corner_of(0, 1, k) * carried
        enter, leave = [], []
        for k in range(blocks):
            enter.append(COUPLE * incoming[k] + (zero if low[k] is None else hot(low[k])))
            leave.append(COUPLE * outgoing[k] + (zero if high[k] is None else hot(high[k])))
        return incoming, outgoing, enter, leave

    def picked(which, options):
        total = zero
        for n, option in enumerate(options):
            if option is not None:
                total = total + jnp.where(which == n, option, 0.0)
        return total

    def at_own(c, weights):
        return pltpu.roll(weights, 128 - 8 * c, 1) if c > 0 else weights

    def left_of(k):
        c = k // x_blocks
        return 8 * (c - 1) + 2 * x_blocks + 1 if k % x_blocks == 0 and c > 0 else None

    def right_of(k):
        c = k // x_blocks
        return 8 * (c + 1) + 2 * x_blocks if k % x_blocks == x_blocks - 1 and c < cols - 1 else None

    incoming, outgoing, enter, leave = carries(
        lambda k: 8 * (k // x_blocks) + k % x_blocks,
        lambda k: 8 * (k // x_blocks) + x_blocks + k % x_blocks,
        left_of,
        right_of,
    )
    to_right = picked(col, [
        at_own(c, incoming[(c + 1) * x_blocks] + hot(8 * c + 2 * x_blocks + 1) / COUPLE)
        if c < cols - 1 else None
        for c in range(cols)
    ])
    to_left = picked(col, [
        at_own(c, leave[c * x_blocks - 1] / COUPLE) if c > 0 else None for c in range(cols)
    ])
    for n in range(kinds):
        wx_send[n] = jnp.where(upper_half, lane_of(to_right, n), lane_of(to_left, n))
    for m in range(2 * x_blocks):
        table = (enter, leave)[m % 2]
        everywhere = picked(col, [table[c * x_blocks + m // 2] for c in range(cols)])
        here = picked(col, [at_own(c, table[c * x_blocks + m // 2]) for c in range(cols)])
        for c in range(cols):
            from_left = jnp.where(col > c, lane_of(everywhere, 8 * c + 2 * x_blocks - 1), 0.0)
            from_right = jnp.where(col < c, lane_of(everywhere, 8 * c), 0.0)
            wx_in[m, c] = jnp.where(upper_half, from_left, from_right)
        for n in range(kinds):
            wx_own[m, n] = lane_of(here, n)

    incoming, outgoing, enter, leave = carries(lambda k: 2 * k, lambda k: 2 * k + 1)
    enters, leaves = picked(row, enter), picked(row, leave)
    for k in range(rows):
        wy_in[0, k] = lane_of(enters, 2 * k + 1)
        wy_in[1, k] = jnp.where(row >= k, lane_of(leaves, 2 * k + 1), lane_of(leaves, 2 * k))
    wy_turn[...] = picked(
        row, [lane_of(outgoing[k - 1], 2 * k + 1) if k > 0 else None for k in range(rows)]
    )

    upper_wide = lax.broadcasted_iota(jnp.int32, (8, cells), 0) < planes
    for j in range(x_blocks):
        turned = inverse[col * x_blocks + j].T
        gx_high[j], gx_low[j] = split(turned)
        for side, at in ((0, 0), (1, last)):
            line = jnp.broadcast_to(turned[at : at + 1], (8, cells))
            gend[side, j] = line
            if j == 0:
                gend[side, x_blocks] = line
            else:
                gend[side, x_blocks] = jnp.where(upper_wide, gend[side, x_blocks], line)
    gy = inverse[row]
    gy_both[:cells], gy_both[cells:] = split(gy)
    gy_ends[0] = jnp.broadcast_to(gy[:, :1], (cells, 128))
    gy_ends[1] = jnp.broadcast_to(gy[:, last:], (cells, 128))

    for k in range(blocks):
        for side, at in ((0, 0), (1, 127)):
            strip = inverse[k, :, (cells - 128) * side : (cells - 128) * side + 128]
            line = strip.T[at : at + 1]
            g_all[side, k] = jnp.broadcast_to(line, (8, cells))

    @pl.when(above)
    def _():
        pl.semaphore_wait(greet.at[0], 1)

    @pl.when(below)
    def _():
        signal_row(greet.at[0], row + 1)
        pl.semaphore_wait(greet.at[1], 1)

    @pl.when(above)
    def _():
        signal_row(greet.at[1], row - 1)

    first_col = jnp.where(col == 0, 1.0, 0.0)
    last_col = jnp.where(col == cols - 1, 1.0, 0.0)
    at_first, at_last = lane == 0, lane == 127

    def keep_damage(it, z, at, row_of):
        tiles = [row_of[:, g * 128 : (g + 1) * 128] for g in range(groups)]
        up = [pltpu.roll(tile, 1, 1) for tile in tiles]
        down = [pltpu.roll(tile, 127, 1) for tile in tiles]
        for g in range(groups):
            before = up[g - 1] if g > 0 else tiles[g] * first_col
            after = down[g + 1] if g < groups - 1 else tiles[g] * last_col
            dz[it, z, g, eight(at + 8), :] = tiles[g]
            dx[z, eight(at), g * 128 : (g + 1) * 128] = jnp.where(
                at_first, before, up[g]
            ) + jnp.where(at_last, after, down[g])

    mixing = [[KAPPA * z_inv[z, k] for k in range(planes)] for z in range(planes)]
    for k in range(planes):
        weights = zero
        for z in range(planes):
            weights = jnp.where(lax.rem(sub, planes) == z, mixing[z][k], weights)
        w_mix[k] = weights

    def scale_energy():
        @pl.loop(0, cells // 8)
        def _(i):
            for z in range(planes):
                sides = 4 + (z > 0) + (z < planes - 1)
                scaled = ez[z, eight(i * 8), :] * (1.0 / KAPPA)
                ez[z, eight(i * 8), :] = scaled
                ec[z, eight(i * 8), :] = scaled + (1.0 / KAPPA + sides)

    def regroup(low, high):
        @pl.loop(low // 8, high // 8, unroll=2)
        def _(i):
            for z in range(planes):
                keep_damage(0, z, i * 8, landing[z, eight(i * 8), :])

    def share_rows(it):
        send(dz.at[it, :, :, pl.ds(cells, 8), :], dz.at[it, :, :, pl.ds(0, 8), :],
             v_sems.at[0, it], v_sems.at[1, it], row=lax.rem(row + 1, rows))
        send(dz.at[it, :, :, pl.ds(8, 8), :], dz.at[it, :, :, pl.ds(cells + 8, 8), :],
             v_sems.at[0, it], v_sems.at[1, it], row=lax.rem(row + rows - 1, rows))

    def two_rows(it):
        return dz.at[it, :, :, pl.ds(0, 16), :]

    def mirror(it):
        for z in range(planes):
            for g in range(groups):
                dz[it, z, g, 7:8, :] = jnp.where(
                    row == 0, dz[it, z, g, 8:9, :], dz[it, z, g, 7:8, :]
                )
                dz[it, z, g, cells + 8 : cells + 9, :] = jnp.where(
                    row == rows - 1,
                    dz[it, z, g, cells + 7 : cells + 8, :],
                    dz[it, z, g, cells + 8 : cells + 9, :],
                )

    def residual(it, low, high):
        @pl.loop(low // 16, high // 16)
        def _(i):
            base = pl.multiple_of(i * 16, 16)
            here = pl.ds(base, 16)
            padded = pl.ds(pl.multiple_of(base + 8, 8), 16)
            for g in range(groups):
                lanes = slice(g * 128, (g + 1) * 128)
                mids = [dz[it, z, g, padded, :] for z in range(planes)]
                value = []
                for z in range(planes):
                    d = mids[z]
                    near = dz[it, z, g, pl.ds(base + 7, 16), :] + dz[it, z, g, pl.ds(base + 9, 16), :]
                    near = near + dx[z, here, lanes]
                    if z > 0:
                        near = near + mids[z - 1]
                    if z < planes - 1:
                        near = near + mids[z + 1]
                    value.append(near + (ez[z, here, lanes] - ec[z, here, lanes] * d))
                for z in range(planes):
                    total = mixing[z][0] * value[0]
                    for k in range(1, planes):
                        total = total + mixing[z][k] * value[k]
                    w_high[z, here, lanes], w_low[z, here, lanes] = split(total)

    def x_product(ranges):
        for j in range(x_blocks):
            block = slice(j * cells, (j + 1) * cells)
            parts = [(z, n) for z in range(planes) for n in range(len(ranges))]
            cut = [slice(*ranges[n]) for _, n in parts]
            high_rows = jnp.concatenate(
                [w_high[z, c, block] for (z, _), c in zip(parts, cut)], axis=0
            )
            low_rows = jnp.concatenate(
                [w_low[z, c, block] for (z, _), c in zip(parts, cut)], axis=0
            )
            count = high_rows.shape[0]
            twice = dot(jnp.concatenate([high_rows, low_rows], axis=0), gx_high[j])
            along = twice[:count] + (twice[count:] + dot(high_rows, gx_low[j]))
            at = 0
            for (z, n), c in zip(parts, cut):
                part = along[at : at + c.stop - c.start]
                at += c.stop - c.start
                a_high[z, c, block], a_low[z, c, block] = split(part)

    def y_times(high, low):
        twice = dot(gy_both[...], high)
        return twice[:cells] + (twice[cells:] + dot(gy_both[:cells], low))

    def y_product(it, z):
        both = y_times(a_high[z], a_low[z])
        mix[z] = both
        for side, at in ((0, 0), (1, last)):
            for j in range(x_blocks):
                y_base[side, z, j : j + 1, :] = both[at : at + 1, j * cells : (j + 1) * cells]
        if it + 1 == ITERS:
            low = backs_at[1]
            rest = pl.ds(8 + low, cells - low)
            d = jnp.concatenate([dz[it, z, g, rest, :] for g in range(groups)], axis=1)
            final[z, low:, :] = d + STEP * both[low:]

    def y_first(it, z):
        count = backs_at[1]
        pair = jnp.concatenate([gy_both[:count], gy_both[cells : cells + count]], axis=0)
        twice = dot(pair, a_high[z])
        both = twice[:count] + (twice[count:] + dot(gy_both[:count], a_low[z]))
        d = jnp.concatenate([dz[it, z, g, pl.ds(8, count), :] for g in range(groups)], axis=1)
        final[z, :count, :] = d + STEP * both

    def x_ends(it):
        tile_lane = lax.broadcasted_iota(jnp.int32, (cells, 128), 1)
        near = pl.ds(8, cells)
        pack = jnp.zeros((cells, 128), f32)
        for z in range(planes):
            tiles = []
            for j in range(x_blocks):
                for spot, at, start_lane in (
                    (j, j * cells, 0), (x_blocks + j, (j + 1) * cells - 128, 127)
                ):
                    lanes = slice(at, at + 128)
                    tile = a_high[z, :, lanes].astype(f32) + a_low[z, :, lanes].astype(f32)
                    tiles.append((tile, start_lane, spot * planes + z))
            tiles.append((dz[it, z, 0, near, :], 0, 2 * x_blocks * planes + z))
            tiles.append((dz[it, z, groups - 1, near, :], 127, (2 * x_blocks + 1) * planes + z))
            for tile, lane_from, lane_to in tiles:
                if lane_from != lane_to:
                    tile = pltpu.roll(tile, (lane_to - lane_from) % 128, 1)
                pack = jnp.where(tile_lane == lane_to, tile, pack)
        turned = y_times(*split(pack)).T

        def keep(n, tile):
            other = pltpu.roll(tile, planes, 0)
            pair = (tile, other) if n % 2 == 0 else (other, tile)
            own_rows[n] = jnp.where(upper_wide, pair[0], pair[1])

        for n in range(2 * x_blocks):
            keep(n, turned[8 * (n // 2) : 8 * (n // 2) + 8])
        tile = turned[8 * x_blocks : 8 * x_blocks + 8]
        total = None
        for k in range(planes):
            line = jnp.where(
                upper_wide,
                jnp.broadcast_to(tile[k : k + 1], (8, cells)),
                jnp.broadcast_to(tile[planes + k : planes + k + 1], (8, cells)),
            )
            term = wide(w_mix[k]) * line
            total = term if total is None else total + term
        for n in range(2):
            keep(2 * x_blocks + n, total)

    def wide(weights):
        return jnp.concatenate([weights] * (cells // 128), axis=1)

    def x_share(it):
        total = None
        for n in range(kinds):
            term = wide(wx_send[n]) * own_rows[n]
            total = term if total is None else total + term
        x_send[it] = total
        x_all[it, col] = total
        for peer in col_peers:
            send(x_send.at[it], x_all.at[it, col], x_sems.at[0, it], x_sems.at[1, it], col=peer)

    def y_share(it):
        sides = []
        for side in range(2):
            parts = []
            for j in range(x_blocks):
                m = 2 * j + side
                total = wide(wx_in[m, 0]) * x_all[it, 0]
                for c in range(1, cols):
                    total = total + wide(wx_in[m, c]) * x_all[it, c]
                total = total + pltpu.roll(total, planes, 0)
                for n in range(kinds):
                    total = total + wide(wx_own[m, n]) * own_rows[n]
                parts.append(total)
            sides.append(jnp.where(upper_wide, parts[0], parts[1]))
        lines = []
        for side, at in ((0, 0), (1, last)):
            line = jnp.concatenate(
                [y_base[side, z, j : j + 1, :] for j in range(x_blocks) for z in range(planes)],
                axis=0,
            )
            for n in range(2):
                scale = jnp.broadcast_to(sides[n][:, at : at + 1], (8, cells))
                line = line + scale * gend[n, x_blocks]
            lines.append(line)
        y_send[it, 0] = lines[1]
        y_send[it, 1] = lines[0] + wide(wy_turn[...]) * lines[1]
        y_all[it, row] = lines[1]
        for n, peer in enumerate(row_peers):
            send(y_send.at[it, lax.div(row + n + 1, rows)], y_all.at[it, row], y_sems.at[0, it],
                 y_sems.at[1, it], row=peer)
        stacked = jnp.concatenate(sides + [jnp.zeros((112, cells), f32)], axis=0).T
        for t in range(cells // 8):
            here = slice(t * 8, t * 8 + 8)
            tile = stacked[here]
            for z in range(planes):
                for j in range(x_blocks):
                    block = slice(j * cells, (j + 1) * cells)
                    n = j * planes + z
                    mix[z, here, block] = (
                        mix[z, here, block]
                        + tile[:, n : n + 1] * gend[0, j]
                        + tile[:, 8 + n : 9 + n] * gend[1, j]
                    )
        finish(y_sems.at[1, it], y_all.at[it, pl.ds(0, rows - 1)])
        carried = []
        for side in range(2):
            total = wide(wy_in[side, 0]) * y_all[it, 0]
            for k in range(1, rows):
                total = total + wide(wy_in[side, k]) * y_all[it, k]
            for z in range(planes):
                for j in range(x_blocks):
                    n = j * planes + z
                    carry_rows[2 * z + side, :, j * cells : (j + 1) * cells] = jnp.broadcast_to(
                        total[n : n + 1], (8, cells)
                    )
            carried.append(total)
        return sides, carried

    def settle(it, low, high, squares):
        def step(i, acc):
            here, padded = eight(i * 8), eight(i * 8 + 8)
            g_first = jnp.concatenate([gy_ends[0, here, :]] * groups, axis=1)
            g_last = jnp.concatenate([gy_ends[1, here, :]] * groups, axis=1)
            for z in range(planes):
                solved = mix[z, here, :] + g_first * carry_rows[2 * z] + g_last * carry_rows[2 * z + 1]
                d = jnp.concatenate([dz[it, z, g, padded, :] for g in range(groups)], axis=1)
                renewed = jnp.minimum(jnp.maximum(d + STEP * solved, fz[z, here, :]), 1.0)
                if it + 1 < ITERS:
                    keep_damage(it + 1, z, i * 8, renewed)
                change = renewed - d
                acc = acc + change * change
            return acc

        return lax.fori_loop(low // 8, high // 8, step, squares, unroll=2)

    def stream(it, ready):
        ready(order[0])
        ready(order[1])
        share_rows(it)
        a = 16
        for n in order[2:]:
            ready(n)
            b = cuts[n + 1] - 16 if n != order[-1] else cuts[4] + 16
            residual(it, a, b)
            x_product([(a, b)])
            a = b
            if n == order[2]:
                finish(v_sems.at[1, it], two_rows(it))
                mirror(it)
                residual(it, 0, 16)
                residual(it, cuts[4] + 16, cells)
                x_product([(0, 16), (cuts[4] + 16, cells)])

    def arrived(n):
        finish(d_rsem.at[n], piece_of(landing, cuts, n))
        regroup(cuts[n], cuts[n + 1])

    finish(e_sems.at[1], ez.at[others])
    scale_energy()
    stream(0, arrived)
    x_ends(0)
    x_share(0)
    for n in order[2:]:
        move_piece(bound, fz, n, f_ssem.at[0], f_rsem)
    for z in range(planes):
        y_product(0, z)
    finish(x_sems.at[1, 0], x_all.at[0, others])
    y_share(0)

    totals = []
    blank = jnp.zeros((8, width), f32)
    held = [blank]

    def settled(n):
        finish(f_rsem.at[n], piece_of(fz, cuts, n))
        held.append(settle(0, cuts[n], cuts[n + 1], held.pop()))

    stream(1, settled)
    def give_back(n, m):
        at = pl.ds(backs_at[n], backs_at[n + 1] - backs_at[n])
        send(final.at[col_peers[m], at, :], out.at[at, slab(col)], back_ssem.at[0],
             back_rsem.at[n], col=col_peers[m])

    def give_all(n):
        for m in range(cols - 1):
            give_back(n, m)

    def complete(low, high):
        @pl.loop(low // 8, high // 8)
        def _(i):
            here = eight(i * 8)
            tile = x_cols[here, :]
            ends_of = [
                jnp.concatenate([gy_ends[n, here, :]] * (cells // 128), axis=1) for n in range(2)
            ]
            for k in range(blocks):
                block = slice(k * cells, (k + 1) * cells)
                n = 8 * (k // x_blocks) + 2 * (k % x_blocks)
                value = (
                    out[here, block]
                    + tile[:, n : n + 1] * g_all[0, k]
                    + tile[:, n + 1 : n + 2] * g_all[1, k]
                    + (ends_of[0] * y_lines[0, k] + ends_of[1] * y_lines[1, k])
                )
                out[here, block] = jnp.minimum(jnp.maximum(value, bound[here, block]), 1.0)

    for m in range(cols - 1):
        y_first(1, col_peers[m])
        give_back(0, m)
    x_ends(1)
    x_share(1)
    for m in range(cols - 1):
        y_product(1, col_peers[m])
        give_back(1, m)
    y_first(1, col)
    y_product(1, col)
    out[:, slab(col)] = final[col]
    finish(x_sems.at[1, 1], x_all.at[1, others])
    sides, carried = y_share(1)
    for z in range(planes):
        for j in range(x_blocks):
            n = j * planes + z
            for side in range(2):
                at = 2 * j + side
                word_send[z, at : at + 1, :] = STEP * sides[side][n : n + 1]
                at += 2 * x_blocks
                word_send[z, at : at + 1, :] = STEP * carried[side][n : n + 1]
    for peer in col_peers:
        send(word_send.at[peer], word_all.at[col], w_sems.at[0], w_sems.at[1], col=peer)
    give_all(2)
    word_all[col] = word_send[col]
    totals.append(jnp.sum(held[0]))
    totals.append(jnp.sum(settle(ITERS - 1, 0, cells, blank)))
    s_send[...] = jnp.where(sub == 0, totals[0], jnp.where(sub == 1, totals[1], 0.0))
    for n, peer in enumerate(row_peers):
        send(s_send, s_row.at[n], s_sems.at[0], s_sems.at[1], row=peer)
    finish(s_sems.at[1], s_row)
    total = s_send[...]
    for n in range(rows - 1):
        total = total + s_row[n]
    s_col_send[...] = total
    for n, peer in enumerate(col_peers):
        send(s_col_send, s_col.at[n], s_sems.at[2], s_sems.at[3], col=peer)
    for n in range(3, len(backs_at) - 1):
        give_all(n)
    finish(w_sems.at[1], word_all.at[others])
    x_cols[...] = jnp.concatenate(
        [word_all[c] for c in range(cols)] + [jnp.zeros((128 - 8 * cols, cells), f32)], axis=0
    ).T
    for k in range(blocks):
        for side in range(2):
            at = 2 * x_blocks + 2 * (k % x_blocks) + side
            y_lines[side, k] = jnp.broadcast_to(
                word_all[k // x_blocks, at : at + 1, :], (8, cells)
            )
    for n in range(len(backs_at) - 2):
        finish(back_rsem.at[n], piece_of(final, backs_at, n))
        complete(backs_at[n], backs_at[n + 1])
    finish(s_sems.at[3], s_col)
    for n in range(cols - 1):
        total = total + s_col[n]
    sizes = jnp.sqrt(total / cell_count + EPSILON) / STEP
    norms[...] = jnp.where(lane == 0, sizes[:1, :], sizes[1:2, :])[0, :ITERS]
    for it in range(ITERS):
        finish(x_sems.at[0, it], x_all.at[it, others])
        finish(y_sems.at[0, it], y_all.at[it, pl.ds(0, rows - 1)])
        finish(v_sems.at[0, it], two_rows(it))
    finish(e_sems.at[0], ez.at[others])
    finish(d_ssem.at[0], landing.at[others])
    finish(f_ssem.at[0], fz.at[others])
    finish(w_sems.at[0], word_all.at[others])
    finish(s_sems.at[0], s_row)
    finish(s_sems.at[2], s_col)
    n = len(backs_at) - 2
    finish(back_rsem.at[n], piece_of(final, backs_at, n))
    complete(backs_at[n], backs_at[n + 1])
    finish(back_ssem.at[0], final.at[others])


def hand_over(damage, norms, damage_out, norms_out, sems):
    parts = 4
    part = damage.shape[0] // parts
    copies = [pltpu.make_async_copy(norms, norms_out, sems.at[parts])]
    for n in range(parts):
        at = pl.ds(n * part, part)
        copies.append(pltpu.make_async_copy(damage.at[at], damage_out.at[0, at], sems.at[n]))
    for copy in copies:
        copy.start()
    for copy in copies:
        copy.wait()


def local(energy, damage_old, crack_seeds, irreversible, line_inverses, z_inverse):
    planes, cells, line_length = energy.shape
    rows, cols = lax.axis_size("row"), lax.axis_size("col")
    blocks, _, _ = line_inverses.shape
    width = line_length // cols
    x_blocks = width // cells
    kinds = 2 * x_blocks + 2
    step = cells // 16
    cuts = (0, 3 * step, 8 * step, 12 * step, 13 * step, cells)
    backs_at = (0, 2 * step, 10 * step, 13 * step, 15 * step, cells)
    cell_count = float(cols * rows * cells * line_length)
    shape = (rows, cols, cells, width, x_blocks, blocks, cell_count, cuts, backs_at)
    f32 = jnp.float32
    bf16 = jnp.bfloat16
    dma = pltpu.SemaphoreType.DMA
    vmem = pl.BlockSpec(memory_space=pltpu.VMEM)
    damage, norms = pl.pallas_call(
        functools.partial(line_kernel, shape),
        out_shape=(
            pltpu.VMEM((cells, line_length), f32),
            pltpu.VMEM((ITERS,), f32),
        ),
        in_specs=[pl.BlockSpec(memory_space=pl.ANY)] * 6,
        out_specs=(vmem, vmem),
        scratch_shapes=[
            pltpu.VMEM((cells, line_length), f32),
            pltpu.VMEM((cells, line_length), jnp.int32),
            pltpu.VMEM((cells, line_length), jnp.int32),
            pltpu.VMEM((cells, line_length), f32),
            pltpu.VMEM((cells, line_length), f32),
            pltpu.VMEM((cells, line_length), f32),
            pltpu.VMEM((cols, cells, width), f32),
            pltpu.VMEM((cols, cells, width), f32),
            pltpu.VMEM((cols, cells, width), f32),
            pltpu.VMEM((cols, cells, width), f32),
            pltpu.VMEM((cols, cells, width), f32),
            pltpu.VMEM((ITERS, cols, width // 128, cells + 16, 128), f32),
            pltpu.VMEM((cols, cells, width), f32),
            pltpu.VMEM((cols, cells, width), bf16),
            pltpu.VMEM((cols, cells, width), bf16),
            pltpu.VMEM((cols, cells, width), bf16),
            pltpu.VMEM((cols, cells, width), bf16),
            pltpu.VMEM((cols, cells, width), f32),
            pltpu.VMEM((blocks, cells, cells), f32),
            pltpu.VMEM((x_blocks, cells, cells), bf16),
            pltpu.VMEM((x_blocks, cells, cells), bf16),
            pltpu.VMEM((2 * cells, cells), bf16),
            pltpu.VMEM((2, cells, 128), f32),
            pltpu.VMEM((2, x_blocks + 1, 8, cells), f32),
            pltpu.VMEM((kinds, 8, 128), f32),
            pltpu.VMEM((2 * x_blocks, cols, 8, 128), f32),
            pltpu.VMEM((2 * x_blocks, kinds, 8, 128), f32),
            pltpu.VMEM((2, rows, 8, 128), f32),
            pltpu.VMEM((8, 128), f32),
            pltpu.VMEM((2 * cols, 8, width), f32),
            pltpu.VMEM((kinds, 8, cells), f32),
            pltpu.VMEM((cols, 8, 128), f32),
            pltpu.VMEM((2, cols, 8, cells), f32),
            pltpu.VMEM((2, blocks, 8, cells), f32),
            pltpu.VMEM((cols, 8, cells), f32),
            pltpu.VMEM((cols, 8, cells), f32),
            pltpu.VMEM((cells, 128), f32),
            pltpu.VMEM((2, blocks, 8, cells), f32),
            pltpu.VMEM((ITERS, 8, cells), f32),
            pltpu.VMEM((ITERS, cols, 8, cells), f32),
            pltpu.VMEM((ITERS, 2, 8, cells), f32),
            pltpu.VMEM((ITERS, rows, 8, cells), f32),
            pltpu.VMEM((8, 128), f32),
            pltpu.VMEM((rows - 1, 8, 128), f32),
            pltpu.VMEM((8, 128), f32),
            pltpu.VMEM((cols - 1, 8, 128), f32),
            pltpu.SMEM((cols, cols), f32),
            dma((7,)),
            pltpu.SemaphoreType.REGULAR((2,)),
            dma((2,)),
            dma((1,)),
            dma((5,)),
            dma((1,)),
            dma((5,)),
            dma((1,)),
            dma((5,)),
            dma((2,)),
            dma((2, ITERS)),
            dma((2, ITERS)),
            dma((2, ITERS)),
            dma((4,)),
        ],
        compiler_params=pltpu.CompilerParams(
            has_side_effects=True, collective_id=0, vmem_limit_bytes=60 * 1024 * 1024
        ),
        name="line_iterations",
    )(
        z_inverse,
        energy[0],
        damage_old[0],
        crack_seeds[0],
        irreversible[0],
        line_inverses,
    )
    return pl.pallas_call(
        hand_over,
        out_shape=(
            jax.ShapeDtypeStruct((1, cells, line_length), f32),
            jax.ShapeDtypeStruct((ITERS,), f32),
        ),
        in_specs=[vmem, vmem],
        out_specs=(pl.BlockSpec(memory_space=pl.ANY), pl.BlockSpec(memory_space=pl.ANY)),
        scratch_shapes=[dma((5,))],
        compiler_params=pltpu.CompilerParams(vmem_limit_bytes=1024 * 1024),
        name="hand_over",
    )(
        pltpu.with_memory_space_constraint(damage, pltpu.VMEM),
        pltpu.with_memory_space_constraint(norms, pltpu.VMEM),
    )


def solution(mesh):
    def local_any(energy, damage_old, crack_seeds, irreversible, line_inverses, z_inverse):
        rows, cols = mesh.shape["row"], mesh.shape["col"]
        block_cells = line_inverses.shape[1]
        width = energy.shape[2] // cols
        whole_blocks = (
            energy.shape[0] == 1
            and energy.shape[1] == block_cells
            and width == 2 * block_cells
            and block_cells % 256 == 0
            and 2 * cols == 8
            and 2 * rows <= 128
            and min(rows, cols) > 2
        )
        chosen = local if whole_blocks else local_turned
        return chosen(energy, damage_old, crack_seeds, irreversible, line_inverses, z_inverse)

    return jax.shard_map(
        local_any,
        mesh=mesh,
        in_specs=(
            P("col", "row", None),
            P("col", "row", None),
            P("col", "row", None),
            P("col", "row", None),
            P(),
            P(),
        ),
        out_specs=(P("col", "row", None), P()),
        check_vma=False,
    )
```

```python
import functools

import jax
import jax.numpy as jnp
from jax import lax
from jax.experimental import pallas as pl
from jax.experimental.pallas import tpu as pltpu
from jax.sharding import PartitionSpec as P

ITERS = 2


KAPPA = 2.0
STEP = 0.02
COUPLE = 0.5
EPSILON = 1e-06
HIGHEST = lax.Precision.HIGHEST


def second_difference(grid_field, along):
    extent = grid_field.shape[along]
    forward_diff = lax.slice_in_dim(grid_field, 1, extent, axis=along) - lax.slice_in_dim(
        grid_field, 0, extent - 1, axis=along
    )
    zero_shape = list(grid_field.shape)
    zero_shape[along] = 1
    zero_rim = jnp.zeros(zero_shape, grid_field.dtype)
    ahead = jnp.concatenate([forward_diff, zero_rim], axis=along)
    behind = jnp.concatenate([zero_rim, forward_diff], axis=along)
    return ahead - behind


def line_solve(line_rows, inverses):
    block_count, block_cells, _ = inverses.shape
    line_count = line_rows.shape[0]
    blocks = line_rows.reshape(line_count, block_count, block_cells)
    products = jnp.einsum("rkb,kcb->rkc", blocks, inverses, precision=lax.Precision.HIGHEST)
    first_col = inverses[:, :, 0]
    last_col = inverses[:, :, block_cells - 1]
    incoming = [jnp.zeros((line_count,), line_rows.dtype)]
    for block_index in range(block_count - 1):
        incoming.append(
            products[:, block_index, block_cells - 1]
            + COUPLE * incoming[block_index] * inverses[block_index, block_cells - 1, 0]
        )
    inflow = jnp.stack(incoming, axis=1)
    forward = products + COUPLE * inflow[:, :, None] * first_col[None]
    head_terms = [jnp.zeros((line_count,), line_rows.dtype) for block_index in range(block_count)]
    carried = forward[:, block_count - 1, 0]
    for block_index in range(block_count - 2, -1, -1):
        head_terms[block_index] = carried
        carried = (
            forward[:, block_index, 0]
            + COUPLE * carried * inverses[block_index, 0, block_cells - 1]
        )
    outflow = jnp.stack(head_terms, axis=1)
    solved = forward + COUPLE * outflow[:, :, None] * last_col[None]
    return solved.reshape(line_count, block_count * block_cells)


def local_turned(energy, damage_old, crack_seeds, irreversible, line_inverses, z_inverse):
    planes, rows_here, line_length = energy.shape
    row_count = lax.axis_size("row")
    col_count = lax.axis_size("col")
    total_planes = planes * col_count
    cell_count = total_planes * rows_here * row_count * line_length
    seeded = crack_seeds == 1
    damage = jnp.where(seeded, 1.0, damage_old)
    lower_bound = jnp.where(irreversible == 1, damage_old, 0.0)
    own_sums = []
    for sweep_index in range(ITERS):
        local_lap = second_difference(damage, 2)
        partial_value = energy - (1.0 + energy) * damage + KAPPA * local_lap
        moved_part, moved_damage = (
            lax.all_to_all(
                lax.all_to_all(
                    jnp.swapaxes(partial_value, 1, 2),
                    "row",
                    split_axis=1,
                    concat_axis=2,
                    tiled=True,
                ),
                "col",
                split_axis=1,
                concat_axis=0,
                tiled=True,
            ),
            lax.all_to_all(
                lax.all_to_all(
                    jnp.swapaxes(damage, 1, 2), "row", split_axis=1, concat_axis=2, tiled=True
                ),
                "col",
                split_axis=1,
                concat_axis=0,
                tiled=True,
            ),
        )
        lap_rest = second_difference(moved_damage, 2) + second_difference(moved_damage, 0)
        turned = moved_part + KAPPA * lap_rest
        turned_shape = turned.shape
        along_y = line_solve(turned.reshape(-1, turned_shape[2]), line_inverses).reshape(
            turned_shape
        )
        along_z = jnp.einsum("zk,kxy->zxy", z_inverse, along_y, precision=lax.Precision.HIGHEST)
        gathered = lax.all_to_all(
            lax.all_to_all(along_z, "row", split_axis=2, concat_axis=1, tiled=True),
            "col",
            split_axis=0,
            concat_axis=1,
            tiled=True,
        )
        piece_cells = gathered.shape[1] // (row_count * col_count)
        reordered = gathered.reshape(planes, col_count, row_count, piece_cells, rows_here)
        restored = jnp.transpose(reordered, (0, 4, 2, 1, 3)).reshape(planes, rows_here, line_length)
        update = STEP * line_solve(restored.reshape(-1, line_length), line_inverses).reshape(
            restored.shape
        )
        clamped = jnp.minimum(jnp.maximum(damage + update, lower_bound), 1.0)
        renewed = jnp.where(seeded, 1.0, clamped)
        own_sum = jnp.sum((renewed - damage) ** 2)
        own_sums.append(own_sum)
        damage = renewed
    global_sums = lax.psum(jnp.stack(own_sums), ("row", "col"))
    update_norms = jnp.sqrt(global_sums / cell_count + EPSILON) / STEP
    return (damage, update_norms)


def line_kernel(
    shape,
    z_hbm,
    energy,
    damage_hbm,
    seeds_hbm,
    irreversible_hbm,
    inverses,
    out,
    norms,
    damage_old,
    crack_seeds,
    irreversible,
    e_home,
    start,
    bound,
    ez,
    ec,
    fz,
    landing,
    dx,
    dz,
    final,
    w_high,
    w_low,
    a_high,
    a_low,
    mix,
    inverse,
    gx_high,
    gx_low,
    gy_both,
    gy_ends,
    gend,
    wx_send,
    wx_in,
    wx_own,
    wy_in,
    wy_turn,
    carry_rows,
    own_rows,
    w_mix,
    y_base,
    g_all,
    word_send,
    word_all,
    x_cols,
    y_lines,
    x_send,
    x_all,
    y_send,
    y_all,
    s_send,
    s_row,
    s_col_send,
    s_col,
    z_inv,
    local_sems,
    greet,
    e_sems,
    d_ssem,
    d_rsem,
    f_ssem,
    f_rsem,
    back_ssem,
    back_rsem,
    w_sems,
    x_sems,
    v_sems,
    y_sems,
    s_sems,
):
    rows, cols, cells, width, x_blocks, blocks, cell_count, cuts, backs_at = shape
    planes = cols
    last = cells - 1
    groups = width // 128
    kinds = 2 * x_blocks + 2
    f32 = jnp.float32
    row, col = lax.axis_index("row"), lax.axis_index("col")
    row_peers = [lax.rem(row + o, rows) for o in range(1, rows)]
    col_peers = [lax.rem(col + o, cols) for o in range(1, cols)]

    def slab(who):
        return pl.ds(pl.multiple_of(who * width, width), width)

    def eight(at):
        return pl.ds(pl.multiple_of(at, 8), 8)

    def send(src, dst, ssem, rsem, **where):
        copy = pltpu.make_async_remote_copy(
            src_ref=src, dst_ref=dst, send_sem=ssem, recv_sem=rsem,
            device_id=where, device_id_type=pl.DeviceIdType.MESH,
        )
        copy.start()
        return copy

    def finish(sem, sized):
        pltpu.make_async_copy(sized, sized, sem).wait()

    def split(a):
        high = a.astype(jnp.bfloat16)
        return high, (a - high.astype(f32)).astype(jnp.bfloat16)

    def dot(a, b):
        return jnp.dot(a, b, preferred_element_type=f32)

    barrier = pltpu.get_barrier_semaphore()
    for peer in col_peers:
        pl.semaphore_signal(
            barrier, inc=1, device_id={"col": peer}, device_id_type=pl.DeviceIdType.MESH
        )
    above, below = row > 0, row < rows - 1

    def signal_row(sem, who):
        pl.semaphore_signal(
            sem, inc=1, device_id={"row": who}, device_id_type=pl.DeviceIdType.MESH
        )

    @pl.when(above)
    def _():
        signal_row(barrier, row - 1)

    @pl.when(below)
    def _():
        signal_row(barrier, row + 1)

    pulls = [
        pltpu.make_async_copy(damage_hbm, damage_old, local_sems.at[0]),
        pltpu.make_async_copy(seeds_hbm, crack_seeds, local_sems.at[1]),
        pltpu.make_async_copy(irreversible_hbm, irreversible, local_sems.at[2]),
    ]
    fetch = [
        pltpu.make_async_copy(inverses, inverse, local_sems.at[4]),
        pltpu.make_async_copy(z_hbm, z_inv, local_sems.at[5]),
    ]
    e_cuts = (0, cells // 8, cells)
    e_parts = [pl.ds(a, b - a) for a, b in zip(e_cuts, e_cuts[1:])]
    loads = [
        pltpu.make_async_copy(energy.at[at], e_home.at[at], local_sems.at[(3, 6)[n]])
        for n, at in enumerate(e_parts)
    ]
    for copy in loads + pulls + fetch:
        copy.start()
    neighbours = jnp.where(above, 1, 0) + jnp.where(below, 1, 0)
    pl.semaphore_wait(barrier, cols - 1 + neighbours)

    def move_piece(src, target, index, ssem, rsem):
        at = pl.ds(cuts[index], cuts[index + 1] - cuts[index])
        for peer in col_peers:
            send(src.at[at, slab(peer)], target.at[col, at, :], ssem, rsem.at[index], col=peer)

    others = pl.ds(0, cols - 1)

    def piece_of(target, marks, index):
        return target.at[others, pl.ds(marks[index], marks[index + 1] - marks[index]), :]

    for copy, at in zip(loads, e_parts):
        copy.wait()
        for peer in col_peers:
            send(e_home.at[at, slab(peer)], ez.at[col, at, :], e_sems.at[0], e_sems.at[1], col=peer)
    for copy in pulls:
        copy.wait()

    @pl.loop(0, cells // 16)
    def _(i):
        at = pl.ds(pl.multiple_of(i * 16, 16), 16)
        old = damage_old[at, :]
        seeded = crack_seeds[at, :] == 1
        start[at, :] = jnp.where(seeded, 1.0, old)
        bound[at, :] = jnp.where(seeded, 1.0, jnp.where(irreversible[at, :] == 1, old, 0.0))

    order = (0, 4, 1, 2, 3)
    for n in order:
        move_piece(start, landing, n, d_ssem.at[0], d_rsem)
    for n in order[:2]:
        move_piece(bound, fz, n, f_ssem.at[0], f_rsem)
    ez[col] = e_home[:, slab(col)]
    landing[col] = start[:, slab(col)]
    fz[col] = bound[:, slab(col)]

    lane = lax.broadcasted_iota(jnp.int32, (8, 128), 1)
    sub = lax.broadcasted_iota(jnp.int32, (8, 128), 0)
    upper_half = sub < planes
    zero = jnp.zeros((8, 128), f32)
    for copy in fetch:
        copy.wait()

    def lane_of(a, n):
        return jnp.broadcast_to(a[:, n : n + 1], (8, 128))

    def corner_of(down, over, k):
        tile = inverse[k, (cells - 8) * down : (cells - 8) * down + 8, (cells - 128) * over : (cells - 128) * over + 128]
        at = (7 if down else 0, 127 if over else 0)
        return jnp.broadcast_to(tile[at[0] : at[0] + 1, at[1] : at[1] + 1], (8, 128))

    def hot(index):
        return jnp.where(lane == index, 1.0, 0.0)

    def carries(first, final_of, lower=None, upper=None):
        firsts, finals = [], []
        low = [None if lower is None else lower(k) for k in range(blocks)]
        high = [None if upper is None else upper(k) for k in range(blocks)]
        for k in range(blocks):
            begin, end = hot(first(k)), hot(final_of(k))
            if low[k] is not None:
                begin = begin + corner_of(0, 0, k) * hot(low[k])
                end = end + corner_of(1, 0, k) * hot(low[k])
            if high[k] is not None:
                begin = begin + corner_of(0, 1, k) * hot(high[k])
                end = end + corner_of(1, 1, k) * hot(high[k])
            firsts.append(begin)
            finals.append(end)
        incoming = [zero]
        for k in range(blocks - 1):
            incoming.append(finals[k] + COUPLE * corner_of(1, 0, k) * incoming[k])
        heads = [
            firsts[k] + COUPLE * corner_of(0, 0, k) * incoming[k] for k in range(blocks)
        ]
        carried = heads[blocks - 1]
        outgoing = [zero] * blocks
        for k in range(blocks - 2, -1, -1):
            outgoing[k] = carried
            carried = heads[k] + COUPLE * corner_of(0, 1, k) * carried
        enter, leave = [], []
        for k in range(blocks):
            enter.append(COUPLE * incoming[k] + (zero if low[k] is None else hot(low[k])))
            leave.append(COUPLE * outgoing[k] + (zero if high[k] is None else hot(high[k])))
        return incoming, outgoing, enter, leave

    def picked(which, options):
        total = zero
        for n, option in enumerate(options):
            if option is not None:
                total = total + jnp.where(which == n, option, 0.0)
        return total

    def at_own(c, weights):
        return pltpu.roll(weights, 128 - 8 * c, 1) if c > 0 else weights

    def left_of(k):
        c = k // x_blocks
        return 8 * (c - 1) + 2 * x_blocks + 1 if k % x_blocks == 0 and c > 0 else None

    def right_of(k):
        c = k // x_blocks
        return 8 * (c + 1) + 2 * x_blocks if k % x_blocks == x_blocks - 1 and c < cols - 1 else None

    incoming, outgoing, enter, leave = carries(
        lambda k: 8 * (k // x_blocks) + k % x_blocks,
        lambda k: 8 * (k // x_blocks) + x_blocks + k % x_blocks,
        left_of,
        right_of,
    )
    to_right = picked(col, [
        at_own(c, incoming[(c + 1) * x_blocks] + hot(8 * c + 2 * x_blocks + 1) / COUPLE)
        if c < cols - 1 else None
        for c in range(cols)
    ])
    to_left = picked(col, [
        at_own(c, leave[c * x_blocks - 1] / COUPLE) if c > 0 else None for c in range(cols)
    ])
    for n in range(kinds):
        wx_send[n] = jnp.where(upper_half, lane_of(to_right, n), lane_of(to_left, n))
    for m in range(2 * x_blocks):
        table = (enter, leave)[m % 2]
        everywhere = picked(col, [table[c * x_blocks + m // 2] for c in range(cols)])
        here = picked(col, [at_own(c, table[c * x_blocks + m // 2]) for c in range(cols)])
        for c in range(cols):
            from_left = jnp.where(col > c, lane_of(everywhere, 8 * c + 2 * x_blocks - 1), 0.0)
            from_right = jnp.where(col < c, lane_of(everywhere, 8 * c), 0.0)
            wx_in[m, c] = jnp.where(upper_half, from_left, from_right)
        for n in range(kinds):
            wx_own[m, n] = lane_of(here, n)

    incoming, outgoing, enter, leave = carries(lambda k: 2 * k, lambda k: 2 * k + 1)
    enters, leaves = picked(row, enter), picked(row, leave)
    for k in range(rows):
        wy_in[0, k] = lane_of(enters, 2 * k + 1)
        wy_in[1, k] = jnp.where(row >= k, lane_of(leaves, 2 * k + 1), lane_of(leaves, 2 * k))
    wy_turn[...] = picked(
        row, [lane_of(outgoing[k - 1], 2 * k + 1) if k > 0 else None for k in range(rows)]
    )

    upper_wide = lax.broadcasted_iota(jnp.int32, (8, cells), 0) < planes
    for j in range(x_blocks):
        turned = inverse[col * x_blocks + j].T
        gx_high[j], gx_low[j] = split(turned)
        for side, at in ((0, 0), (1, last)):
            line = jnp.broadcast_to(turned[at : at + 1], (8, cells))
            gend[side, j] = line
            if j == 0:
                gend[side, x_blocks] = line
            else:
                gend[side, x_blocks] = jnp.where(upper_wide, gend[side, x_blocks], line)
    gy = inverse[row]
    gy_both[:cells], gy_both[cells:] = split(gy)
    gy_ends[0] = jnp.broadcast_to(gy[:, :1], (cells, 128))
    gy_ends[1] = jnp.broadcast_to(gy[:, last:], (cells, 128))

    for k in range(blocks):
        for side, at in ((0, 0), (1, 127)):
            strip = inverse[k, :, (cells - 128) * side : (cells - 128) * side + 128]
            line = strip.T[at : at + 1]
            g_all[side, k] = jnp.broadcast_to(line, (8, cells))

    @pl.when(above)
    def _():
        pl.semaphore_wait(greet.at[0], 1)

    @pl.when(below)
    def _():
        signal_row(greet.at[0], row + 1)
        pl.semaphore_wait(greet.at[1], 1)

    @pl.when(above)
    def _():
        signal_row(greet.at[1], row - 1)

    first_col = jnp.where(col == 0, 1.0, 0.0)
    last_col = jnp.where(col == cols - 1, 1.0, 0.0)
    at_first, at_last = lane == 0, lane == 127

    def keep_damage(it, z, at, row_of):
        tiles = [row_of[:, g * 128 : (g + 1) * 128] for g in range(groups)]
        up = [pltpu.roll(tile, 1, 1) for tile in tiles]
        down = [pltpu.roll(tile, 127, 1) for tile in tiles]
        for g in range(groups):
            before = up[g - 1] if g > 0 else tiles[g] * first_col
            after = down[g + 1] if g < groups - 1 else tiles[g] * last_col
            dz[it, z, g, eight(at + 8), :] = tiles[g]
            dx[z, eight(at), g * 128 : (g + 1) * 128] = jnp.where(
                at_first, before, up[g]
            ) + jnp.where(at_last, after, down[g])

    mixing = [[KAPPA * z_inv[z, k] for k in range(planes)] for z in range(planes)]
    for k in range(planes):
        weights = zero
        for z in range(planes):
            weights = jnp.where(lax.rem(sub, planes) == z, mixing[z][k], weights)
        w_mix[k] = weights

    def scale_energy():
        @pl.loop(0, cells // 8)
        def _(i):
            for z in range(planes):
                sides = 4 + (z > 0) + (z < planes - 1)
                scaled = ez[z, eight(i * 8), :] * (1.0 / KAPPA)
                ez[z, eight(i * 8), :] = scaled
                ec[z, eight(i * 8), :] = scaled + (1.0 / KAPPA + sides)

    def regroup(low, high):
        @pl.loop(low // 8, high // 8, unroll=2)
        def _(i):
            for z in range(planes):
                keep_damage(0, z, i * 8, landing[z, eight(i * 8), :])

    def share_rows(it):
        send(dz.at[it, :, :, pl.ds(cells, 8), :], dz.at[it, :, :, pl.ds(0, 8), :],
             v_sems.at[0, it], v_sems.at[1, it], row=lax.rem(row + 1, rows))
        send(dz.at[it, :, :, pl.ds(8, 8), :], dz.at[it, :, :, pl.ds(cells + 8, 8), :],
             v_sems.at[0, it], v_sems.at[1, it], row=lax.rem(row + rows - 1, rows))

    def two_rows(it):
        return dz.at[it, :, :, pl.ds(0, 16), :]

    def mirror(it):
        for z in range(planes):
            for g in range(groups):
                dz[it, z, g, 7:8, :] = jnp.where(
                    row == 0, dz[it, z, g, 8:9, :], dz[it, z, g, 7:8, :]
                )
                dz[it, z, g, cells + 8 : cells + 9, :] = jnp.where(
                    row == rows - 1,
                    dz[it, z, g, cells + 7 : cells + 8, :],
                    dz[it, z, g, cells + 8 : cells + 9, :],
                )

    def residual(it, low, high):
        @pl.loop(low // 16, high // 16)
        def _(i):
            base = pl.multiple_of(i * 16, 16)
            here = pl.ds(base, 16)
            padded = pl.ds(pl.multiple_of(base + 8, 8), 16)
            for g in range(groups):
                lanes = slice(g * 128, (g + 1) * 128)
                mids = [dz[it, z, g, padded, :] for z in range(planes)]
                value = []
                for z in range(planes):
                    d = mids[z]
                    near = dz[it, z, g, pl.ds(base + 7, 16), :] + dz[it, z, g, pl.ds(base + 9, 16), :]
                    near = near + dx[z, here, lanes]
                    if z > 0:
                        near = near + mids[z - 1]
                    if z < planes - 1:
                        near = near + mids[z + 1]
                    value.append(near + (ez[z, here, lanes] - ec[z, here, lanes] * d))
                for z in range(planes):
                    total = mixing[z][0] * value[0]
                    for k in range(1, planes):
                        total = total + mixing[z][k] * value[k]
                    w_high[z, here, lanes], w_low[z, here, lanes] = split(total)

    def x_product(ranges):
        for j in range(x_blocks):
            block = slice(j * cells, (j + 1) * cells)
            parts = [(z, n) for z in range(planes) for n in range(len(ranges))]
            cut = [slice(*ranges[n]) for _, n in parts]
            high_rows = jnp.concatenate(
                [w_high[z, c, block] for (z, _), c in zip(parts, cut)], axis=0
            )
            low_rows = jnp.concatenate(
                [w_low[z, c, block] for (z, _), c in zip(parts, cut)], axis=0
            )
            count = high_rows.shape[0]
            twice = dot(jnp.concatenate([high_rows, low_rows], axis=0), gx_high[j])
            along = twice[:count] + (twice[count:] + dot(high_rows, gx_low[j]))
            at = 0
            for (z, n), c in zip(parts, cut):
                part = along[at : at + c.stop - c.start]
                at += c.stop - c.start
                a_high[z, c, block], a_low[z, c, block] = split(part)

    def y_times(high, low):
        twice = dot(gy_both[...], high)
        return twice[:cells] + (twice[cells:] + dot(gy_both[:cells], low))

    def y_product(it, z):
        both = y_times(a_high[z], a_low[z])
        mix[z] = both
        for side, at in ((0, 0), (1, last)):
            for j in range(x_blocks):
                y_base[side, z, j : j + 1, :] = both[at : at + 1, j * cells : (j + 1) * cells]
        if it + 1 == ITERS:
            low = backs_at[1]
            rest = pl.ds(8 + low, cells - low)
            d = jnp.concatenate([dz[it, z, g, rest, :] for g in range(groups)], axis=1)
            final[z, low:, :] = d + STEP * both[low:]

    def y_first(it, z):
        count = backs_at[1]
        pair = jnp.concatenate([gy_both[:count], gy_both[cells : cells + count]], axis=0)
        twice = dot(pair, a_high[z])
        both = twice[:count] + (twice[count:] + dot(gy_both[:count], a_low[z]))
        d = jnp.concatenate([dz[it, z, g, pl.ds(8, count), :] for g in range(groups)], axis=1)
        final[z, :count, :] = d + STEP * both

    def x_ends(it):
        tile_lane = lax.broadcasted_iota(jnp.int32, (cells, 128), 1)
        near = pl.ds(8, cells)
        pack = jnp.zeros((cells, 128), f32)
        for z in range(planes):
            tiles = []
            for j in range(x_blocks):
                for spot, at, start_lane in (
                    (j, j * cells, 0), (x_blocks + j, (j + 1) * cells - 128, 127)
                ):
                    lanes = slice(at, at + 128)
                    tile = a_high[z, :, lanes].astype(f32) + a_low[z, :, lanes].astype(f32)
                    tiles.append((tile, start_lane, spot * planes + z))
            tiles.append((dz[it, z, 0, near, :], 0, 2 * x_blocks * planes + z))
            tiles.append((dz[it, z, groups - 1, near, :], 127, (2 * x_blocks + 1) * planes + z))
            for tile, lane_from, lane_to in tiles:
                if lane_from != lane_to:
                    tile = pltpu.roll(tile, (lane_to - lane_from) % 128, 1)
                pack = jnp.where(tile_lane == lane_to, tile, pack)
        turned = y_times(*split(pack)).T

        def keep(n, tile):
            other = pltpu.roll(tile, planes, 0)
            pair = (tile, other) if n % 2 == 0 else (other, tile)
            own_rows[n] = jnp.where(upper_wide, pair[0], pair[1])

        for n in range(2 * x_blocks):
            keep(n, turned[8 * (n // 2) : 8 * (n // 2) + 8])
        tile = turned[8 * x_blocks : 8 * x_blocks + 8]
        total = None
        for k in range(planes):
            line = jnp.where(
                upper_wide,
                jnp.broadcast_to(tile[k : k + 1], (8, cells)),
                jnp.broadcast_to(tile[planes + k : planes + k + 1], (8, cells)),
            )
            term = wide(w_mix[k]) * line
            total = term if total is None else total + term
        for n in range(2):
            keep(2 * x_blocks + n, total)

    def wide(weights):
        return jnp.concatenate([weights] * (cells // 128), axis=1)

    def x_share(it):
        total = None
        for n in range(kinds):
            term = wide(wx_send[n]) * own_rows[n]
            total = term if total is None else total + term
        x_send[it] = total
        x_all[it, col] = total
        for peer in col_peers:
            send(x_send.at[it], x_all.at[it, col], x_sems.at[0, it], x_sems.at[1, it], col=peer)

    def y_share(it):
        sides = []
        for side in range(2):
            parts = []
            for j in range(x_blocks):
                m = 2 * j + side
                total = wide(wx_in[m, 0]) * x_all[it, 0]
                for c in range(1, cols):
                    total = total + wide(wx_in[m, c]) * x_all[it, c]
                total = total + pltpu.roll(total, planes, 0)
                for n in range(kinds):
                    total = total + wide(wx_own[m, n]) * own_rows[n]
                parts.append(total)
            sides.append(jnp.where(upper_wide, parts[0], parts[1]))
        lines = []
        for side, at in ((0, 0), (1, last)):
            line = jnp.concatenate(
                [y_base[side, z, j : j + 1, :] for j in range(x_blocks) for z in range(planes)],
                axis=0,
            )
            for n in range(2):
                scale = jnp.broadcast_to(sides[n][:, at : at + 1], (8, cells))
                line = line + scale * gend[n, x_blocks]
            lines.append(line)
        y_send[it, 0] = lines[1]
        y_send[it, 1] = lines[0] + wide(wy_turn[...]) * lines[1]
        y_all[it, row] = lines[1]
        for n, peer in enumerate(row_peers):
            send(y_send.at[it, lax.div(row + n + 1, rows)], y_all.at[it, row], y_sems.at[0, it],
                 y_sems.at[1, it], row=peer)
        stacked = jnp.concatenate(sides + [jnp.zeros((112, cells), f32)], axis=0).T
        for t in range(cells // 8):
            here = slice(t * 8, t * 8 + 8)
            tile = stacked[here]
            for z in range(planes):
                for j in range(x_blocks):
                    block = slice(j * cells, (j + 1) * cells)
                    n = j * planes + z
                    mix[z, here, block] = (
                        mix[z, here, block]
                        + tile[:, n : n + 1] * gend[0, j]
                        + tile[:, 8 + n : 9 + n] * gend[1, j]
                    )
        finish(y_sems.at[1, it], y_all.at[it, pl.ds(0, rows - 1)])
        carried = []
        for side in range(2):
            total = wide(wy_in[side, 0]) * y_all[it, 0]
            for k in range(1, rows):
                total = total + wide(wy_in[side, k]) * y_all[it, k]
            for z in range(planes):
                for j in range(x_blocks):
                    n = j * planes + z
                    carry_rows[2 * z + side, :, j * cells : (j + 1) * cells] = jnp.broadcast_to(
                        total[n : n + 1], (8, cells)
                    )
            carried.append(total)
        return sides, carried

    def settle(it, low, high, squares):
        def step(i, acc):
            here, padded = eight(i * 8), eight(i * 8 + 8)
            g_first = jnp.concatenate([gy_ends[0, here, :]] * groups, axis=1)
            g_last = jnp.concatenate([gy_ends[1, here, :]] * groups, axis=1)
            for z in range(planes):
                solved = mix[z, here, :] + g_first * carry_rows[2 * z] + g_last * carry_rows[2 * z + 1]
                d = jnp.concatenate([dz[it, z, g, padded, :] for g in range(groups)], axis=1)
                renewed = jnp.minimum(jnp.maximum(d + STEP * solved, fz[z, here, :]), 1.0)
                if it + 1 < ITERS:
                    keep_damage(it + 1, z, i * 8, renewed)
                change = renewed - d
                acc = acc + change * change
            return acc

        return lax.fori_loop(low // 8, high // 8, step, squares, unroll=2)

    def stream(it, ready):
        ready(order[0])
        ready(order[1])
        share_rows(it)
        a = 16
        for n in order[2:]:
            ready(n)
            b = cuts[n + 1] - 16 if n != order[-1] else cuts[4] + 16
            residual(it, a, b)
            x_product([(a, b)])
            a = b
            if n == order[2]:
                finish(v_sems.at[1, it], two_rows(it))
                mirror(it)
                residual(it, 0, 16)
                residual(it, cuts[4] + 16, cells)
                x_product([(0, 16), (cuts[4] + 16, cells)])

    def arrived(n):
        finish(d_rsem.at[n], piece_of(landing, cuts, n))
        regroup(cuts[n], cuts[n + 1])

    finish(e_sems.at[1], ez.at[others])
    scale_energy()
    stream(0, arrived)
    x_ends(0)
    x_share(0)
    for n in order[2:]:
        move_piece(bound, fz, n, f_ssem.at[0], f_rsem)
    for z in range(planes):
        y_product(0, z)
    finish(x_sems.at[1, 0], x_all.at[0, others])
    y_share(0)

    totals = []
    blank = jnp.zeros((8, width), f32)
    held = [blank]

    def settled(n):
        finish(f_rsem.at[n], piece_of(fz, cuts, n))
        held.append(settle(0, cuts[n], cuts[n + 1], held.pop()))

    stream(1, settled)
    def give_back(n, m):
        at = pl.ds(backs_at[n], backs_at[n + 1] - backs_at[n])
        send(final.at[col_peers[m], at, :], out.at[at, slab(col)], back_ssem.at[0],
             back_rsem.at[n], col=col_peers[m])

    def give_all(n):
        for m in range(cols - 1):
            give_back(n, m)

    def complete(low, high):
        @pl.loop(low // 8, high // 8, unroll=2)
        def _(i):
            here = eight(i * 8)
            tile = x_cols[here, :]
            ends_of = [
                jnp.concatenate([gy_ends[n, here, :]] * (cells // 128), axis=1) for n in range(2)
            ]
            for k in range(blocks):
                block = slice(k * cells, (k + 1) * cells)
                n = 8 * (k // x_blocks) + 2 * (k % x_blocks)
                value = (
                    out[here, block]
                    + tile[:, n : n + 1] * g_all[0, k]
                    + tile[:, n + 1 : n + 2] * g_all[1, k]
                    + (ends_of[0] * y_lines[0, k] + ends_of[1] * y_lines[1, k])
                )
                out[here, block] = jnp.minimum(jnp.maximum(value, bound[here, block]), 1.0)

    for m in range(cols - 1):
        y_first(1, col_peers[m])
        give_back(0, m)
    x_ends(1)
    x_share(1)
    for m in range(cols - 1):
        y_product(1, col_peers[m])
        give_back(1, m)
    y_first(1, col)
    y_product(1, col)
    out[:, slab(col)] = final[col]
    finish(x_sems.at[1, 1], x_all.at[1, others])
    sides, carried = y_share(1)
    for z in range(planes):
        for j in range(x_blocks):
            n = j * planes + z
            for side in range(2):
                at = 2 * j + side
                word_send[z, at : at + 1, :] = STEP * sides[side][n : n + 1]
                at += 2 * x_blocks
                word_send[z, at : at + 1, :] = STEP * carried[side][n : n + 1]
    for peer in col_peers:
        send(word_send.at[peer], word_all.at[col], w_sems.at[0], w_sems.at[1], col=peer)
    give_all(2)
    word_all[col] = word_send[col]
    totals.append(jnp.sum(held[0]))
    totals.append(jnp.sum(settle(ITERS - 1, 0, cells, blank)))
    s_send[...] = jnp.where(sub == 0, totals[0], jnp.where(sub == 1, totals[1], 0.0))
    for n, peer in enumerate(row_peers):
        send(s_send, s_row.at[n], s_sems.at[0], s_sems.at[1], row=peer)
    finish(s_sems.at[1], s_row)
    total = s_send[...]
    for n in range(rows - 1):
        total = total + s_row[n]
    s_col_send[...] = total
    for n, peer in enumerate(col_peers):
        send(s_col_send, s_col.at[n], s_sems.at[2], s_sems.at[3], col=peer)
    for n in range(3, len(backs_at) - 1):
        give_all(n)
    finish(w_sems.at[1], word_all.at[others])
    x_cols[...] = jnp.concatenate(
        [word_all[c] for c in range(cols)] + [jnp.zeros((128 - 8 * cols, cells), f32)], axis=0
    ).T
    for k in range(blocks):
        for side in range(2):
            at = 2 * x_blocks + 2 * (k % x_blocks) + side
            y_lines[side, k] = jnp.broadcast_to(
                word_all[k // x_blocks, at : at + 1, :], (8, cells)
            )
    for n in range(len(backs_at) - 2):
        finish(back_rsem.at[n], piece_of(final, backs_at, n))
        complete(backs_at[n], backs_at[n + 1])
    finish(s_sems.at[3], s_col)
    for n in range(cols - 1):
        total = total + s_col[n]
    sizes = jnp.sqrt(total / cell_count + EPSILON) / STEP
    norms[...] = jnp.where(lane == 0, sizes[:1, :], sizes[1:2, :])[0, :ITERS]
    for it in range(ITERS):
        finish(x_sems.at[0, it], x_all.at[it, others])
        finish(y_sems.at[0, it], y_all.at[it, pl.ds(0, rows - 1)])
        finish(v_sems.at[0, it], two_rows(it))
    finish(e_sems.at[0], ez.at[others])
    finish(d_ssem.at[0], landing.at[others])
    finish(f_ssem.at[0], fz.at[others])
    finish(w_sems.at[0], word_all.at[others])
    finish(s_sems.at[0], s_row)
    finish(s_sems.at[2], s_col)
    n = len(backs_at) - 2
    finish(back_rsem.at[n], piece_of(final, backs_at, n))
    complete(backs_at[n], backs_at[n + 1])
    finish(back_ssem.at[0], final.at[others])


def hand_over(damage, norms, damage_out, norms_out, sems):
    parts = 4
    part = damage.shape[0] // parts
    copies = [pltpu.make_async_copy(norms, norms_out, sems.at[parts])]
    for n in range(parts):
        at = pl.ds(n * part, part)
        copies.append(pltpu.make_async_copy(damage.at[at], damage_out.at[0, at], sems.at[n]))
    for copy in copies:
        copy.start()
    for copy in copies:
        copy.wait()


def local(energy, damage_old, crack_seeds, irreversible, line_inverses, z_inverse):
    planes, cells, line_length = energy.shape
    rows, cols = lax.axis_size("row"), lax.axis_size("col")
    blocks, _, _ = line_inverses.shape
    width = line_length // cols
    x_blocks = width // cells
    kinds = 2 * x_blocks + 2
    step = cells // 16
    cuts = (0, 3 * step, 8 * step, 12 * step, 13 * step, cells)
    backs_at = (0, 2 * step, 10 * step, 13 * step, 15 * step, cells)
    cell_count = float(cols * rows * cells * line_length)
    shape = (rows, cols, cells, width, x_blocks, blocks, cell_count, cuts, backs_at)
    f32 = jnp.float32
    bf16 = jnp.bfloat16
    dma = pltpu.SemaphoreType.DMA
    vmem = pl.BlockSpec(memory_space=pltpu.VMEM)
    damage, norms = pl.pallas_call(
        functools.partial(line_kernel, shape),
        out_shape=(
            pltpu.VMEM((cells, line_length), f32),
            pltpu.VMEM((ITERS,), f32),
        ),
        in_specs=[pl.BlockSpec(memory_space=pl.ANY)] * 6,
        out_specs=(vmem, vmem),
        scratch_shapes=[
            pltpu.VMEM((cells, line_length), f32),
            pltpu.VMEM((cells, line_length), jnp.int32),
            pltpu.VMEM((cells, line_length), jnp.int32),
            pltpu.VMEM((cells, line_length), f32),
            pltpu.VMEM((cells, line_length), f32),
            pltpu.VMEM((cells, line_length), f32),
            pltpu.VMEM((cols, cells, width), f32),
            pltpu.VMEM((cols, cells, width), f32),
            pltpu.VMEM((cols, cells, width), f32),
            pltpu.VMEM((cols, cells, width), f32),
            pltpu.VMEM((cols, cells, width), f32),
            pltpu.VMEM((ITERS, cols, width // 128, cells + 16, 128), f32),
            pltpu.VMEM((cols, cells, width), f32),
            pltpu.VMEM((cols, cells, width), bf16),
            pltpu.VMEM((cols, cells, width), bf16),
            pltpu.VMEM((cols, cells, width), bf16),
            pltpu.VMEM((cols, cells, width), bf16),
            pltpu.VMEM((cols, cells, width), f32),
            pltpu.VMEM((blocks, cells, cells), f32),
            pltpu.VMEM((x_blocks, cells, cells), bf16),
            pltpu.VMEM((x_blocks, cells, cells), bf16),
            pltpu.VMEM((2 * cells, cells), bf16),
            pltpu.VMEM((2, cells, 128), f32),
            pltpu.VMEM((2, x_blocks + 1, 8, cells), f32),
            pltpu.VMEM((kinds, 8, 128), f32),
            pltpu.VMEM((2 * x_blocks, cols, 8, 128), f32),
            pltpu.VMEM((2 * x_blocks, kinds, 8, 128), f32),
            pltpu.VMEM((2, rows, 8, 128), f32),
            pltpu.VMEM((8, 128), f32),
            pltpu.VMEM((2 * cols, 8, width), f32),
            pltpu.VMEM((kinds, 8, cells), f32),
            pltpu.VMEM((cols, 8, 128), f32),
            pltpu.VMEM((2, cols, 8, cells), f32),
            pltpu.VMEM((2, blocks, 8, cells), f32),
            pltpu.VMEM((cols, 8, cells), f32),
            pltpu.VMEM((cols, 8, cells), f32),
            pltpu.VMEM((cells, 128), f32),
            pltpu.VMEM((2, blocks, 8, cells), f32),
            pltpu.VMEM((ITERS, 8, cells), f32),
            pltpu.VMEM((ITERS, cols, 8, cells), f32),
            pltpu.VMEM((ITERS, 2, 8, cells), f32),
            pltpu.VMEM((ITERS, rows, 8, cells), f32),
            pltpu.VMEM((8, 128), f32),
            pltpu.VMEM((rows - 1, 8, 128), f32),
            pltpu.VMEM((8, 128), f32),
            pltpu.VMEM((cols - 1, 8, 128), f32),
            pltpu.SMEM((cols, cols), f32),
            dma((7,)),
            pltpu.SemaphoreType.REGULAR((2,)),
            dma((2,)),
            dma((1,)),
            dma((5,)),
            dma((1,)),
            dma((5,)),
            dma((1,)),
            dma((5,)),
            dma((2,)),
            dma((2, ITERS)),
            dma((2, ITERS)),
            dma((2, ITERS)),
            dma((4,)),
        ],
        compiler_params=pltpu.CompilerParams(
            has_side_effects=True, collective_id=0, vmem_limit_bytes=60 * 1024 * 1024
        ),
        name="line_iterations",
    )(
        z_inverse,
        energy[0],
        damage_old[0],
        crack_seeds[0],
        irreversible[0],
        line_inverses,
    )
    return pl.pallas_call(
        hand_over,
        out_shape=(
            jax.ShapeDtypeStruct((1, cells, line_length), f32),
            jax.ShapeDtypeStruct((ITERS,), f32),
        ),
        in_specs=[vmem, vmem],
        out_specs=(pl.BlockSpec(memory_space=pl.ANY), pl.BlockSpec(memory_space=pl.ANY)),
        scratch_shapes=[dma((5,))],
        compiler_params=pltpu.CompilerParams(vmem_limit_bytes=1024 * 1024),
        name="hand_over",
    )(
        pltpu.with_memory_space_constraint(damage, pltpu.VMEM),
        pltpu.with_memory_space_constraint(norms, pltpu.VMEM),
    )


def solution(mesh):
    def local_any(energy, damage_old, crack_seeds, irreversible, line_inverses, z_inverse):
        rows, cols = mesh.shape["row"], mesh.shape["col"]
        block_cells = line_inverses.shape[1]
        width = energy.shape[2] // cols
        whole_blocks = (
            energy.shape[0] == 1
            and energy.shape[1] == block_cells
            and width == 2 * block_cells
            and block_cells % 256 == 0
            and 2 * cols == 8
            and 2 * rows <= 128
            and min(rows, cols) > 2
        )
        chosen = local if whole_blocks else local_turned
        return chosen(energy, damage_old, crack_seeds, irreversible, line_inverses, z_inverse)

    return jax.shard_map(
        local_any,
        mesh=mesh,
        in_specs=(
            P("col", "row", None),
            P("col", "row", None),
            P("col", "row", None),
            P("col", "row", None),
            P(),
            P(),
        ),
        out_specs=(P("col", "row", None), P()),
        check_vma=False,
    )
```
